32 devices in a mesh: tp: 4 (over z), sp: 8 (over y, x, core).
Axes of the slice: x: 2, y: 2, z: 4, core: 2. Of those that a mesh axis runs over, the one named last changes fastest.
Arguments:
- x_tok: bfloat16 [256, 4096], replicated
- seq_lens: int32 [256], replicated
- k_cache: bfloat16 [256, 512, 8, 128], P(None, 'sp', 'tp')
- v_cache: bfloat16 [256, 512, 8, 128], P(None, 'sp', 'tp')
- g_attn: bfloat16 [4096], replicated
- w_q: bfloat16 [4096, 4096], P(None, 'tp')
- w_k: bfloat16 [4096, 1024], P(None, 'tp')
- w_v: bfloat16 [4096, 1024], P(None, 'tp')
- w_o: bfloat16 [4096, 4096], P('tp')
- g_mlp: bfloat16 [4096], replicated
- w_gate: bfloat16 [4096, 14336], P(None, 'tp')
- w_up: bfloat16 [4096, 14336], P(None, 'tp')
- w_down: bfloat16 [14336, 4096], P('tp')
Outputs:
- output 1: bfloat16 [256, 4096], replicated
- output 2: bfloat16 [256, 512, 8, 128], P(None, 'sp', 'tp')
- output 3: bfloat16 [256, 512, 8, 128], P(None, 'sp', 'tp')
All inputs are finite; a program needn't handle non-finite values.
Results may differ from the reference program's by a relative error of at most 0.0133669.
Values sent between devices are 32-bit elements.
A program may use at most 1 GiB of HBM per device.

```python
import math
import jax
import jax.numpy as jnp
from jax import lax

MODEL_DIM = 4096
Q_HEADS = 32
KV_HEADS = 8
HEAD_DIM = 128
FF_DIM = 14336
BATCH_SIZE = 256
SEQ_LEN = 512

ROPE_BASE = 500000.0
NORM_EPS = 1e-5


def gauss_draw(rng_key, arr_shape):
    return jax.random.normal(rng_key, arr_shape, jnp.float32)


def draw_lens(rng_key):
    low_len = SEQ_LEN // 4
    key_len, key_hi, key_lo = jax.random.split(rng_key, 3)
    lens_raw = jax.random.randint(key_len, (BATCH_SIZE,), low_len, SEQ_LEN)
    idx_hi = jax.random.randint(key_hi, (), 0, BATCH_SIZE)
    idx_lo = (idx_hi + jax.random.randint(key_lo, (), 1, BATCH_SIZE)) % BATCH_SIZE
    row_ids = jnp.arange(BATCH_SIZE)
    lens_raw = jnp.where(row_ids == idx_hi, SEQ_LEN - 1, lens_raw)
    lens_raw = jnp.where(row_ids == idx_lo, low_len, lens_raw)
    return lens_raw.astype(jnp.int32)


def setup_inputs(seed: int = 0) -> dict:
    key_list = jax.random.split(jax.random.key(seed), 14)
    q_width = Q_HEADS * HEAD_DIM
    kv_width = KV_HEADS * HEAD_DIM
    groups = Q_HEADS // KV_HEADS
    cache_shape = (BATCH_SIZE, SEQ_LEN, KV_HEADS, HEAD_DIM)
    w_q32 = gauss_draw(key_list[4], (MODEL_DIM, q_width)) * MODEL_DIM ** -0.5
    self_gain = (math.log(SEQ_LEN) - 0.6) * math.sqrt(groups / HEAD_DIM)
    group_sum = jnp.sum(w_q32.reshape(MODEL_DIM, KV_HEADS, groups, HEAD_DIM), axis=2).reshape(MODEL_DIM, kv_width)
    w_k32 = group_sum * (self_gain / math.sqrt(groups)) + gauss_draw(key_list[5], (MODEL_DIM, kv_width)) * (0.5 * MODEL_DIM ** -0.5)
    value_scale = 0.5 * math.sqrt(SEQ_LEN)
    return {
        "x_tok": gauss_draw(key_list[0], (BATCH_SIZE, MODEL_DIM)).astype(jnp.bfloat16),
        "seq_lens": draw_lens(key_list[1]),
        "k_cache": gauss_draw(key_list[2], cache_shape).astype(jnp.bfloat16),
        "v_cache": (gauss_draw(key_list[3], cache_shape) * value_scale).astype(jnp.bfloat16),
        "g_attn": (1.0 + 0.2 * gauss_draw(key_list[6], (MODEL_DIM,))).astype(jnp.bfloat16),
        "w_q": w_q32.astype(jnp.bfloat16),
        "w_k": w_k32.astype(jnp.bfloat16),
        "w_v": (gauss_draw(key_list[7], (MODEL_DIM, kv_width)) * MODEL_DIM ** -0.5).astype(jnp.bfloat16),
        "w_o": (gauss_draw(key_list[8], (q_width, MODEL_DIM)) * q_width ** -0.5).astype(jnp.bfloat16),
        "g_mlp": (1.0 + 0.2 * gauss_draw(key_list[9], (MODEL_DIM,))).astype(jnp.bfloat16),
        "w_gate": (gauss_draw(key_list[10], (MODEL_DIM, FF_DIM)) * MODEL_DIM ** -0.5).astype(jnp.bfloat16),
        "w_up": (gauss_draw(key_list[11], (MODEL_DIM, FF_DIM)) * MODEL_DIM ** -0.5).astype(jnp.bfloat16),
        "w_down": (gauss_draw(key_list[12], (FF_DIM, MODEL_DIM)) * FF_DIM ** -0.5).astype(jnp.bfloat16),
    }


def rms_norm(x_in, norm_gain):
    x_f32 = x_in.astype(jnp.float32)
    inv_rms = lax.rsqrt(jnp.mean(x_f32 * x_f32, axis=-1, keepdims=True) + NORM_EPS)
    return (x_f32 * inv_rms * norm_gain.astype(jnp.float32)).astype(jnp.bfloat16)


def apply_rope(heads_in, positions):
    head_dim = heads_in.shape[-1]
    half_dim = head_dim // 2
    inv_freq = jnp.power(jnp.float32(ROPE_BASE), jnp.arange(half_dim, dtype=jnp.float32) * (-2.0 / head_dim))
    angles = positions.astype(jnp.float32)[:, None, None] * inv_freq
    cos_a = jnp.cos(angles)
    sin_a = jnp.sin(angles)
    heads_f32 = heads_in.astype(jnp.float32)
    first_half = heads_f32[..., :half_dim]
    second_half = heads_f32[..., half_dim:]
    rotated = jnp.concatenate([first_half * cos_a - second_half * sin_a, second_half * cos_a + first_half * sin_a], axis=-1)
    return rotated.astype(jnp.bfloat16)


def reference(x_tok, seq_lens, k_cache, v_cache, g_attn, w_q, w_k, w_v, w_o, g_mlp, w_gate, w_up, w_down):
    groups = Q_HEADS // KV_HEADS
    x_norm = rms_norm(x_tok, g_attn)
    q_new = jnp.dot(x_norm, w_q, preferred_element_type=jnp.float32).astype(jnp.bfloat16).reshape(BATCH_SIZE, Q_HEADS, HEAD_DIM)
    k_new = jnp.dot(x_norm, w_k, preferred_element_type=jnp.float32).astype(jnp.bfloat16).reshape(BATCH_SIZE, KV_HEADS, HEAD_DIM)
    v_new = jnp.dot(x_norm, w_v, preferred_element_type=jnp.float32).astype(jnp.bfloat16).reshape(BATCH_SIZE, KV_HEADS, HEAD_DIM)
    q_rot = apply_rope(q_new, seq_lens)
    k_rot = apply_rope(k_new, seq_lens)
    row_ids = jnp.arange(BATCH_SIZE)
    k_out = k_cache.at[row_ids, seq_lens].set(k_rot)
    v_out = v_cache.at[row_ids, seq_lens].set(v_new)
    score_scale = HEAD_DIM ** -0.5

    def attend_row(row_inputs):
        q_row, k_rows, v_rows, row_len = row_inputs
        scores = jnp.einsum("kgd,tkd->kgt", q_row.astype(jnp.float32), k_rows.astype(jnp.float32)) * score_scale
        is_valid = jnp.arange(SEQ_LEN) <= row_len
        masked = jnp.where(is_valid, scores, -jnp.inf)
        row_max = jnp.max(masked, axis=-1, keepdims=True)
        weights = jnp.exp(masked - row_max)
        row_sum = jnp.sum(weights, axis=-1, keepdims=True)
        mixed = jnp.einsum("kgt,tkd->kgd", weights.astype(jnp.bfloat16).astype(jnp.float32), v_rows.astype(jnp.float32))
        return (mixed / row_sum).astype(jnp.bfloat16)

    attn_heads = lax.map(attend_row, (q_rot.reshape(BATCH_SIZE, KV_HEADS, groups, HEAD_DIM), k_out, v_out, seq_lens))
    attn_flat = attn_heads.reshape(BATCH_SIZE, Q_HEADS * HEAD_DIM)
    attn_proj = jnp.dot(attn_flat, w_o, preferred_element_type=jnp.float32)
    hidden = (x_tok.astype(jnp.float32) + attn_proj).astype(jnp.bfloat16)
    h_norm = rms_norm(hidden, g_mlp)
    gate_proj = jnp.dot(h_norm, w_gate, preferred_element_type=jnp.float32).astype(jnp.bfloat16)
    up_proj = jnp.dot(h_norm, w_up, preferred_element_type=jnp.float32).astype(jnp.bfloat16)
    act_prod = (jax.nn.silu(gate_proj.astype(jnp.float32)) * up_proj.astype(jnp.float32)).astype(jnp.bfloat16)
    mlp_out = jnp.dot(act_prod, w_down, preferred_element_type=jnp.float32)
    y_out = (hidden.astype(jnp.float32) + mlp_out).astype(jnp.bfloat16)
    return (y_out, k_out, v_out)
```

```python
import functools

import jax
import jax.numpy as jnp
from jax import lax
from jax.experimental import pallas as pl
from jax.experimental.pallas import tpu as pltpu
from jax.sharding import PartitionSpec as P

ROPE_BASE = 500000.0
NORM_EPS = 1e-5
MESH = pl.DeviceIdType.MESH
F32 = jnp.float32
BF16 = jnp.bfloat16
ANY = pl.BlockSpec(memory_space=pl.ANY)
VMEM = pl.BlockSpec(memory_space=pltpu.VMEM)
NEG = -1e30
BLK = 256


def qkv_kernel(x_hbm, g_ref, cos_ref, sin_ref, wq_hbm, wk_hbm, wv_hbm, q_ref, k_ref, v_ref, x_buf, u_buf, w_buf, x_sem, w_sem):
    rows = x_buf.shape[0]
    dim = x_buf.shape[1]
    nq = wq_hbm.shape[1] // BLK
    heads = wq_hbm.shape[1] // 128
    copies = [pltpu.make_async_copy(wq_hbm.at[:, pl.ds(i * BLK, BLK)], w_buf.at[i], w_sem.at[i]) for i in range(nq)]
    copies.append(pltpu.make_async_copy(wk_hbm, w_buf.at[nq], w_sem.at[nq]))
    copies.append(pltpu.make_async_copy(wv_hbm, w_buf.at[nq + 1], w_sem.at[nq + 1]))
    x_copy = pltpu.make_async_copy(x_hbm, x_buf, x_sem)
    x_copy.start()
    for cp in copies:
        cp.start()
    x_copy.wait()
    gain = g_ref[...]

    def norm(i, carry):
        at = pl.ds(pl.multiple_of(i * 16, 16), 16)
        xf = x_buf[at, :].astype(F32)
        inv = lax.rsqrt(jnp.sum(xf * xf, axis=-1, keepdims=True) * (1.0 / dim) + NORM_EPS)
        u_buf[at, :] = (xf * inv * gain).astype(BF16)
        return carry

    lax.fori_loop(0, rows // 16, norm, 0)
    cosv = cos_ref[...]
    sinv = sin_ref[...]

    def rope(h):
        h = h.astype(BF16).astype(F32)
        return (h * cosv + pltpu.roll(h, 64, 1) * sinv).astype(BF16).astype(F32)

    for i in range(nq + 2):
        copies[i].wait()
        prod = jnp.dot(u_buf[...], w_buf[i], preferred_element_type=F32)
        for s in range(2):
            part = prod[:, s * 128 : (s + 1) * 128]
            if i < nq:
                q_ref[pl.ds(2 * i + s, rows, stride=heads), :] = rope(part)
            elif i == nq:
                k_ref[pl.ds(s, rows, stride=2), :] = rope(part)
            else:
                v_ref[pl.ds(s, rows, stride=2), :] = part.astype(BF16).astype(F32)


def qkv(x, g, cosv, sinv, wq, wk, wv):
    rows, dim = x.shape
    heads = wq.shape[1] // 128
    nblk = wq.shape[1] // BLK + 2
    return pl.pallas_call(
        qkv_kernel,
        out_shape=(
            jax.ShapeDtypeStruct((rows * heads, 128), F32),
            jax.ShapeDtypeStruct((rows * 2, 128), F32),
            jax.ShapeDtypeStruct((rows * 2, 128), F32),
        ),
        in_specs=[ANY, VMEM, VMEM, VMEM, ANY, ANY, ANY],
        out_specs=(VMEM, VMEM, VMEM),
        scratch_shapes=[
            pltpu.VMEM((rows, dim), BF16),
            pltpu.VMEM((rows, dim), BF16),
            pltpu.VMEM((nblk, dim, BLK), BF16),
            pltpu.SemaphoreType.DMA,
            pltpu.SemaphoreType.DMA((nblk,)),
        ],
        compiler_params=pltpu.CompilerParams(vmem_limit_bytes=63_000_000),
        cost_estimate=pl.CostEstimate(flops=2 * rows * dim * nblk * BLK, bytes_accessed=2 * dim * nblk * BLK, transcendentals=0),
        name="qkv",
    )(x, g, cosv, sinv, wq, wk, wv)


def attn_kernel(lens_ref, q_ref, kn_ref, vn_ref, k_ref, v_ref, ko_ref, vo_ref, out_ref):
    nreq = k_ref.shape[0]
    base = lax.axis_index("sp") * 64
    g = pl.program_id(0)
    lane = lax.broadcasted_iota(jnp.int32, (8, 128), 1)
    head = lax.broadcasted_iota(jnp.int32, (8, 128), 0)
    match = (lane % 2) == (head // 4)
    lane_pos = jnp.where(match, lane // 2, 1 << 20)
    row_pos = (lax.broadcasted_iota(jnp.int32, (8, 16, 128), 0) * 8 + lax.broadcasted_iota(jnp.int32, (8, 16, 128), 1) // 2).astype(F32).astype(BF16)
    odd = (lax.broadcasted_iota(jnp.int32, (16, 128), 0) % 2) == 1
    scale = 128.0**-0.5
    zero = jnp.zeros((8, 128), BF16)

    def update(c_ref, n_ref, o_ref, b, pos_b):
        row0 = jnp.broadcast_to(n_ref[pl.ds(2 * b, 1), :], (16, 128))
        row1 = jnp.broadcast_to(n_ref[pl.ds(2 * b + 1, 1), :], (16, 128))
        new = jnp.where(odd, row1, row0).astype(BF16)
        upd = jnp.where(row_pos == pos_b, new[None], c_ref[b])
        o_ref[b] = upd
        return upd.reshape(128, 128)

    def step(it, carry):
        stm, stl = carry
        for pair in range(4):
            keys, vals, poss = [], [], []
            first = it * 8 + pair * 2
            for j in range(2):
                b = first + j
                pos = lens_ref[g * nreq + b] - base
                pos_b = jnp.full((8, 16, 128), pos, jnp.int32).astype(F32).astype(BF16)
                keys.append(update(k_ref, kn_ref, ko_ref, b, pos_b))
                vals.append(update(v_ref, vn_ref, vo_ref, b, pos_b))
                poss.append(pos)
            qrow = pl.multiple_of(first * 8, 16)
            qp = q_ref[pl.ds(qrow, 16), :].astype(BF16)
            sc = lax.dot_general(qp, jnp.concatenate(keys, axis=0), (((1,), (1,)), ((), ())), preferred_element_type=F32) * scale
            wts = []
            for j in range(2):
                s = sc[8 * j : 8 * j + 8, 128 * j : 128 * j + 128]
                valid = lane_pos <= poss[j]
                m = jnp.max(jnp.where(valid, s, NEG), axis=1, keepdims=True)
                w = jnp.where(valid, jnp.exp(s - m), 0.0)
                here = lane == first + j
                stm = jnp.where(here, m, stm)
                stl = jnp.where(here, jnp.sum(w, axis=1, keepdims=True), stl)
                wts.append(w.astype(BF16))
            wp = jnp.concatenate([jnp.concatenate([wts[0], zero], axis=1), jnp.concatenate([zero, wts[1]], axis=1)], axis=0)
            out_ref[0, pl.ds(qrow, 16), :] = jnp.dot(wp, jnp.concatenate(vals, axis=0), preferred_element_type=F32)
        return stm, stl

    stm, stl = lax.fori_loop(0, nreq // 8, step, (jnp.zeros((8, 128), F32), jnp.ones((8, 128), F32)))
    out_ref[0, pl.ds(nreq * 8, 8), :] = stm
    out_ref[0, pl.ds(nreq * 8 + 8, 8), :] = stl


def attn(lens, q, kn, vn, k, v):
    batch = k.shape[0]
    nreq = 32
    steps = batch // nreq
    cache = pl.BlockSpec((nreq, 8, 16, 128), lambda i, *_: (i, 0, 0, 0))
    return pl.pallas_call(
        attn_kernel,
        grid_spec=pltpu.PrefetchScalarGridSpec(
            num_scalar_prefetch=1,
            grid=(steps,),
            in_specs=[
                pl.BlockSpec((nreq * 8, 128), lambda i, *_: (i, 0)),
                pl.BlockSpec((nreq * 2, 128), lambda i, *_: (i, 0)),
                pl.BlockSpec((nreq * 2, 128), lambda i, *_: (i, 0)),
                cache,
                cache,
            ],
            out_specs=[cache, cache, pl.BlockSpec((1, nreq * 8 + 16, 128), lambda i, *_: (i, 0, 0))],
        ),
        out_shape=[
            jax.ShapeDtypeStruct(k.shape, BF16),
            jax.ShapeDtypeStruct(v.shape, BF16),
            jax.ShapeDtypeStruct((steps, nreq * 8 + 16, 128), F32),
        ],
        compiler_params=pltpu.CompilerParams(vmem_limit_bytes=63_000_000, dimension_semantics=("arbitrary",)),
        cost_estimate=pl.CostEstimate(flops=batch * 2**20, bytes_accessed=8 * k.size, transcendentals=0),
        name="attn",
    )(lens, q, kn, vn, k, v)


def merge(blocks, out_ref, rows, last):
    maxs = [b[rows : rows + 8, :] for b in blocks]
    top = functools.reduce(jnp.maximum, maxs)
    facs = [jnp.exp(m - top) for m in maxs]
    tot = functools.reduce(jnp.add, [f * b[rows + 8 : rows + 16, :] for f, b in zip(facs, blocks)])
    if last:
        inv = 1.0 / tot
        facs = [f * inv for f in facs]
    else:
        out_ref[rows : rows + 8, :] = top
        out_ref[rows + 8 : rows + 16, :] = tot
    for i in range(rows // 8):
        at = slice(8 * i, 8 * i + 8)
        out_ref[at, :] = functools.reduce(jnp.add, [b[at, :] * f[:, i : i + 1] for f, b in zip(facs, blocks)])


def tail_kernel(
    att_ref, x_hbm, g_ref, wo_hbm, wg_hbm, wu_hbm, wd_hbm, y_ref,
    d1_buf, m_buf, r1_buf, o_buf, p_buf, z1_buf, h_buf, hb_buf, a_buf, p2_buf, d2_buf, s2_buf, z2_buf, yg_buf, x_buf, hid_buf,
    wo_buf, wg_buf, wu_buf, wd_buf,
    lsem, gsem, usem, dsem, d1s, d1r, r1s, r1r, z1s, z1r, hs, hr, hds, hdr, d2s, d2r, z2s, z2r, ys, yr, ydr,
):
    tp, sp = lax.axis_index("tp"), lax.axis_index("sp")
    core, chip = sp % 2, sp // 2
    cx, cy = chip % 2, chip // 2
    mate = {"tp": tp, "sp": 2 * chip + (1 - core)}
    plane = [(chip + k) % 4 for k in range(4)]
    plane_id = [{"tp": tp, "sp": 2 * q + core} for q in plane]
    zs = [(tp + k) % 4 for k in range(4)]
    z_id = [{"tp": z, "sp": sp} for z in zs]
    rows = att_ref.shape[1] - 16
    dim = x_buf.shape[1]
    ring = wg_buf.shape[0]
    half = wd_buf.shape[1]
    nff = half // BLK
    ndn = wd_buf.shape[0]
    dcol = wd_buf.shape[2]

    me8 = pl.multiple_of(32 * sp + 8 * tp, 8)
    x_copy = pltpu.make_async_copy(x_hbm.at[pl.ds(me8, 8), :], x_buf, lsem.at[0])
    wo_copy = pltpu.make_async_copy(wo_hbm, wo_buf, lsem.at[1])

    def ff_copies(j, slot):
        at = pl.ds(pl.multiple_of(core * half + j * BLK, BLK), BLK)
        return (
            pltpu.make_async_copy(wg_hbm.at[:, at], wg_buf.at[slot], gsem.at[slot]),
            pltpu.make_async_copy(wu_hbm.at[:, at], wu_buf.at[slot], usem.at[slot]),
        )

    def dn_copy(j):
        return pltpu.make_async_copy(
            wd_hbm.at[pl.ds(pl.multiple_of(core * half, BLK), half), pl.ds(pl.multiple_of(j * dcol, dcol), dcol)], wd_buf.at[j], dsem.at[j]
        )

    wo_copy.start()
    x_copy.start()
    for j in range(min(ring, nff)):
        for cp in ff_copies(j, j):
            cp.start()
    for j in range(ndn):
        dn_copy(j).start()

    bar = pltpu.get_barrier_semaphore()
    for dev in [mate] + plane_id[1:] + z_id[1:]:
        pl.semaphore_signal(bar, inc=1, device_id=dev, device_id_type=MESH)
    pl.semaphore_wait(bar, 7)

    def send(src, dst, ssem, rsem, dev):
        cp = pltpu.make_async_remote_copy(src_ref=src, dst_ref=dst, send_sem=ssem, recv_sem=rsem, device_id=dev, device_id_type=MESH)
        cp.start()
        return cp

    order = [1, 2, 3, 0]
    d1 = {k: send(att_ref.at[2 * plane[k] + (1 - core)], d1_buf.at[k], d1s.at[k], d1r.at[k], mate) for k in order}
    r1 = {}
    for k in order:
        d1[k].wait_recv()
        merge([att_ref.at[2 * plane[k] + core], d1_buf.at[k]], m_buf.at[k], rows, False)
        if k:
            r1[k] = send(m_buf.at[k], r1_buf.at[k - 1], r1s.at[k - 1], r1r.at[k - 1], plane_id[k])
    for k in (1, 2, 3):
        r1[k].wait_recv()
    merge([m_buf.at[0]] + [r1_buf.at[k] for k in range(3)], o_buf, rows, True)

    nreq = rows // 8
    o = jnp.concatenate([o_buf[pl.ds(h, nreq, stride=8), :].astype(BF16) for h in range(8)], axis=1)
    wo_copy.wait()

    def proj(j, carry):
        at = pl.ds(pl.multiple_of(j * 512, 512), 512)
        p_buf[:, at] = jnp.dot(o, wo_buf[:, at], preferred_element_type=F32)
        return carry

    lax.fori_loop(0, dim // 512, proj, 0)

    def z_scatter(src, buf, ss, rs):
        return [send(src.at[pl.ds(pl.multiple_of(8 * zs[k], 8), 8), :], buf.at[k - 1], ss.at[k - 1], rs.at[k - 1], z_id[k]) for k in (1, 2, 3)]

    own = pl.ds(pl.multiple_of(8 * tp, 8), 8)
    z1 = z_scatter(p_buf, z1_buf, z1s, z1r)
    x_copy.wait()
    for cp in z1:
        cp.wait_recv()
    hid = (x_buf[...].astype(F32) + (p_buf[own, :] + z1_buf[0] + z1_buf[1] + z1_buf[2])).astype(BF16).astype(F32)
    hid_buf[...] = hid
    inv = lax.rsqrt(jnp.sum(hid * hid, axis=-1, keepdims=True) * (1.0 / dim) + NORM_EPS)
    mine = core * 4
    h_buf[mine + tp] = (hid * inv * g_ref[...]).astype(BF16).astype(F32)

    hz = [send(h_buf.at[mine + tp], h_buf.at[mine + tp], hs.at[k - 1], hr.at[k - 1], z_id[k]) for k in (1, 2, 3)]
    hd = [send(h_buf.at[mine + tp], h_buf.at[mine + tp], hds.at[0], hdr.at[0], mate)]
    for k in (1, 2, 3):
        hz[k - 1].wait_recv()
        slot = mine + (tp + 4 - k) % 4
        hd.append(send(h_buf.at[slot], h_buf.at[slot], hds.at[k], hdr.at[k], mate))
    for cp in hd:
        cp.wait_recv()
    for i in range(4):
        hb_buf[16 * i : 16 * i + 16, :] = jnp.concatenate([h_buf[2 * i], h_buf[2 * i + 1]], axis=0).astype(BF16)

    def ff(j, carry):
        slot = lax.rem(j, ring)
        for cp in ff_copies(j, slot):
            cp.wait()
        gate = jnp.dot(hb_buf[...], wg_buf[slot], preferred_element_type=F32).astype(BF16).astype(F32)
        up = jnp.dot(hb_buf[...], wu_buf[slot], preferred_element_type=F32).astype(BF16).astype(F32)
        a_buf[:, pl.ds(pl.multiple_of(j * BLK, BLK), BLK)] = (gate * jax.nn.sigmoid(gate) * up).astype(BF16)

        @pl.when(j + ring < nff)
        def _():
            for cp in ff_copies(j + ring, slot):
                cp.start()

        return carry

    lax.fori_loop(0, nff, ff, 0)

    def down(j, carry):
        dn_copy(j).wait()
        p2_buf[:, pl.ds(pl.multiple_of(j * dcol, dcol), dcol)] = jnp.dot(a_buf[...], wd_buf[j], preferred_element_type=F32)
        return carry

    lax.fori_loop(0, ndn, down, 0)

    d2 = send(p2_buf.at[pl.ds(pl.multiple_of(32 * (1 - core), 32), 32), :], d2_buf, d2s, d2r, mate)
    d2.wait_recv()
    s2_buf[...] = p2_buf[pl.ds(pl.multiple_of(32 * core, 32), 32), :] + d2_buf[...]
    z2 = z_scatter(s2_buf, z2_buf, z2s, z2r)
    for cp in z2:
        cp.wait_recv()

    xn = 2 * cy + (1 - cx)
    yn = 2 * (1 - cy) + cx
    dg = 2 * (1 - cy) + (1 - cx)
    xn_id, yn_id = {"tp": tp, "sp": 2 * xn + core}, {"tp": tp, "sp": 2 * yn + core}

    def block(c, k):
        return yg_buf.at[4 * (2 * c + core) + (tp + k) % 4]

    started = []

    def pass_on(c, k, dev, rs):
        started.append(send(block(c, k), block(c, k), ys.at[len(started)], rs, dev))

    def landed(c, k, rs):
        pltpu.make_async_copy(block(c, k), block(c, k), rs).wait()

    yg_buf[4 * sp + tp] = (hid_buf[...] + (s2_buf[own, :] + z2_buf[0] + z2_buf[1] + z2_buf[2])).astype(BF16).astype(F32)
    for k in (1, 2, 3):
        pass_on(chip, 0, z_id[k], yr.at[(4 - k) % 4])
    pass_on(chip, 0, xn_id, yr.at[4])
    pass_on(chip, 0, yn_id, yr.at[8])
    pass_on(chip, 0, mate, ydr.at[0])

    def around(k):
        landed(xn, k, yr.at[4 + k])
        if k % 2 == 0:
            pass_on(xn, k, yn_id, yr.at[12 + k])
        pass_on(xn, k, mate, ydr.at[4 + k])
        landed(yn, k, yr.at[8 + k])
        if k % 2 == 1:
            pass_on(yn, k, xn_id, yr.at[12 + k])
        pass_on(yn, k, mate, ydr.at[8 + k])

    for k in (1, 2, 3):
        landed(chip, k, yr.at[k])
        pass_on(chip, k, xn_id, yr.at[4 + k])
        pass_on(chip, k, yn_id, yr.at[8 + k])
        pass_on(chip, k, mate, ydr.at[k])
        around(k - 1)
    around(3)
    for k in range(4):
        landed(dg, k, yr.at[12 + k])
        pass_on(dg, k, mate, ydr.at[12 + k])
    for i, c in enumerate((chip, xn, yn, dg)):
        for k in range(4):
            other = yg_buf.at[4 * (2 * c + (1 - core)) + (tp + k) % 4]
            pltpu.make_async_copy(other, other, ydr.at[4 * i + k]).wait()

    def out(i, carry):
        y_ref[pl.ds(pl.multiple_of(i * 16, 16), 16), :] = jnp.concatenate([yg_buf[2 * i], yg_buf[2 * i + 1]], axis=0).astype(BF16)
        return carry

    lax.fori_loop(0, yg_buf.shape[0] // 2, out, 0)
    for cp in list(d1.values()) + list(r1.values()) + z1 + hz + hd + [d2] + z2 + started:
        cp.wait_send()


def tail(att, x, g, wo, wg, wu, wd):
    batch, dim = x.shape
    groups, rows16, _ = att.shape
    half = wg.shape[1] // 2
    ring = min(4, half // BLK)
    ndn = 8
    dma = pltpu.SemaphoreType.DMA
    return pl.pallas_call(
        tail_kernel,
        out_shape=jax.ShapeDtypeStruct((batch, dim), BF16),
        in_specs=[VMEM, ANY, VMEM, ANY, ANY, ANY, ANY],
        out_specs=VMEM,
        scratch_shapes=[
            pltpu.VMEM((4, rows16, 128), F32),
            pltpu.VMEM((4, rows16, 128), F32),
            pltpu.VMEM((3, rows16, 128), F32),
            pltpu.VMEM((rows16 - 16, 128), F32),
            pltpu.VMEM((32, dim), F32),
            pltpu.VMEM((3, 8, dim), F32),
            pltpu.VMEM((8, 8, dim), F32),
            pltpu.VMEM((64, dim), BF16),
            pltpu.VMEM((64, half), BF16),
            pltpu.VMEM((64, dim), F32),
            pltpu.VMEM((32, dim), F32),
            pltpu.VMEM((32, dim), F32),
            pltpu.VMEM((3, 8, dim), F32),
            pltpu.VMEM((batch // 8, 8, dim), F32),
            pltpu.VMEM((8, dim), BF16),
            pltpu.VMEM((8, dim), F32),
            pltpu.VMEM(wo.shape, BF16),
            pltpu.VMEM((ring, dim, BLK), BF16),
            pltpu.VMEM((ring, dim, BLK), BF16),
            pltpu.VMEM((ndn, half, dim // ndn), BF16),
            dma((2,)), dma((ring,)), dma((ring,)), dma((ndn,)),
            dma((4,)), dma((4,)), dma((3,)), dma((3,)), dma((3,)), dma((3,)),
            dma((3,)), dma((3,)), dma((4,)), dma((4,)), dma, dma, dma((3,)), dma((3,)),
            dma((40,)), dma((16,)), dma((16,)),
        ],
        compiler_params=pltpu.CompilerParams(collective_id=0, has_side_effects=True, vmem_limit_bytes=63_000_000),
        cost_estimate=pl.CostEstimate(flops=2 * 64 * dim * half * 3, bytes_accessed=6 * dim * half, transcendentals=0),
        name="tail",
    )(att, x, g, wo, wg, wu, wd)


def solution(mesh):
    cache_spec = P(None, "sp", "tp", None)
    col_spec = P(None, "tp")
    row_spec = P("tp", None)
    full_spec = P()

    def local_step(x_tok, seq_lens, k_blk, v_blk, g_attn, wq, wk, wv, wo, g_mlp, wg, wu, wd):
        batch = x_tok.shape[0]
        inv_freq = jnp.power(jnp.float32(ROPE_BASE), jnp.arange(64, dtype=F32) * (-2.0 / 128))
        angles = seq_lens.astype(F32)[:, None] * inv_freq
        cos_a, sin_a = jnp.cos(angles), jnp.sin(angles)
        cosv = jnp.concatenate([cos_a, cos_a], axis=1)
        sinv = jnp.concatenate([-sin_a, sin_a], axis=1)
        q, kn, vn = qkv(x_tok, g_attn.astype(F32)[None, :], cosv, sinv, wq, wk, wv)
        shape = (batch, 8, 16, 128)
        k_out, v_out, att = attn(seq_lens, q, kn, vn, k_blk.reshape(shape), v_blk.reshape(shape))
        y = tail(att, x_tok, g_mlp.astype(F32)[None, :], wo, wg, wu, wd)
        return y, k_out.reshape(k_blk.shape), v_out.reshape(v_blk.shape)

    return jax.shard_map(local_step, mesh=mesh, in_specs=(full_spec, full_spec, cache_spec, cache_spec, full_spec, col_spec, col_spec, col_spec, row_spec, full_spec, col_spec, col_spec, row_spec), out_specs=(full_spec, cache_spec, cache_spec), check_vma=False)
```

```python
import functools

import jax
import jax.numpy as jnp
import numpy as np
from jax import lax
from jax.experimental import pallas as pl
from jax.experimental.pallas import tpu as pltpu
from jax.sharding import PartitionSpec as P

ROPE_BASE = 500000.0
NORM_EPS = 1e-5
MESH = pl.DeviceIdType.MESH
F32 = jnp.float32
BF16 = jnp.bfloat16
ANY = pl.BlockSpec(memory_space=pl.ANY)
VMEM = pl.BlockSpec(memory_space=pltpu.VMEM)
NEG = -1e30
BLK = 256


def front_kernel(
    lens_ref, x_hbm, g_ref, cos_ref, sin_ref, wq_hbm, wk_hbm, wv_hbm, k_hbm, v_hbm, ko_hbm, vo_hbm, out_ref,
    x_buf, u_buf, w_buf, k_buf, v_buf, q_buf, kn_buf, vn_buf, xsem, wsem, kvsem, osem,
):
    rows, dim = x_buf.shape
    wide = 2 * BLK
    nq = wq_hbm.shape[1] // wide
    heads = wq_hbm.shape[1] // 128
    nreq = 32
    groups = rows // nreq
    base = lax.axis_index("sp") * 64

    x_copy = pltpu.make_async_copy(x_hbm, x_buf, xsem)
    x_copy.start()
    w_copies = [[pltpu.make_async_copy(wq_hbm.at[:, pl.ds(i * wide, wide)], w_buf.at[i], wsem.at[i])] for i in range(nq)]
    w_copies.append([
        pltpu.make_async_copy(wk_hbm, w_buf.at[nq, :, pl.ds(0, BLK)], wsem.at[nq]),
        pltpu.make_async_copy(wv_hbm, w_buf.at[nq, :, pl.ds(BLK, BLK)], wsem.at[nq + 1]),
    ])
    for cps in w_copies:
        for cp in cps:
            cp.start()

    def cache_copies(g):
        at = pl.ds(g * nreq, nreq)
        return (
            pltpu.make_async_copy(k_hbm.at[at], k_buf.at[at], kvsem.at[0, g]),
            pltpu.make_async_copy(v_hbm.at[at], v_buf.at[at], kvsem.at[1, g]),
        )

    def out_copies(g):
        at = pl.ds(g * nreq, nreq)
        return (
            pltpu.make_async_copy(k_buf.at[at], ko_hbm.at[at], osem.at[0, g]),
            pltpu.make_async_copy(v_buf.at[at], vo_hbm.at[at], osem.at[1, g]),
        )

    for g in range(groups):
        for cp in cache_copies(g):
            cp.start()
    x_copy.wait()
    gain = g_ref[...]

    def norm(i, carry):
        at = pl.ds(pl.multiple_of(i * 16, 16), 16)
        xf = x_buf[at, :].astype(F32)
        inv = lax.rsqrt(jnp.sum(xf * xf, axis=-1, keepdims=True) * (1.0 / dim) + NORM_EPS)
        u_buf[at, :] = (xf * inv * gain).astype(BF16)
        return carry

    lax.fori_loop(0, rows // 16, norm, 0)
    cosv = cos_ref[...]
    sinv = sin_ref[...]

    def rope(h):
        h = h.astype(BF16).astype(F32)
        return (h * cosv + pltpu.roll(h, 64, 1) * sinv).astype(BF16).astype(F32)

    for i in range(nq + 1):
        for cp in w_copies[i]:
            cp.wait()
        prod = jnp.dot(u_buf[...], w_buf[i], preferred_element_type=F32)
        for s in range(4):
            part = prod[:, s * 128 : (s + 1) * 128]
            if i < nq:
                q_buf[pl.ds(4 * i + s, rows, stride=heads), :] = rope(part)
            elif s < 2:
                kn_buf[pl.ds(s, rows, stride=2), :] = rope(part)
            else:
                vn_buf[pl.ds(s - 2, rows, stride=2), :] = part.astype(BF16).astype(F32)

    lane = lax.broadcasted_iota(jnp.int32, (8, 128), 1)
    head = lax.broadcasted_iota(jnp.int32, (8, 128), 0)
    match = (lane % 2) == (head // 4)
    lane_pos = jnp.where(match, lane // 2, 1 << 20)
    row16 = lax.broadcasted_iota(jnp.int32, (16, 128), 0)
    scale = 128.0**-0.5
    zero = jnp.zeros((8, 128), BF16)

    def insert(b, c_buf, n_buf, blk, off):
        row0 = jnp.broadcast_to(n_buf[pl.ds(2 * b, 1), :], (16, 128))
        row1 = jnp.broadcast_to(n_buf[pl.ds(2 * b + 1, 1), :], (16, 128))
        new = jnp.where(row16 == off, row0, row1)
        old = c_buf[b, blk].astype(F32)
        c_buf[b, blk] = jnp.where((row16 == off) | (row16 == off + 1), new, old).astype(BF16)

    def group(g, carry):
        for cp in cache_copies(g):
            cp.wait()

        def put(i, c):
            b = g * nreq + i
            pos = lens_ref[b] - base
            inside = (pos >= 0) & (pos < 64)
            at = jnp.where(inside, pos, 0)
            off = jnp.where(inside, 2 * (at % 8), -8)
            insert(b, k_buf, kn_buf, at // 8, off)
            insert(b, v_buf, vn_buf, at // 8, off)
            return c

        lax.fori_loop(0, nreq, put, 0, unroll=4)
        for cp in out_copies(g):
            cp.start()

        def step(it, c):
            stm, stl = c
            first = g * nreq + it * 16
            scores = []
            for p in range(8):
                b = first + 2 * p
                keys = k_buf[pl.ds(b, 2)].reshape(256, 128)
                qp = q_buf[pl.ds(pl.multiple_of(b * 8, 16), 16), :].astype(BF16)
                scores.append(lax.dot_general(qp, keys, (((1,), (1,)), ((), ())), preferred_element_type=F32))
            wts = []
            for p in range(8):
                for j in range(2):
                    s = scores[p][8 * j : 8 * j + 8, 128 * j : 128 * j + 128] * scale
                    valid = lane_pos <= lens_ref[first + 2 * p + j] - base
                    m = jnp.max(jnp.where(valid, s, NEG), axis=1, keepdims=True)
                    w = jnp.where(valid, jnp.exp(s - m), 0.0)
                    here = lane == it * 16 + 2 * p + j
                    stm = jnp.where(here, m, stm)
                    stl = jnp.where(here, jnp.sum(w, axis=1, keepdims=True), stl)
                    wts.append(w.astype(BF16))
            for p in range(8):
                wp = jnp.concatenate([jnp.concatenate([wts[2 * p], zero], axis=1), jnp.concatenate([zero, wts[2 * p + 1]], axis=1)], axis=0)
                vals = v_buf[pl.ds(first + 2 * p, 2)].reshape(256, 128)
                out_ref[g, pl.ds(pl.multiple_of(it * 128 + p * 16, 16), 16), :] = jnp.dot(wp, vals, preferred_element_type=F32)
            return stm, stl

        stm, stl = lax.fori_loop(0, nreq // 16, step, (jnp.zeros((8, 128), F32), jnp.ones((8, 128), F32)))
        out_ref[g, pl.ds(nreq * 8, 8), :] = stm
        out_ref[g, pl.ds(nreq * 8 + 8, 8), :] = stl
        return carry

    lax.fori_loop(0, groups, group, 0)
    for g in range(groups):
        for cp in out_copies(g):
            cp.wait()


def front(lens, x, g, cosv, sinv, wq, wk, wv, k, v):
    rows, dim = x.shape
    heads = wq.shape[1] // 128
    nblk = wq.shape[1] // (2 * BLK) + 1
    groups = rows // 32
    dma = pltpu.SemaphoreType.DMA
    return pl.pallas_call(
        front_kernel,
        out_shape=(
            jax.ShapeDtypeStruct(k.shape, BF16),
            jax.ShapeDtypeStruct(v.shape, BF16),
            jax.ShapeDtypeStruct((groups, 32 * 8 + 16, 128), F32),
        ),
        in_specs=[pl.BlockSpec(memory_space=pltpu.SMEM), ANY, VMEM, VMEM, VMEM, ANY, ANY, ANY, ANY, ANY],
        out_specs=(ANY, ANY, VMEM),
        scratch_shapes=[
            pltpu.VMEM((rows, dim), BF16),
            pltpu.VMEM((rows, dim), BF16),
            pltpu.VMEM((nblk, dim, 2 * BLK), BF16),
            pltpu.VMEM(k.shape, BF16),
            pltpu.VMEM(v.shape, BF16),
            pltpu.VMEM((rows * heads, 128), F32),
            pltpu.VMEM((rows * 2, 128), F32),
            pltpu.VMEM((rows * 2, 128), F32),
            dma,
            dma((nblk + 1,)),
            dma((2, groups)),
            dma((2, groups)),
        ],
        compiler_params=pltpu.CompilerParams(vmem_limit_bytes=63_000_000),
        cost_estimate=pl.CostEstimate(flops=4 * rows * dim * nblk * BLK, bytes_accessed=4 * dim * nblk * BLK + 8 * k.size, transcendentals=0),
        name="front",
    )(lens, x, g, cosv, sinv, wq, wk, wv, k, v)


def merge(blocks, out_ref, rows, last):
    maxs = [b[rows : rows + 8, :] for b in blocks]
    top = functools.reduce(jnp.maximum, maxs)
    facs = [jnp.exp(m - top) for m in maxs]
    tot = functools.reduce(jnp.add, [f * b[rows + 8 : rows + 16, :] for f, b in zip(facs, blocks)])
    if last:
        inv = 1.0 / tot
        facs = [f * inv for f in facs]
    else:
        out_ref[rows : rows + 8, :] = top
        out_ref[rows + 8 : rows + 16, :] = tot
    for i in range(rows // 8):
        at = slice(8 * i, 8 * i + 8)
        out_ref[at, :] = functools.reduce(jnp.add, [b[at, :] * f[:, i : i + 1] for f, b in zip(facs, blocks)])


def tail_kernel(
    att_ref, x_hbm, g_ref, wo_hbm, wg_hbm, wu_hbm, wd_hbm, y_ref,
    d1_buf, m_buf, r1_buf, o_buf, p_buf, z1_buf, h_buf, hb_buf, a_buf, p2_buf, d2_buf, s2_buf, z2_buf, yg_buf, x_buf, hid_buf,
    wo_buf, wg_buf, wu_buf, wd_buf,
    lsem, gsem, usem, dsem, d1s, d1r, r1s, r1r, z1s, z1r, hs, hr, hds, hdr, d2s, d2r, z2s, z2r, ys, yr, ydr,
):
    tp, sp = lax.axis_index("tp"), lax.axis_index("sp")
    core, chip = sp % 2, sp // 2
    cx, cy = chip % 2, chip // 2
    mate = {"tp": tp, "sp": 2 * chip + (1 - core)}
    plane = [(chip + k) % 4 for k in range(4)]
    plane_id = [{"tp": tp, "sp": 2 * q + core} for q in plane]
    zs = [(tp + k) % 4 for k in range(4)]
    z_id = [{"tp": z, "sp": sp} for z in zs]
    rows = att_ref.shape[1] - 16
    dim = x_buf.shape[1]
    ring = wg_buf.shape[0]
    half = wd_buf.shape[1]
    nff = half // BLK
    ndn = wd_buf.shape[0]
    dcol = wd_buf.shape[2]

    me8 = pl.multiple_of(32 * sp + 8 * tp, 8)
    x_copy = pltpu.make_async_copy(x_hbm.at[pl.ds(me8, 8), :], x_buf, lsem.at[0])
    wo_copy = pltpu.make_async_copy(wo_hbm, wo_buf, lsem.at[1])

    def ff_copies(j, slot):
        at = pl.ds(pl.multiple_of(core * half + j * BLK, BLK), BLK)
        return (
            pltpu.make_async_copy(wg_hbm.at[:, at], wg_buf.at[slot], gsem.at[slot]),
            pltpu.make_async_copy(wu_hbm.at[:, at], wu_buf.at[slot], usem.at[slot]),
        )

    def dn_copy(j):
        return pltpu.make_async_copy(
            wd_hbm.at[pl.ds(pl.multiple_of(core * half, BLK), half), pl.ds(pl.multiple_of(j * dcol, dcol), dcol)], wd_buf.at[j], dsem.at[j]
        )

    wo_copy.start()
    x_copy.start()
    for j in range(min(ring, nff)):
        for cp in ff_copies(j, j):
            cp.start()
    for j in range(ndn):
        dn_copy(j).start()

    bar = pltpu.get_barrier_semaphore()
    for dev in [mate] + plane_id[1:] + z_id[1:]:
        pl.semaphore_signal(bar, inc=1, device_id=dev, device_id_type=MESH)
    pl.semaphore_wait(bar, 7)

    def send(src, dst, ssem, rsem, dev):
        cp = pltpu.make_async_remote_copy(src_ref=src, dst_ref=dst, send_sem=ssem, recv_sem=rsem, device_id=dev, device_id_type=MESH)
        cp.start()
        return cp

    order = [1, 2, 3, 0]
    d1 = {k: send(att_ref.at[2 * plane[k] + (1 - core)], d1_buf.at[k], d1s.at[k], d1r.at[k], mate) for k in order}
    r1 = {}
    for k in order:
        d1[k].wait_recv()
        merge([att_ref.at[2 * plane[k] + core], d1_buf.at[k]], m_buf.at[k], rows, False)
        if k:
            r1[k] = send(m_buf.at[k], r1_buf.at[k - 1], r1s.at[k - 1], r1r.at[k - 1], plane_id[k])
    for k in (1, 2, 3):
        r1[k].wait_recv()
    merge([m_buf.at[0]] + [r1_buf.at[k] for k in range(3)], o_buf, rows, True)

    nreq = rows // 8
    o = jnp.concatenate([o_buf[pl.ds(h, nreq, stride=8), :].astype(BF16) for h in range(8)], axis=1)
    wo_copy.wait()

    def proj(j, carry):
        at = pl.ds(pl.multiple_of(j * 512, 512), 512)
        p_buf[:, at] = jnp.dot(o, wo_buf[:, at], preferred_element_type=F32)
        return carry

    lax.fori_loop(0, dim // 512, proj, 0)

    def z_scatter(src, buf, ss, rs):
        return [send(src.at[pl.ds(pl.multiple_of(8 * zs[k], 8), 8), :], buf.at[k - 1], ss.at[k - 1], rs.at[k - 1], z_id[k]) for k in (1, 2, 3)]

    own = pl.ds(pl.multiple_of(8 * tp, 8), 8)
    z1 = z_scatter(p_buf, z1_buf, z1s, z1r)
    x_copy.wait()
    for cp in z1:
        cp.wait_recv()
    hid = (x_buf[...].astype(F32) + (p_buf[own, :] + z1_buf[0] + z1_buf[1] + z1_buf[2])).astype(BF16).astype(F32)
    hid_buf[...] = hid
    inv = lax.rsqrt(jnp.sum(hid * hid, axis=-1, keepdims=True) * (1.0 / dim) + NORM_EPS)
    mine = core * 4
    h_buf[mine + tp] = (hid * inv * g_ref[...]).astype(BF16).astype(F32)

    hz = [send(h_buf.at[mine + tp], h_buf.at[mine + tp], hs.at[k - 1], hr.at[k - 1], z_id[k]) for k in (1, 2, 3)]
    hd = [send(h_buf.at[mine + tp], h_buf.at[mine + tp], hds.at[0], hdr.at[0], mate)]
    for k in (1, 2, 3):
        hz[k - 1].wait_recv()
        slot = mine + (tp + 4 - k) % 4
        hd.append(send(h_buf.at[slot], h_buf.at[slot], hds.at[k], hdr.at[k], mate))
    for cp in hd:
        cp.wait_recv()
    for i in range(4):
        hb_buf[16 * i : 16 * i + 16, :] = jnp.concatenate([h_buf[2 * i], h_buf[2 * i + 1]], axis=0).astype(BF16)

    def ff(j, carry):
        slot = lax.rem(j, ring)
        for cp in ff_copies(j, slot):
            cp.wait()
        gate = jnp.dot(hb_buf[...], wg_buf[slot], preferred_element_type=F32).astype(BF16).astype(F32)
        up = jnp.dot(hb_buf[...], wu_buf[slot], preferred_element_type=F32).astype(BF16).astype(F32)
        a_buf[:, pl.ds(pl.multiple_of(j * BLK, BLK), BLK)] = (gate * jax.nn.sigmoid(gate) * up).astype(BF16)

        @pl.when(j + ring < nff)
        def _():
            for cp in ff_copies(j + ring, slot):
                cp.start()

        return carry

    lax.fori_loop(0, nff, ff, 0)

    def down(j, carry):
        dn_copy(j).wait()
        p2_buf[:, pl.ds(pl.multiple_of(j * dcol, dcol), dcol)] = jnp.dot(a_buf[...], wd_buf[j], preferred_element_type=F32)
        return carry

    lax.fori_loop(0, ndn, down, 0)

    d2 = send(p2_buf.at[pl.ds(pl.multiple_of(32 * (1 - core), 32), 32), :], d2_buf, d2s, d2r, mate)
    d2.wait_recv()
    s2_buf[...] = p2_buf[pl.ds(pl.multiple_of(32 * core, 32), 32), :] + d2_buf[...]
    z2 = z_scatter(s2_buf, z2_buf, z2s, z2r)
    for cp in z2:
        cp.wait_recv()

    xn = 2 * cy + (1 - cx)
    yn = 2 * (1 - cy) + cx
    dg = 2 * (1 - cy) + (1 - cx)
    xn_id, yn_id = {"tp": tp, "sp": 2 * xn + core}, {"tp": tp, "sp": 2 * yn + core}

    def block(c, k):
        return yg_buf.at[4 * (2 * c + core) + (tp + k) % 4]

    started = []

    def pass_on(c, k, dev, rs):
        started.append(send(block(c, k), block(c, k), ys.at[len(started)], rs, dev))

    def landed(c, k, rs):
        pltpu.make_async_copy(block(c, k), block(c, k), rs).wait()

    yg_buf[4 * sp + tp] = (hid_buf[...] + (s2_buf[own, :] + z2_buf[0] + z2_buf[1] + z2_buf[2])).astype(BF16).astype(F32)
    for k in (1, 2, 3):
        pass_on(chip, 0, z_id[k], yr.at[(4 - k) % 4])
    pass_on(chip, 0, xn_id, yr.at[4])
    pass_on(chip, 0, yn_id, yr.at[8])
    pass_on(chip, 0, mate, ydr.at[0])

    def around(k):
        landed(xn, k, yr.at[4 + k])
        if k % 2 == 0:
            pass_on(xn, k, yn_id, yr.at[12 + k])
        pass_on(xn, k, mate, ydr.at[4 + k])
        landed(yn, k, yr.at[8 + k])
        if k % 2 == 1:
            pass_on(yn, k, xn_id, yr.at[12 + k])
        pass_on(yn, k, mate, ydr.at[8 + k])

    for k in (1, 2, 3):
        landed(chip, k, yr.at[k])
        pass_on(chip, k, xn_id, yr.at[4 + k])
        pass_on(chip, k, yn_id, yr.at[8 + k])
        pass_on(chip, k, mate, ydr.at[k])
        around(k - 1)
    around(3)
    for k in range(4):
        landed(dg, k, yr.at[12 + k])
        pass_on(dg, k, mate, ydr.at[12 + k])
    for i, c in enumerate((chip, xn, yn, dg)):
        for k in range(4):
            other = yg_buf.at[4 * (2 * c + (1 - core)) + (tp + k) % 4]
            pltpu.make_async_copy(other, other, ydr.at[4 * i + k]).wait()

    def out(i, carry):
        y_ref[pl.ds(pl.multiple_of(i * 16, 16), 16), :] = jnp.concatenate([yg_buf[2 * i], yg_buf[2 * i + 1]], axis=0).astype(BF16)
        return carry

    lax.fori_loop(0, yg_buf.shape[0] // 2, out, 0)
    for cp in list(d1.values()) + list(r1.values()) + z1 + hz + hd + [d2] + z2 + started:
        cp.wait_send()


def tail(att, x, g, wo, wg, wu, wd):
    batch, dim = x.shape
    groups, rows16, _ = att.shape
    half = wg.shape[1] // 2
    ring = min(4, half // BLK)
    ndn = 8
    dma = pltpu.SemaphoreType.DMA
    return pl.pallas_call(
        tail_kernel,
        out_shape=jax.ShapeDtypeStruct((batch, dim), BF16),
        in_specs=[VMEM, ANY, VMEM, ANY, ANY, ANY, ANY],
        out_specs=VMEM,
        scratch_shapes=[
            pltpu.VMEM((4, rows16, 128), F32),
            pltpu.VMEM((4, rows16, 128), F32),
            pltpu.VMEM((3, rows16, 128), F32),
            pltpu.VMEM((rows16 - 16, 128), F32),
            pltpu.VMEM((32, dim), F32),
            pltpu.VMEM((3, 8, dim), F32),
            pltpu.VMEM((8, 8, dim), F32),
            pltpu.VMEM((64, dim), BF16),
            pltpu.VMEM((64, half), BF16),
            pltpu.VMEM((64, dim), F32),
            pltpu.VMEM((32, dim), F32),
            pltpu.VMEM((32, dim), F32),
            pltpu.VMEM((3, 8, dim), F32),
            pltpu.VMEM((batch // 8, 8, dim), F32),
            pltpu.VMEM((8, dim), BF16),
            pltpu.VMEM((8, dim), F32),
            pltpu.VMEM(wo.shape, BF16),
            pltpu.VMEM((ring, dim, BLK), BF16),
            pltpu.VMEM((ring, dim, BLK), BF16),
            pltpu.VMEM((ndn, half, dim // ndn), BF16),
            dma((2,)), dma((ring,)), dma((ring,)), dma((ndn,)),
            dma((4,)), dma((4,)), dma((3,)), dma((3,)), dma((3,)), dma((3,)),
            dma((3,)), dma((3,)), dma((4,)), dma((4,)), dma, dma, dma((3,)), dma((3,)),
            dma((40,)), dma((16,)), dma((16,)),
        ],
        compiler_params=pltpu.CompilerParams(collective_id=0, has_side_effects=True, vmem_limit_bytes=63_000_000),
        cost_estimate=pl.CostEstimate(flops=2 * 64 * dim * half * 3, bytes_accessed=6 * dim * half, transcendentals=0),
        name="tail",
    )(att, x, g, wo, wg, wu, wd)


def solution(mesh):
    cache_spec = P(None, "sp", "tp", None)
    col_spec = P(None, "tp")
    row_spec = P("tp", None)
    full_spec = P()

    def local_step(x_tok, seq_lens, k_blk, v_blk, g_attn, wq, wk, wv, wo, g_mlp, wg, wu, wd):
        batch = x_tok.shape[0]
        freq = np.power(np.float32(ROPE_BASE), np.arange(64, dtype=np.float32) * np.float32(-2.0 / 128))
        angles = seq_lens.astype(F32)[:, None] * jnp.asarray(np.concatenate([freq, freq])[None, :], F32)
        sign = jnp.asarray(np.concatenate([-np.ones(64), np.ones(64)])[None, :], F32)
        shape = (batch, 8, 16, 128)
        k_out, v_out, att = front(seq_lens, x_tok, g_attn.astype(F32)[None, :], jnp.cos(angles), jnp.sin(angles) * sign, wq, wk, wv, k_blk.reshape(shape), v_blk.reshape(shape))
        y = tail(att, x_tok, g_mlp.astype(F32)[None, :], wo, wg, wu, wd)
        return y, k_out.reshape(k_blk.shape), v_out.reshape(v_blk.shape)

    return jax.shard_map(local_step, mesh=mesh, in_specs=(full_spec, full_spec, cache_spec, cache_spec, full_spec, col_spec, col_spec, col_spec, row_spec, full_spec, col_spec, col_spec, row_spec), out_specs=(full_spec, cache_spec, cache_spec), check_vma=False)
```

```python
import functools

import jax
import jax.numpy as jnp
import numpy as np
from jax import lax
from jax.experimental import pallas as pl
from jax.experimental.pallas import tpu as pltpu
from jax.sharding import PartitionSpec as P

ROPE_BASE = 500000.0
NORM_EPS = 1e-5
MESH = pl.DeviceIdType.MESH
F32 = jnp.float32
BF16 = jnp.bfloat16
ANY = pl.BlockSpec(memory_space=pl.ANY)
VMEM = pl.BlockSpec(memory_space=pltpu.VMEM)
NEG = -1e30
BLK = 256
PART = 144


def front_kernel(
    lens_ref, x_hbm, g_hbm, tab_hbm, wq_hbm, wk_hbm, wv_hbm, k_hbm, v_hbm, ko_hbm, vo_hbm, out_hbm,
    x_buf, g_buf, tab_buf, rot_buf, u_buf, w_buf, k_buf, v_buf, q_buf, kn_buf, vn_buf, out_buf, xsem, wsem, kvsem, osem,
):
    rows, dim = x_buf.shape
    wide = 2 * BLK
    nq = wq_hbm.shape[1] // wide
    heads = wq_hbm.shape[1] // 128
    nreq = 32
    groups = rows // nreq
    base = lax.axis_index("sp") * 64

    x_copy = pltpu.make_async_copy(x_hbm, x_buf, xsem.at[0])
    g_copy = pltpu.make_async_copy(g_hbm, g_buf, xsem.at[1])
    tab_copy = pltpu.make_async_copy(tab_hbm, tab_buf, xsem.at[2])
    g_copy.start()
    x_copy.start()
    tab_copy.start()
    w_copies = [[pltpu.make_async_copy(wq_hbm.at[:, pl.ds(i * wide, wide)], w_buf.at[i], wsem.at[i])] for i in range(nq)]
    w_copies.append([
        pltpu.make_async_copy(wk_hbm, w_buf.at[nq, :, pl.ds(0, BLK)], wsem.at[nq]),
        pltpu.make_async_copy(wv_hbm, w_buf.at[nq, :, pl.ds(BLK, BLK)], wsem.at[nq + 1]),
    ])
    for cps in w_copies:
        for cp in cps:
            cp.start()

    def cache_copies(g):
        at = pl.ds(g * nreq, nreq)
        return (
            pltpu.make_async_copy(k_hbm.at[at], k_buf.at[at], kvsem.at[0, g]),
            pltpu.make_async_copy(v_hbm.at[at], v_buf.at[at], kvsem.at[1, g]),
        )

    def out_copies(g):
        at = pl.ds(g * nreq, nreq)
        return (
            pltpu.make_async_copy(k_buf.at[at], ko_hbm.at[at], osem.at[0, g]),
            pltpu.make_async_copy(v_buf.at[at], vo_hbm.at[at], osem.at[1, g]),
        )

    def part_copy(g):
        return pltpu.make_async_copy(out_buf.at[pl.ds(2 * g, 2)], out_hbm.at[pl.ds(2 * g, 2)], osem.at[2, g])

    for g in range(groups):
        for cp in cache_copies(g):
            cp.start()
    g_copy.wait()
    gain = g_buf[...].astype(F32).reshape(1, dim)
    x_copy.wait()

    def norm(i, carry):
        at = pl.ds(pl.multiple_of(i * 16, 16), 16)
        xf = x_buf[at, :].astype(F32)
        inv = lax.rsqrt(jnp.sum(xf * xf, axis=-1, keepdims=True) * (1.0 / dim) + NORM_EPS)
        u_buf[at, :] = (xf * inv * gain).astype(BF16)
        return carry

    lax.fori_loop(0, rows // 16, norm, 0, unroll=2)
    tab_copy.wait()

    def angle(i, carry):
        rot_buf[pl.ds(i, 1), :] = tab_buf[pl.ds(lens_ref[i], 1), :]
        return carry

    lax.fori_loop(0, rows, angle, 0, unroll=16)
    cosv = rot_buf[:, :128]
    sinv = rot_buf[:, 128:]

    def rope(h):
        h = h.astype(BF16).astype(F32)
        return (h * cosv + pltpu.roll(h, 64, 1) * sinv).astype(BF16).astype(F32)

    for i in range(nq + 1):
        for cp in w_copies[i]:
            cp.wait()
        prod = jnp.dot(u_buf[...], w_buf[i], preferred_element_type=F32)
        for s in range(4):
            part = prod[:, s * 128 : (s + 1) * 128]
            if i < nq:
                q_buf[pl.ds(4 * i + s, rows, stride=heads), :] = rope(part)
            elif s < 2:
                kn_buf[pl.ds(s, rows, stride=2), :] = rope(part)
            else:
                vn_buf[pl.ds(s - 2, rows, stride=2), :] = part.astype(BF16).astype(F32)

    lane = lax.broadcasted_iota(jnp.int32, (8, 128), 1)
    head = lax.broadcasted_iota(jnp.int32, (8, 128), 0)
    match = (lane % 2) == (head // 4)
    lane_pos = jnp.where(match, lane // 2, 1 << 20)
    row16 = lax.broadcasted_iota(jnp.int32, (16, 128), 0)
    scale = 128.0**-0.5
    zero = jnp.zeros((8, 128), BF16)

    def insert(b, c_buf, n_buf, blk, off):
        row0 = jnp.broadcast_to(n_buf[pl.ds(2 * b, 1), :], (16, 128))
        row1 = jnp.broadcast_to(n_buf[pl.ds(2 * b + 1, 1), :], (16, 128))
        new = jnp.where(row16 == off, row0, row1)
        old = c_buf[b, blk].astype(F32)
        c_buf[b, blk] = jnp.where((row16 == off) | (row16 == off + 1), new, old).astype(BF16)

    def group(g, carry):
        for cp in cache_copies(g):
            cp.wait()

        def put(i, c):
            b = g * nreq + i
            pos = lens_ref[b] - base
            inside = (pos >= 0) & (pos < 64)
            at = jnp.where(inside, pos, 0)
            off = jnp.where(inside, 2 * (at % 8), -8)
            insert(b, k_buf, kn_buf, at // 8, off)
            insert(b, v_buf, vn_buf, at // 8, off)
            return c

        lax.fori_loop(0, nreq, put, 0, unroll=8)
        for cp in out_copies(g):
            cp.start()

        first = g * nreq
        scores = []
        for p in range(16):
            b = first + 2 * p
            keys = k_buf[pl.ds(b, 2)].reshape(256, 128)
            qp = q_buf[pl.ds(pl.multiple_of(b * 8, 16), 16), :].astype(BF16)
            scores.append(lax.dot_general(qp, keys, (((1,), (1,)), ((), ())), preferred_element_type=F32))
        for h in range(2):
            half = g * 2 + h
            wts = []
            stm, stl = jnp.zeros((8, 128), F32), jnp.ones((8, 128), F32)
            for p in range(8):
                for j in range(2):
                    s = scores[8 * h + p][8 * j : 8 * j + 8, 128 * j : 128 * j + 128] * scale
                    valid = lane_pos <= lens_ref[first + 16 * h + 2 * p + j] - base
                    m = jnp.max(jnp.where(valid, s, NEG), axis=1, keepdims=True)
                    w = jnp.where(valid, jnp.exp(s - m), 0.0)
                    here = lane == 2 * p + j
                    stm = jnp.where(here, m, stm)
                    stl = jnp.where(here, jnp.sum(w, axis=1, keepdims=True), stl)
                    wts.append(w.astype(BF16))
            out_buf[half, 128:136, :] = stm
            out_buf[half, 136:144, :] = stl
            for p in range(8):
                wp = jnp.concatenate([jnp.concatenate([wts[2 * p], zero], axis=1), jnp.concatenate([zero, wts[2 * p + 1]], axis=1)], axis=0)
                vals = v_buf[pl.ds(first + 16 * h + 2 * p, 2)].reshape(256, 128)
                out_buf[half, 16 * p : 16 * p + 16, :] = jnp.dot(wp, vals, preferred_element_type=F32)
        part_copy(g).start()
        return carry

    lax.fori_loop(0, groups, group, 0)
    for g in range(groups):
        for cp in out_copies(g):
            cp.wait()
        part_copy(g).wait()


def front(lens, x, g, tab, wq, wk, wv, k, v):
    rows, dim = x.shape
    heads = wq.shape[1] // 128
    nblk = wq.shape[1] // (2 * BLK) + 1
    groups = rows // 32
    dma = pltpu.SemaphoreType.DMA
    return pl.pallas_call(
        front_kernel,
        out_shape=(
            jax.ShapeDtypeStruct(k.shape, BF16),
            jax.ShapeDtypeStruct(v.shape, BF16),
            jax.ShapeDtypeStruct((2 * groups, PART, 128), F32),
        ),
        in_specs=[pl.BlockSpec(memory_space=pltpu.SMEM)] + [ANY] * 8,
        out_specs=(ANY, ANY, ANY),
        scratch_shapes=[
            pltpu.VMEM((rows, dim), BF16),
            pltpu.VMEM((dim,), BF16),
            pltpu.VMEM(tab.shape, F32),
            pltpu.VMEM((rows, 256), F32),
            pltpu.VMEM((rows, dim), BF16),
            pltpu.VMEM((nblk, dim, 2 * BLK), BF16),
            pltpu.VMEM(k.shape, BF16),
            pltpu.VMEM(v.shape, BF16),
            pltpu.VMEM((rows * heads, 128), F32),
            pltpu.VMEM((rows * 2, 128), F32),
            pltpu.VMEM((rows * 2, 128), F32),
            pltpu.VMEM((2 * groups, PART, 128), F32),
            dma((3,)),
            dma((nblk + 1,)),
            dma((2, groups)),
            dma((3, groups)),
        ],
        compiler_params=pltpu.CompilerParams(vmem_limit_bytes=63_000_000),
        cost_estimate=pl.CostEstimate(flops=4 * rows * dim * nblk * BLK, bytes_accessed=4 * dim * nblk * BLK + 8 * k.size, transcendentals=0),
        name="front",
    )(lens, x, g, tab, wq, wk, wv, k, v)


def merge(blocks, out_ref, last):
    rows = PART - 16
    maxs = [b[rows : rows + 8, :] for b in blocks]
    top = functools.reduce(jnp.maximum, maxs)
    facs = [jnp.exp(m - top) for m in maxs]
    tot = functools.reduce(jnp.add, [f * b[rows + 8 : rows + 16, :] for f, b in zip(facs, blocks)])
    if last:
        inv = 1.0 / tot
        facs = [f * inv for f in facs]
    else:
        out_ref[rows : rows + 8, :] = top
        out_ref[rows + 8 : rows + 16, :] = tot
    for i in range(rows // 8):
        at = slice(8 * i, 8 * i + 8)
        out_ref[at, :] = functools.reduce(jnp.add, [b[at, :] * f[:, i : i + 1] for f, b in zip(facs, blocks)])


def tail_kernel(
    att_ref, x_hbm, g_ref, wo_hbm, wg_hbm, wu_hbm, wd_hbm, y_ref,
    d1_buf, m_buf, r1_buf, o_buf, p_buf, z1_buf, h_buf, hb_buf, a_buf, p2_buf, d2_buf, s2_buf, z2_buf, yg_buf, x_buf, hid_buf,
    wo_buf, wg_buf, wu_buf, wd_buf,
    lsem, gsem, usem, dsem, d1s, d1r, r1s, r1r, z1s, z1r, hs, hr, hds, hdr, d2s, d2r, z2s, z2r, ys, yr, ydr,
):
    tp, sp = lax.axis_index("tp"), lax.axis_index("sp")
    core, chip = sp % 2, sp // 2
    cx, cy = chip % 2, chip // 2
    mate = {"tp": tp, "sp": 2 * chip + (1 - core)}
    plane = [(chip + k) % 4 for k in range(4)]
    plane_id = [{"tp": tp, "sp": 2 * q + core} for q in plane]
    zs = [(tp + k) % 4 for k in range(4)]
    z_id = [{"tp": z, "sp": sp} for z in zs]
    dim = x_buf.shape[1]
    ring = wg_buf.shape[0]
    half = wd_buf.shape[1]
    nff = half // BLK
    ndn = wd_buf.shape[0]
    dcol = wd_buf.shape[2]

    me8 = pl.multiple_of(32 * sp + 8 * tp, 8)
    x_copy = pltpu.make_async_copy(x_hbm.at[pl.ds(me8, 8), :], x_buf, lsem.at[0])
    wo_copy = pltpu.make_async_copy(wo_hbm, wo_buf, lsem.at[1])

    def ff_copies(j, slot):
        at = pl.ds(pl.multiple_of(core * half + j * BLK, BLK), BLK)
        return (
            pltpu.make_async_copy(wg_hbm.at[:, at], wg_buf.at[slot], gsem.at[slot]),
            pltpu.make_async_copy(wu_hbm.at[:, at], wu_buf.at[slot], usem.at[slot]),
        )

    def dn_copy(j):
        return pltpu.make_async_copy(
            wd_hbm.at[pl.ds(pl.multiple_of(core * half, BLK), half), pl.ds(pl.multiple_of(j * dcol, dcol), dcol)], wd_buf.at[j], dsem.at[j]
        )

    wo_copy.start()
    x_copy.start()
    for j in range(min(ring, nff)):
        for cp in ff_copies(j, j):
            cp.start()
    for j in range(ndn):
        dn_copy(j).start()

    bar = pltpu.get_barrier_semaphore()
    for dev in [mate] + plane_id[1:] + z_id[1:]:
        pl.semaphore_signal(bar, inc=1, device_id=dev, device_id_type=MESH)
    pl.semaphore_wait(bar, 7)

    def send(src, dst, ssem, rsem, dev):
        cp = pltpu.make_async_remote_copy(src_ref=src, dst_ref=dst, send_sem=ssem, recv_sem=rsem, device_id=dev, device_id_type=MESH)
        cp.start()
        return cp

    order = [1, 2, 3, 0]
    d1 = {k: send(att_ref.at[pl.ds(4 * plane[k] + 2 * (1 - core), 2)], d1_buf.at[k], d1s.at[k], d1r.at[k], mate) for k in order}
    r1 = {}
    for k in order:
        d1[k].wait_recv()
        for h in range(2):
            merge([att_ref.at[4 * plane[k] + 2 * core + h], d1_buf.at[k, h]], m_buf.at[k, h], False)
        if k:
            r1[k] = send(m_buf.at[k], r1_buf.at[k - 1], r1s.at[k - 1], r1r.at[k - 1], plane_id[k])
    for k in (1, 2, 3):
        r1[k].wait_recv()
    for h in range(2):
        merge([m_buf.at[0, h]] + [r1_buf.at[k, h] for k in range(3)], o_buf.at[pl.ds(128 * h, 128)], True)

    o = jnp.concatenate([o_buf[pl.ds(h, 32, stride=8), :].astype(BF16) for h in range(8)], axis=1)
    wo_copy.wait()

    def proj(j, carry):
        at = pl.ds(pl.multiple_of(j * 512, 512), 512)
        p_buf[:, at] = jnp.dot(o, wo_buf[:, at], preferred_element_type=F32)
        return carry

    lax.fori_loop(0, dim // 512, proj, 0)

    def z_scatter(src, buf, ss, rs):
        return [send(src.at[pl.ds(pl.multiple_of(8 * zs[k], 8), 8), :], buf.at[k - 1], ss.at[k - 1], rs.at[k - 1], z_id[k]) for k in (1, 2, 3)]

    own = pl.ds(pl.multiple_of(8 * tp, 8), 8)
    z1 = z_scatter(p_buf, z1_buf, z1s, z1r)
    x_copy.wait()
    for cp in z1:
        cp.wait_recv()
    hid = (x_buf[...].astype(F32) + (p_buf[own, :] + z1_buf[0] + z1_buf[1] + z1_buf[2])).astype(BF16).astype(F32)
    hid_buf[...] = hid
    inv = lax.rsqrt(jnp.sum(hid * hid, axis=-1, keepdims=True) * (1.0 / dim) + NORM_EPS)
    mine = core * 4
    h_buf[mine + tp] = (hid * inv * g_ref[...].astype(F32).reshape(1, dim)).astype(BF16).astype(F32)

    hz = [send(h_buf.at[mine + tp], h_buf.at[mine + tp], hs.at[k - 1], hr.at[k - 1], z_id[k]) for k in (1, 2, 3)]
    hd = [send(h_buf.at[mine + tp], h_buf.at[mine + tp], hds.at[0], hdr.at[0], mate)]
    for k in (1, 2, 3):
        hz[k - 1].wait_recv()
        slot = mine + (tp + 4 - k) % 4
        hd.append(send(h_buf.at[slot], h_buf.at[slot], hds.at[k], hdr.at[k], mate))
    for cp in hd:
        cp.wait_recv()
    for i in range(4):
        hb_buf[16 * i : 16 * i + 16, :] = jnp.concatenate([h_buf[2 * i], h_buf[2 * i + 1]], axis=0).astype(BF16)

    def ff(j, carry):
        slot = lax.rem(j, ring)
        for cp in ff_copies(j, slot):
            cp.wait()
        gate = jnp.dot(hb_buf[...], wg_buf[slot], preferred_element_type=F32).astype(BF16).astype(F32)
        up = jnp.dot(hb_buf[...], wu_buf[slot], preferred_element_type=F32).astype(BF16).astype(F32)
        a_buf[:, pl.ds(pl.multiple_of(j * BLK, BLK), BLK)] = (gate * jax.nn.sigmoid(gate) * up).astype(BF16)

        @pl.when(j + ring < nff)
        def _():
            for cp in ff_copies(j + ring, slot):
                cp.start()

        return carry

    lax.fori_loop(0, nff, ff, 0)

    def down(j, carry):
        dn_copy(j).wait()
        p2_buf[:, pl.ds(pl.multiple_of(j * dcol, dcol), dcol)] = jnp.dot(a_buf[...], wd_buf[j], preferred_element_type=F32)
        return carry

    lax.fori_loop(0, ndn, down, 0)

    d2 = send(p2_buf.at[pl.ds(pl.multiple_of(32 * (1 - core), 32), 32), :], d2_buf, d2s, d2r, mate)
    d2.wait_recv()
    s2_buf[...] = p2_buf[pl.ds(pl.multiple_of(32 * core, 32), 32), :] + d2_buf[...]
    z2 = z_scatter(s2_buf, z2_buf, z2s, z2r)
    for cp in z2:
        cp.wait_recv()

    xn = 2 * cy + (1 - cx)
    yn = 2 * (1 - cy) + cx
    dg = 2 * (1 - cy) + (1 - cx)
    xn_id, yn_id = {"tp": tp, "sp": 2 * xn + core}, {"tp": tp, "sp": 2 * yn + core}

    def block(c, k):
        return yg_buf.at[4 * (2 * c + core) + (tp + k) % 4]

    started = []

    def pass_on(c, k, dev, rs):
        started.append(send(block(c, k), block(c, k), ys.at[len(started)], rs, dev))

    def landed(c, k, rs):
        pltpu.make_async_copy(block(c, k), block(c, k), rs).wait()

    yg_buf[4 * sp + tp] = (hid_buf[...] + (s2_buf[own, :] + z2_buf[0] + z2_buf[1] + z2_buf[2])).astype(BF16).astype(F32)
    for k in (1, 2, 3):
        pass_on(chip, 0, z_id[k], yr.at[(4 - k) % 4])
    pass_on(chip, 0, xn_id, yr.at[4])
    pass_on(chip, 0, yn_id, yr.at[8])
    pass_on(chip, 0, mate, ydr.at[0])

    def around(k):
        landed(xn, k, yr.at[4 + k])
        if k % 2 == 0:
            pass_on(xn, k, yn_id, yr.at[12 + k])
        pass_on(xn, k, mate, ydr.at[4 + k])
        landed(yn, k, yr.at[8 + k])
        if k % 2 == 1:
            pass_on(yn, k, xn_id, yr.at[12 + k])
        pass_on(yn, k, mate, ydr.at[8 + k])

    for k in (1, 2, 3):
        landed(chip, k, yr.at[k])
        pass_on(chip, k, xn_id, yr.at[4 + k])
        pass_on(chip, k, yn_id, yr.at[8 + k])
        pass_on(chip, k, mate, ydr.at[k])
        around(k - 1)
    around(3)
    for k in range(4):
        landed(dg, k, yr.at[12 + k])
        pass_on(dg, k, mate, ydr.at[12 + k])
    for i, c in enumerate((chip, xn, yn, dg)):
        for k in range(4):
            other = yg_buf.at[4 * (2 * c + (1 - core)) + (tp + k) % 4]
            pltpu.make_async_copy(other, other, ydr.at[4 * i + k]).wait()

    def out(i, carry):
        y_ref[pl.ds(pl.multiple_of(i * 16, 16), 16), :] = jnp.concatenate([yg_buf[2 * i], yg_buf[2 * i + 1]], axis=0).astype(BF16)
        return carry

    lax.fori_loop(0, yg_buf.shape[0] // 2, out, 0)
    for cp in list(d1.values()) + list(r1.values()) + z1 + hz + hd + [d2] + z2 + started:
        cp.wait_send()


def tail(att, x, g, wo, wg, wu, wd):
    batch, dim = x.shape
    half = wg.shape[1] // 2
    ring = min(4, half // BLK)
    ndn = 8
    dma = pltpu.SemaphoreType.DMA
    return pl.pallas_call(
        tail_kernel,
        out_shape=jax.ShapeDtypeStruct((batch, dim), BF16),
        in_specs=[VMEM, ANY, VMEM, ANY, ANY, ANY, ANY],
        out_specs=VMEM,
        scratch_shapes=[
            pltpu.VMEM((4, 2, PART, 128), F32),
            pltpu.VMEM((4, 2, PART, 128), F32),
            pltpu.VMEM((3, 2, PART, 128), F32),
            pltpu.VMEM((256, 128), F32),
            pltpu.VMEM((32, dim), F32),
            pltpu.VMEM((3, 8, dim), F32),
            pltpu.VMEM((8, 8, dim), F32),
            pltpu.VMEM((64, dim), BF16),
            pltpu.VMEM((64, half), BF16),
            pltpu.VMEM((64, dim), F32),
            pltpu.VMEM((32, dim), F32),
            pltpu.VMEM((32, dim), F32),
            pltpu.VMEM((3, 8, dim), F32),
            pltpu.VMEM((batch // 8, 8, dim), F32),
            pltpu.VMEM((8, dim), BF16),
            pltpu.VMEM((8, dim), F32),
            pltpu.VMEM(wo.shape, BF16),
            pltpu.VMEM((ring, dim, BLK), BF16),
            pltpu.VMEM((ring, dim, BLK), BF16),
            pltpu.VMEM((ndn, half, dim // ndn), BF16),
            dma((2,)), dma((ring,)), dma((ring,)), dma((ndn,)),
            dma((4,)), dma((4,)), dma((3,)), dma((3,)), dma((3,)), dma((3,)),
            dma((3,)), dma((3,)), dma((4,)), dma((4,)), dma, dma, dma((3,)), dma((3,)),
            dma((40,)), dma((16,)), dma((16,)),
        ],
        compiler_params=pltpu.CompilerParams(collective_id=0, has_side_effects=True, vmem_limit_bytes=63_000_000),
        cost_estimate=pl.CostEstimate(flops=2 * 64 * dim * half * 3, bytes_accessed=6 * dim * half, transcendentals=0),
        name="tail",
    )(att, x, g, wo, wg, wu, wd)


def rope_table(length):
    freq = np.power(ROPE_BASE, np.arange(64) * (-2.0 / 128)).astype(np.float32)
    angles = (np.arange(length, dtype=np.float32)[:, None] * freq).astype(np.float64)
    cos, sin = np.cos(angles), np.sin(angles)
    return jnp.asarray(np.concatenate([cos, cos, -sin, sin], axis=1), F32)


def solution(mesh):
    cache_spec = P(None, "sp", "tp", None)
    col_spec = P(None, "tp")
    row_spec = P("tp", None)
    full_spec = P()

    def local_step(x_tok, seq_lens, k_blk, v_blk, g_attn, wq, wk, wv, wo, g_mlp, wg, wu, wd):
        batch = x_tok.shape[0]
        shape = (batch, 8, 16, 128)
        k_out, v_out, att = front(seq_lens, x_tok, g_attn, rope_table(k_blk.shape[1] * mesh.shape["sp"]), wq, wk, wv, k_blk.reshape(shape), v_blk.reshape(shape))
        y = tail(att, x_tok, g_mlp, wo, wg, wu, wd)
        return y, k_out.reshape(k_blk.shape), v_out.reshape(v_blk.shape)

    return jax.shard_map(local_step, mesh=mesh, in_specs=(full_spec, full_spec, cache_spec, cache_spec, full_spec, col_spec, col_spec, col_spec, row_spec, full_spec, col_spec, col_spec, row_spec), out_specs=(full_spec, cache_spec, cache_spec), check_vma=False)
```

```python
import functools

import jax
import jax.numpy as jnp
import numpy as np
from jax import lax
from jax.experimental import pallas as pl
from jax.experimental.pallas import tpu as pltpu
from jax.sharding import PartitionSpec as P

ROPE_BASE = 500000.0
NORM_EPS = 1e-5
MESH = pl.DeviceIdType.MESH
F32 = jnp.float32
BF16 = jnp.bfloat16
ANY = pl.BlockSpec(memory_space=pl.ANY)
VMEM = pl.BlockSpec(memory_space=pltpu.VMEM)
NEG = -1e30
BLK = 256
CHUNKS = 4
PART = 144


def front_kernel(
    lens_ref, x_hbm, g_hbm, tab_hbm, wq_hbm, wk_hbm, wv_hbm, k_hbm, v_hbm, ko_hbm, vo_hbm, out_hbm,
    x_buf, g_buf, tab_buf, rot_buf, u_buf, w_buf, k_buf, v_buf, q_buf, kn_buf, vn_buf, out_buf, xsem, wsem, kvsem, osem,
):
    rows, dim = x_buf.shape
    wide = 2 * BLK
    nq = wq_hbm.shape[1] // wide
    heads = wq_hbm.shape[1] // 128
    nreq = 32
    groups = rows // nreq
    base = lax.axis_index("sp") * 64

    x_copy = pltpu.make_async_copy(x_hbm, x_buf, xsem.at[0])
    g_copy = pltpu.make_async_copy(g_hbm, g_buf, xsem.at[1])
    tab_copy = pltpu.make_async_copy(tab_hbm, tab_buf, xsem.at[2])
    g_copy.start()
    x_copy.start()
    tab_copy.start()
    w_copies = [[pltpu.make_async_copy(wq_hbm.at[:, pl.ds(i * wide, wide)], w_buf.at[i], wsem.at[i])] for i in range(nq)]
    w_copies.append([
        pltpu.make_async_copy(wk_hbm, w_buf.at[nq, :, pl.ds(0, BLK)], wsem.at[nq]),
        pltpu.make_async_copy(wv_hbm, w_buf.at[nq, :, pl.ds(BLK, BLK)], wsem.at[nq + 1]),
    ])
    for cps in w_copies:
        for cp in cps:
            cp.start()

    def cache_copies(g):
        at = pl.ds(g * nreq, nreq)
        return (
            pltpu.make_async_copy(k_hbm.at[at], k_buf.at[at], kvsem.at[0, g]),
            pltpu.make_async_copy(v_hbm.at[at], v_buf.at[at], kvsem.at[1, g]),
        )

    def out_copies(g):
        at = pl.ds(g * nreq, nreq)
        return (
            pltpu.make_async_copy(k_buf.at[at], ko_hbm.at[at], osem.at[0, g]),
            pltpu.make_async_copy(v_buf.at[at], vo_hbm.at[at], osem.at[1, g]),
        )

    def part_copy(g):
        return pltpu.make_async_copy(out_buf.at[pl.ds(2 * g, 2)], out_hbm.at[pl.ds(2 * g, 2)], osem.at[2, g])

    for g in range(groups):
        for cp in cache_copies(g):
            cp.start()
    g_copy.wait()
    gain = g_buf[...].astype(F32).reshape(1, dim)
    x_copy.wait()

    def norm(i, carry):
        at = pl.ds(pl.multiple_of(i * 16, 16), 16)
        xf = x_buf[at, :].astype(F32)
        inv = lax.rsqrt(jnp.sum(xf * xf, axis=-1, keepdims=True) * (1.0 / dim) + NORM_EPS)
        u_buf[at, :] = (xf * inv * gain).astype(BF16)
        return carry

    lax.fori_loop(0, rows // 16, norm, 0, unroll=2)
    tab_copy.wait()

    def angle(i, carry):
        rot_buf[pl.ds(i, 1), :] = tab_buf[pl.ds(lens_ref[i], 1), :]
        return carry

    lax.fori_loop(0, rows, angle, 0, unroll=16)
    cosv = rot_buf[:, :128]
    sinv = rot_buf[:, 128:]

    def rope(h):
        h = h.astype(BF16).astype(F32)
        return (h * cosv + pltpu.roll(h, 64, 1) * sinv).astype(BF16).astype(F32)

    for i in range(nq + 1):
        for cp in w_copies[i]:
            cp.wait()
        prod = jnp.dot(u_buf[...], w_buf[i], preferred_element_type=F32)
        for s in range(4):
            part = prod[:, s * 128 : (s + 1) * 128]
            if i < nq:
                q_buf[pl.ds(4 * i + s, rows, stride=heads), :] = rope(part)
            elif s < 2:
                kn_buf[pl.ds(s, rows, stride=2), :] = rope(part)
            else:
                vn_buf[pl.ds(s - 2, rows, stride=2), :] = part.astype(BF16).astype(F32)

    lane = lax.broadcasted_iota(jnp.int32, (8, 128), 1)
    head = lax.broadcasted_iota(jnp.int32, (8, 128), 0)
    match = (lane % 2) == (head // 4)
    lane_pos = jnp.where(match, lane // 2, 1 << 20)
    row16 = lax.broadcasted_iota(jnp.int32, (16, 128), 0)
    scale = 128.0**-0.5
    zero = jnp.zeros((8, 128), BF16)

    def insert(b, c_buf, n_buf, blk, off):
        row0 = jnp.broadcast_to(n_buf[pl.ds(2 * b, 1), :], (16, 128))
        row1 = jnp.broadcast_to(n_buf[pl.ds(2 * b + 1, 1), :], (16, 128))
        new = jnp.where(row16 == off, row0, row1)
        old = c_buf[b, blk].astype(F32)
        c_buf[b, blk] = jnp.where((row16 == off) | (row16 == off + 1), new, old).astype(BF16)

    def group(g, carry):
        for cp in cache_copies(g):
            cp.wait()

        def put(i, c):
            b = g * nreq + i
            pos = lens_ref[b] - base
            inside = (pos >= 0) & (pos < 64)
            at = jnp.where(inside, pos, 0)
            off = jnp.where(inside, 2 * (at % 8), -8)
            insert(b, k_buf, kn_buf, at // 8, off)
            insert(b, v_buf, vn_buf, at // 8, off)
            return c

        lax.fori_loop(0, nreq, put, 0, unroll=8)
        for cp in out_copies(g):
            cp.start()

        first = g * nreq
        scores = []
        for p in range(16):
            b = first + 2 * p
            keys = k_buf[pl.ds(b, 2)].reshape(256, 128)
            qp = q_buf[pl.ds(pl.multiple_of(b * 8, 16), 16), :].astype(BF16)
            scores.append(lax.dot_general(qp, keys, (((1,), (1,)), ((), ())), preferred_element_type=F32))
        for h in range(2):
            half = g * 2 + h
            wts = []
            stm, stl = jnp.zeros((8, 128), F32), jnp.ones((8, 128), F32)
            for p in range(8):
                for j in range(2):
                    s = scores[8 * h + p][8 * j : 8 * j + 8, 128 * j : 128 * j + 128] * scale
                    valid = lane_pos <= lens_ref[first + 16 * h + 2 * p + j] - base
                    m = jnp.max(jnp.where(valid, s, NEG), axis=1, keepdims=True)
                    w = jnp.where(valid, jnp.exp(s - m), 0.0)
                    here = lane == 2 * p + j
                    stm = jnp.where(here, m, stm)
                    stl = jnp.where(here, jnp.sum(w, axis=1, keepdims=True), stl)
                    wts.append(w.astype(BF16))
            out_buf[half, 128:136, :] = stm
            out_buf[half, 136:144, :] = stl
            for p in range(8):
                wp = jnp.concatenate([jnp.concatenate([wts[2 * p], zero], axis=1), jnp.concatenate([zero, wts[2 * p + 1]], axis=1)], axis=0)
                vals = v_buf[pl.ds(first + 16 * h + 2 * p, 2)].reshape(256, 128)
                out_buf[half, 16 * p : 16 * p + 16, :] = jnp.dot(wp, vals, preferred_element_type=F32)
        part_copy(g).start()
        return carry

    lax.fori_loop(0, groups, group, 0)
    for g in range(groups):
        for cp in out_copies(g):
            cp.wait()
        part_copy(g).wait()


def front(lens, x, g, tab, wq, wk, wv, k, v):
    rows, dim = x.shape
    heads = wq.shape[1] // 128
    nblk = wq.shape[1] // (2 * BLK) + 1
    groups = rows // 32
    dma = pltpu.SemaphoreType.DMA
    return pl.pallas_call(
        front_kernel,
        out_shape=(
            jax.ShapeDtypeStruct(k.shape, BF16),
            jax.ShapeDtypeStruct(v.shape, BF16),
            jax.ShapeDtypeStruct((2 * groups, PART, 128), F32),
        ),
        in_specs=[pl.BlockSpec(memory_space=pltpu.SMEM)] + [ANY] * 8,
        out_specs=(ANY, ANY, ANY),
        scratch_shapes=[
            pltpu.VMEM((rows, dim), BF16),
            pltpu.VMEM((dim,), BF16),
            pltpu.VMEM(tab.shape, F32),
            pltpu.VMEM((rows, 256), F32),
            pltpu.VMEM((rows, dim), BF16),
            pltpu.VMEM((nblk, dim, 2 * BLK), BF16),
            pltpu.VMEM(k.shape, BF16),
            pltpu.VMEM(v.shape, BF16),
            pltpu.VMEM((rows * heads, 128), F32),
            pltpu.VMEM((rows * 2, 128), F32),
            pltpu.VMEM((rows * 2, 128), F32),
            pltpu.VMEM((2 * groups, PART, 128), F32),
            dma((3,)),
            dma((nblk + 1,)),
            dma((2, groups)),
            dma((3, groups)),
        ],
        compiler_params=pltpu.CompilerParams(vmem_limit_bytes=63_000_000),
        cost_estimate=pl.CostEstimate(flops=4 * rows * dim * nblk * BLK, bytes_accessed=4 * dim * nblk * BLK + 8 * k.size, transcendentals=0),
        name="front",
    )(lens, x, g, tab, wq, wk, wv, k, v)


def merge(blocks, out_ref, last):
    rows = PART - 16
    maxs = [b[rows : rows + 8, :] for b in blocks]
    top = functools.reduce(jnp.maximum, maxs)
    facs = [jnp.exp(m - top) for m in maxs]
    tot = functools.reduce(jnp.add, [f * b[rows + 8 : rows + 16, :] for f, b in zip(facs, blocks)])
    if last:
        inv = 1.0 / tot
        facs = [f * inv for f in facs]
    else:
        out_ref[rows : rows + 8, :] = top
        out_ref[rows + 8 : rows + 16, :] = tot
    for i in range(rows // 8):
        at = slice(8 * i, 8 * i + 8)
        out_ref[at, :] = functools.reduce(jnp.add, [b[at, :] * f[:, i : i + 1] for f, b in zip(facs, blocks)])


def tail_kernel(
    att_ref, x_hbm, g_ref, wo_hbm, wg_hbm, wu_hbm, wd_hbm, y_hbm,
    d1_buf, m_buf, r1_buf, o_buf, p_buf, z1_buf, a1_buf, h_buf, hb_buf, a_buf, p2_buf, d2_buf, s2_buf, z2_buf, a2_buf, yg_buf, yo_buf, x_buf, hid_buf,
    wo_buf, wg_buf, wu_buf, wd_buf,
    lsem, gsem, usem, dsem, osem, d1s, d1r, r1s, r1r, z1s, z1r, hs, hr, hds, hdr, d2s, d2r, z2s, z2r, ys, yr, ydr,
):
    tp, sp = lax.axis_index("tp"), lax.axis_index("sp")
    core, chip = sp % 2, sp // 2
    cx, cy = chip % 2, chip // 2
    mate = {"tp": tp, "sp": 2 * chip + (1 - core)}
    plane = [(chip + k) % 4 for k in range(4)]
    plane_id = [{"tp": tp, "sp": 2 * q + core} for q in plane]
    side = tp // 2
    inside = tp * (1 - 2 * side) + 3 * side
    is_end, is_in = inside == 0, inside == 1

    def place(m):
        return m + side * (3 - 2 * m)

    near, second, far = place(1 - inside), place(2), place(3)

    def zdev(z):
        return {"tp": z, "sp": sp}

    dim = x_buf.shape[1]
    ring = wg_buf.shape[0]
    half = wd_buf.shape[1]
    nff = half // BLK
    ndn = wd_buf.shape[0]
    dcol = wd_buf.shape[2]

    me8 = pl.multiple_of(32 * sp + 8 * tp, 8)
    x_copy = pltpu.make_async_copy(x_hbm.at[pl.ds(me8, 8), :], x_buf, lsem.at[0])
    wo_copy = pltpu.make_async_copy(wo_hbm, wo_buf, lsem.at[1])

    def ff_copies(j, slot):
        at = pl.ds(pl.multiple_of(core * half + j * BLK, BLK), BLK)
        return (
            pltpu.make_async_copy(wg_hbm.at[:, at], wg_buf.at[slot], gsem.at[slot]),
            pltpu.make_async_copy(wu_hbm.at[:, at], wu_buf.at[slot], usem.at[slot]),
        )

    def dn_copy(j):
        return pltpu.make_async_copy(
            wd_hbm.at[pl.ds(pl.multiple_of(core * half, BLK), half), pl.ds(pl.multiple_of(j * dcol, dcol), dcol)], wd_buf.at[j], dsem.at[j]
        )

    wo_copy.start()
    x_copy.start()
    for j in range(min(ring, nff)):
        for cp in ff_copies(j, j):
            cp.start()
    for j in range(ndn):
        dn_copy(j).start()

    @pl.when(is_end)
    def _():
        z1_buf[2] = jnp.zeros_like(z1_buf[2])
        z2_buf[2] = jnp.zeros_like(z2_buf[2])

    bar = pltpu.get_barrier_semaphore()
    for dev in [mate] + plane_id[1:] + [zdev((tp + k) % 4) for k in (1, 2, 3)]:
        pl.semaphore_signal(bar, inc=1, device_id=dev, device_id_type=MESH)
    pl.semaphore_wait(bar, 7)

    drains = []

    def send(src, dst, ssem, rsem, dev, cond=None):
        def make():
            return pltpu.make_async_remote_copy(src_ref=src, dst_ref=dst, send_sem=ssem, recv_sem=rsem, device_id=dev, device_id_type=MESH)

        def go():
            make().start()

        def done():
            make().wait_send()

        if cond is None:
            go()
            drains.append(done)
        else:
            pl.when(cond)(go)
            drains.append(lambda: pl.when(cond)(done))

    def landed(ref, rsem):
        pltpu.make_async_copy(ref, ref, rsem).wait()

    order = [1, 2, 3, 0]
    for k in order:
        send(att_ref.at[pl.ds(4 * plane[k] + 2 * (1 - core), 2)], d1_buf.at[k], d1s.at[k], d1r.at[k], mate)
    for k in order:
        landed(d1_buf.at[k], d1r.at[k])
        for h in range(2):
            merge([att_ref.at[4 * plane[k] + 2 * core + h], d1_buf.at[k, h]], m_buf.at[k, h], False)
        if k:
            send(m_buf.at[k], r1_buf.at[k - 1], r1s.at[k - 1], r1r.at[k - 1], plane_id[k])
    for k in (1, 2, 3):
        landed(r1_buf.at[k - 1], r1r.at[k - 1])
    for h in range(2):
        merge([m_buf.at[0, h]] + [r1_buf.at[k, h] for k in range(3)], o_buf.at[pl.ds(128 * h, 128)], True)

    def rows8(z):
        return pl.ds(pl.multiple_of(8 * z, 8), 8)

    def scatter(j, cols, src, buf, agg, ss, rs):
        send(src.at[rows8(second), cols], buf.at[2 - inside, :, cols], ss.at[j, 0], rs.at[j, 2 - inside], zdev(second))
        send(src.at[rows8(far), cols], agg.at[:, cols], ss.at[j, 1], rs.at[j, 3], zdev(near), is_end)
        send(src.at[rows8(near), cols], buf.at[0, :, cols], ss.at[j, 2], rs.at[j, 0], zdev(near))

    def relay(j, cols, src, buf, agg, ss, rs):
        @pl.when(is_in)
        def _():
            landed(agg.at[:, cols], rs.at[j, 3])
            src[rows8(far), cols] = src[rows8(far), cols] + agg[:, cols]

        send(src.at[rows8(far), cols], buf.at[1, :, cols], ss.at[j, 1], rs.at[j, 1], zdev(far), is_in)

    def gathered(j, cols, src, buf, rs):
        landed(buf.at[0, :, cols], rs.at[j, 0])
        landed(buf.at[1, :, cols], rs.at[j, 1])

        @pl.when(is_in)
        def _():
            landed(buf.at[2, :, cols], rs.at[j, 2])

        return src[rows8(tp), cols] + buf[0, :, cols] + buf[1, :, cols] + buf[2, :, cols]

    o = jnp.concatenate([o_buf[pl.ds(h, 32, stride=8), :].astype(BF16) for h in range(8)], axis=1)
    wo_copy.wait()

    def proj(j, carry):
        at = pl.ds(pl.multiple_of(j * 512, 512), 512)
        p_buf[:, at] = jnp.dot(o, wo_buf[:, at], preferred_element_type=F32)
        return carry

    parts1 = [pl.ds(i * (dim // 2), dim // 2) for i in range(2)]
    for i in range(2):
        lax.fori_loop(i * (dim // 1024), (i + 1) * (dim // 1024), proj, 0)
        scatter(i, parts1[i], p_buf, z1_buf, a1_buf, z1s, z1r)
    for i in range(2):
        relay(i, parts1[i], p_buf, z1_buf, a1_buf, z1s, z1r)
    x_copy.wait()
    for i in range(2):
        hid_buf[:, parts1[i]] = (x_buf[:, parts1[i]].astype(F32) + gathered(i, parts1[i], p_buf, z1_buf, z1r)).astype(BF16).astype(F32)
    hid = hid_buf[...]
    inv = lax.rsqrt(jnp.sum(hid * hid, axis=-1, keepdims=True) * (1.0 / dim) + NORM_EPS)
    mine = core * 4
    h_buf[mine + tp] = (hid * inv * g_ref[...].astype(F32).reshape(1, dim)).astype(BF16).astype(F32)

    def spread(block, ss, rs, first):
        send(block(tp), block(tp), ss(first), rs(tp), zdev(second))
        send(block(tp), block(tp), ss(first + 1), rs(tp), zdev(far), is_in)
        send(block(tp), block(tp), ss(first + 2), rs(tp), zdev(near))

    def h_block(z):
        return h_buf.at[mine + z]

    spread(h_block, lambda i: hs.at[i], lambda z: hr.at[z], 0)
    send(h_block(tp), h_block(tp), hds.at[0], hdr.at[tp], mate)
    for i, z in enumerate((near, second, far)):
        landed(h_block(z), hr.at[z])
        if i == 2:
            send(h_block(z), h_block(z), hs.at[3], hr.at[z], zdev(near), is_in)
        send(h_block(z), h_block(z), hds.at[1 + i], hdr.at[z], mate)
    for z in range(4):
        landed(h_buf.at[4 * (1 - core) + z], hdr.at[z])
    for i in range(4):
        hb_buf[16 * i : 16 * i + 16, :] = jnp.concatenate([h_buf[2 * i], h_buf[2 * i + 1]], axis=0).astype(BF16)

    def ff(j, carry):
        slot = lax.rem(j, ring)
        for cp in ff_copies(j, slot):
            cp.wait()
        gate = jnp.dot(hb_buf[...], wg_buf[slot], preferred_element_type=F32).astype(BF16).astype(F32)
        up = jnp.dot(hb_buf[...], wu_buf[slot], preferred_element_type=F32).astype(BF16).astype(F32)
        a_buf[:, pl.ds(pl.multiple_of(j * BLK, BLK), BLK)] = (gate * jax.nn.sigmoid(gate) * up).astype(BF16)

        @pl.when(j + ring < nff)
        def _():
            for cp in ff_copies(j + ring, slot):
                cp.start()

        return carry

    lax.fori_loop(0, nff, ff, 0)

    nc = CHUNKS
    width = dim // nc
    cols = [pl.ds(j * width, width) for j in range(nc)]
    xn = 2 * cy + (1 - cx)
    yn = 2 * (1 - cy) + cx
    dg = 2 * (1 - cy) + (1 - cx)
    xn_id, yn_id = {"tp": tp, "sp": 2 * xn + core}, {"tp": tp, "sp": 2 * yn + core}
    zorder = (tp, near, second, far)
    count = [0] * nc

    def block(j, c, z):
        return yg_buf.at[4 * (2 * c + core) + z, :, cols[j]]

    def pass_on(j, c, z, dev, rs, cond=None):
        send(block(j, c, z), block(j, c, z), ys.at[j, count[j]], rs, dev, cond)
        count[j] += 1

    def down(j):
        def one(i, carry):
            dn_copy(i).wait()
            p2_buf[:, pl.ds(pl.multiple_of(i * dcol, dcol), dcol)] = jnp.dot(a_buf[...], wd_buf[i], preferred_element_type=F32)
            return carry

        lax.fori_loop(j * ndn // nc, (j + 1) * ndn // nc, one, 0)
        send(p2_buf.at[pl.ds(pl.multiple_of(32 * (1 - core), 32), 32), cols[j]], d2_buf.at[:, cols[j]], d2s.at[j], d2r.at[j], mate)

    def pair(j):
        landed(d2_buf.at[:, cols[j]], d2r.at[j])
        s2_buf[:, cols[j]] = p2_buf[pl.ds(pl.multiple_of(32 * core, 32), 32), cols[j]] + d2_buf[:, cols[j]]
        scatter(j, cols[j], s2_buf, z2_buf, a2_buf, z2s, z2r)

    def mid(j):
        relay(j, cols[j], s2_buf, z2_buf, a2_buf, z2s, z2r)

    def own(j):
        yg_buf[4 * sp + tp, :, cols[j]] = (hid_buf[:, cols[j]] + gathered(j, cols[j], s2_buf, z2_buf, z2r)).astype(BF16).astype(F32)
        pass_on(j, chip, tp, xn_id, yr.at[j, 4 + tp])
        pass_on(j, chip, tp, yn_id, yr.at[j, 8 + tp])
        at = count[j]
        spread(lambda z: block(j, chip, z), lambda i: ys.at[j, i], lambda z: yr.at[j, z], at)
        count[j] = at + 3
        pass_on(j, chip, tp, mate, ydr.at[j, tp])

    def column(j):
        for i, z in enumerate(zorder[1:]):
            landed(block(j, chip, z), yr.at[j, z])
            if i == 2:
                pass_on(j, chip, z, zdev(near), yr.at[j, z], is_in)
            pass_on(j, chip, z, xn_id, yr.at[j, 4 + z])
            pass_on(j, chip, z, yn_id, yr.at[j, 8 + z])
            pass_on(j, chip, z, mate, ydr.at[j, z])

    def around(j):
        for i, z in enumerate(zorder):
            landed(block(j, xn, z), yr.at[j, 4 + z])
            if i % 2 == 0:
                pass_on(j, xn, z, yn_id, yr.at[j, 12 + z])
            pass_on(j, xn, z, mate, ydr.at[j, 4 + z])
            landed(block(j, yn, z), yr.at[j, 8 + z])
            if i % 2 == 1:
                pass_on(j, yn, z, xn_id, yr.at[j, 12 + z])
            pass_on(j, yn, z, mate, ydr.at[j, 8 + z])

    def across(j):
        for z in zorder:
            landed(block(j, dg, z), yr.at[j, 12 + z])
            pass_on(j, dg, z, mate, ydr.at[j, 12 + z])

    def out_copy(j):
        return pltpu.make_async_copy(yo_buf.at[:, cols[j]], y_hbm.at[:, cols[j]], osem.at[j])

    def finish(j):
        for i, c in enumerate((chip, xn, yn, dg)):
            for z in zorder:
                landed(yg_buf.at[4 * (2 * c + (1 - core)) + z, :, cols[j]], ydr.at[j, 4 * i + z])

        def out(i, carry):
            yo_buf[pl.ds(pl.multiple_of(i * 16, 16), 16), cols[j]] = jnp.concatenate([yg_buf[2 * i, :, cols[j]], yg_buf[2 * i + 1, :, cols[j]]], axis=0).astype(BF16)
            return carry

        lax.fori_loop(0, yg_buf.shape[0] // 2, out, 0)
        out_copy(j).start()

    def run(stages, steps):
        for t in range(steps):
            for lag, stage in stages:
                if 0 <= t - lag < nc:
                    stage(t - lag)

    run([(0, down), (1, pair), (2, mid)], nc + 2)
    run([(0, own), (1, column), (2, around), (3, across), (4, finish)], nc + 4)
    for done in drains:
        done()
    for j in range(nc):
        out_copy(j).wait()


def tail(att, x, g, wo, wg, wu, wd):
    batch, dim = x.shape
    half = wg.shape[1] // 2
    ring = min(4, half // BLK)
    ndn = 8
    dma = pltpu.SemaphoreType.DMA
    return pl.pallas_call(
        tail_kernel,
        out_shape=jax.ShapeDtypeStruct((batch, dim), BF16),
        in_specs=[VMEM, ANY, VMEM, ANY, ANY, ANY, ANY],
        out_specs=ANY,
        scratch_shapes=[
            pltpu.VMEM((4, 2, PART, 128), F32),
            pltpu.VMEM((4, 2, PART, 128), F32),
            pltpu.VMEM((3, 2, PART, 128), F32),
            pltpu.VMEM((256, 128), F32),
            pltpu.VMEM((32, dim), F32),
            pltpu.VMEM((3, 8, dim), F32),
            pltpu.VMEM((8, dim), F32),
            pltpu.VMEM((8, 8, dim), F32),
            pltpu.VMEM((64, dim), BF16),
            pltpu.VMEM((64, half), BF16),
            pltpu.VMEM((64, dim), F32),
            pltpu.VMEM((32, dim), F32),
            pltpu.VMEM((32, dim), F32),
            pltpu.VMEM((3, 8, dim), F32),
            pltpu.VMEM((8, dim), F32),
            pltpu.VMEM((batch // 8, 8, dim), F32),
            pltpu.VMEM((batch, dim), BF16),
            pltpu.VMEM((8, dim), BF16),
            pltpu.VMEM((8, dim), F32),
            pltpu.VMEM(wo.shape, BF16),
            pltpu.VMEM((ring, dim, BLK), BF16),
            pltpu.VMEM((ring, dim, BLK), BF16),
            pltpu.VMEM((ndn, half, dim // ndn), BF16),
            dma((2,)), dma((ring,)), dma((ring,)), dma((ndn,)), dma((CHUNKS,)),
            dma((4,)), dma((4,)), dma((3,)), dma((3,)), dma((2, 3)), dma((2, 4)),
            dma((4,)), dma((4,)), dma((4,)), dma((4,)), dma((CHUNKS,)), dma((CHUNKS,)), dma((CHUNKS, 3)), dma((CHUNKS, 4)),
            dma((CHUNKS, 34)), dma((CHUNKS, 16)), dma((CHUNKS, 16)),
        ],
        compiler_params=pltpu.CompilerParams(collective_id=0, has_side_effects=True, vmem_limit_bytes=63_000_000),
        cost_estimate=pl.CostEstimate(flops=2 * 64 * dim * half * 3, bytes_accessed=6 * dim * half, transcendentals=0),
        name="tail",
    )(att, x, g, wo, wg, wu, wd)


def rope_table(length):
    freq = np.power(ROPE_BASE, np.arange(64) * (-2.0 / 128)).astype(np.float32)
    angles = (np.arange(length, dtype=np.float32)[:, None] * freq).astype(np.float64)
    cos, sin = np.cos(angles), np.sin(angles)
    return jnp.asarray(np.concatenate([cos, cos, -sin, sin], axis=1), F32)


def solution(mesh):
    cache_spec = P(None, "sp", "tp", None)
    col_spec = P(None, "tp")
    row_spec = P("tp", None)
    full_spec = P()

    def local_step(x_tok, seq_lens, k_blk, v_blk, g_attn, wq, wk, wv, wo, g_mlp, wg, wu, wd):
        batch = x_tok.shape[0]
        shape = (batch, 8, 16, 128)
        k_out, v_out, att = front(seq_lens, x_tok, g_attn, rope_table(k_blk.shape[1] * mesh.shape["sp"]), wq, wk, wv, k_blk.reshape(shape), v_blk.reshape(shape))
        y = tail(att, x_tok, g_mlp, wo, wg, wu, wd)
        return y, k_out.reshape(k_blk.shape), v_out.reshape(v_blk.shape)

    return jax.shard_map(local_step, mesh=mesh, in_specs=(full_spec, full_spec, cache_spec, cache_spec, full_spec, col_spec, col_spec, col_spec, row_spec, full_spec, col_spec, col_spec, row_spec), out_specs=(full_spec, cache_spec, cache_spec), check_vma=False)
```

```python
import functools

import jax
import jax.numpy as jnp
import numpy as np
from jax import lax
from jax.experimental import pallas as pl
from jax.experimental.pallas import tpu as pltpu
from jax.sharding import PartitionSpec as P

ROPE_BASE = 500000.0
NORM_EPS = 1e-5
MESH = pl.DeviceIdType.MESH
F32 = jnp.float32
BF16 = jnp.bfloat16
ANY = pl.BlockSpec(memory_space=pl.ANY)
VMEM = pl.BlockSpec(memory_space=pltpu.VMEM)
NEG = -1e30
BLK = 256
CHUNKS = 4
PART = 144


def front_kernel(
    lens_ref, x_hbm, g_hbm, tab_hbm, wq_hbm, wk_hbm, wv_hbm, k_hbm, v_hbm, ko_hbm, vo_hbm, out_hbm,
    x_buf, g_buf, tab_buf, rot_buf, u_buf, w_buf, k_buf, v_buf, q_buf, kn_buf, vn_buf, out_buf, xsem, wsem, kvsem, osem,
):
    rows, dim = x_buf.shape
    wide = 2 * BLK
    nq = wq_hbm.shape[1] // wide
    heads = wq_hbm.shape[1] // 128
    nreq = 32
    groups = rows // nreq
    base = lax.axis_index("sp") * 64

    x_copy = pltpu.make_async_copy(x_hbm, x_buf, xsem.at[0])
    g_copy = pltpu.make_async_copy(g_hbm, g_buf, xsem.at[1])
    tab_copy = pltpu.make_async_copy(tab_hbm, tab_buf, xsem.at[2])
    g_copy.start()
    x_copy.start()
    tab_copy.start()
    w_copies = [[pltpu.make_async_copy(wq_hbm.at[:, pl.ds(i * wide, wide)], w_buf.at[i], wsem.at[i])] for i in range(nq)]
    w_copies.append([
        pltpu.make_async_copy(wk_hbm, w_buf.at[nq, :, pl.ds(0, BLK)], wsem.at[nq]),
        pltpu.make_async_copy(wv_hbm, w_buf.at[nq, :, pl.ds(BLK, BLK)], wsem.at[nq + 1]),
    ])
    for cps in w_copies:
        for cp in cps:
            cp.start()

    def cache_copies(g):
        at = pl.ds(g * nreq, nreq)
        return (
            pltpu.make_async_copy(k_hbm.at[at], k_buf.at[at], kvsem.at[0, g]),
            pltpu.make_async_copy(v_hbm.at[at], v_buf.at[at], kvsem.at[1, g]),
        )

    def out_copies(g):
        at = pl.ds(g * nreq, nreq)
        return (
            pltpu.make_async_copy(k_buf.at[at], ko_hbm.at[at], osem.at[0, g]),
            pltpu.make_async_copy(v_buf.at[at], vo_hbm.at[at], osem.at[1, g]),
        )

    def part_copy(g):
        return pltpu.make_async_copy(out_buf.at[pl.ds(2 * g, 2)], out_hbm.at[pl.ds(2 * g, 2)], osem.at[2, g])

    for g in range(groups):
        for cp in cache_copies(g):
            cp.start()
    g_copy.wait()
    gain = g_buf[...].astype(F32).reshape(1, dim)
    x_copy.wait()

    def norm(i, carry):
        at = pl.ds(pl.multiple_of(i * 16, 16), 16)
        xf = x_buf[at, :].astype(F32)
        inv = lax.rsqrt(jnp.sum(xf * xf, axis=-1, keepdims=True) * (1.0 / dim) + NORM_EPS)
        u_buf[at, :] = (xf * inv * gain).astype(BF16)
        return carry

    lax.fori_loop(0, rows // 16, norm, 0, unroll=2)
    tab_copy.wait()

    def angle(i, carry):
        rot_buf[pl.ds(i, 1), :] = tab_buf[pl.ds(lens_ref[i], 1), :]
        return carry

    lax.fori_loop(0, rows, angle, 0, unroll=16)
    cosv = rot_buf[:, :128]
    sinv = rot_buf[:, 128:]

    def rope(h):
        h = h.astype(BF16).astype(F32)
        return (h * cosv + pltpu.roll(h, 64, 1) * sinv).astype(BF16).astype(F32)

    for i in range(nq + 1):
        for cp in w_copies[i]:
            cp.wait()
        prod = jnp.dot(u_buf[...], w_buf[i], preferred_element_type=F32)
        for s in range(4):
            part = prod[:, s * 128 : (s + 1) * 128]
            if i < nq:
                q_buf[pl.ds(4 * i + s, rows, stride=heads), :] = rope(part)
            elif s < 2:
                kn_buf[pl.ds(s, rows, stride=2), :] = rope(part)
            else:
                vn_buf[pl.ds(s - 2, rows, stride=2), :] = part.astype(BF16).astype(F32)

    lane = lax.broadcasted_iota(jnp.int32, (8, 128), 1)
    head = lax.broadcasted_iota(jnp.int32, (8, 128), 0)
    match = (lane % 2) == (head // 4)
    lane_pos = jnp.where(match, lane // 2, 1 << 20)
    row16 = lax.broadcasted_iota(jnp.int32, (16, 128), 0)
    scale = 128.0**-0.5
    zero = jnp.zeros((8, 128), BF16)

    def insert(b, c_buf, n_buf, blk, off):
        row0 = jnp.broadcast_to(n_buf[pl.ds(2 * b, 1), :], (16, 128))
        row1 = jnp.broadcast_to(n_buf[pl.ds(2 * b + 1, 1), :], (16, 128))
        new = jnp.where(row16 == off, row0, row1)
        old = c_buf[b, blk].astype(F32)
        c_buf[b, blk] = jnp.where((row16 == off) | (row16 == off + 1), new, old).astype(BF16)

    def group(g, carry):
        for cp in cache_copies(g):
            cp.wait()

        def put(i, c):
            b = g * nreq + i
            pos = lens_ref[b] - base
            inside = (pos >= 0) & (pos < 64)
            at = jnp.where(inside, pos, 0)
            off = jnp.where(inside, 2 * (at % 8), -8)
            insert(b, k_buf, kn_buf, at // 8, off)
            insert(b, v_buf, vn_buf, at // 8, off)
            return c

        lax.fori_loop(0, nreq, put, 0, unroll=8)
        for cp in out_copies(g):
            cp.start()

        first = g * nreq
        scores = []
        for p in range(16):
            b = first + 2 * p
            keys = k_buf[pl.ds(b, 2)].reshape(256, 128)
            qp = q_buf[pl.ds(pl.multiple_of(b * 8, 16), 16), :].astype(BF16)
            scores.append(lax.dot_general(qp, keys, (((1,), (1,)), ((), ())), preferred_element_type=F32))
        for h in range(2):
            half = g * 2 + h
            wts = []
            stm, stl = jnp.zeros((8, 128), F32), jnp.ones((8, 128), F32)
            for p in range(8):
                for j in range(2):
                    s = scores[8 * h + p][8 * j : 8 * j + 8, 128 * j : 128 * j + 128] * scale
                    valid = lane_pos <= lens_ref[first + 16 * h + 2 * p + j] - base
                    m = jnp.max(jnp.where(valid, s, NEG), axis=1, keepdims=True)
                    w = jnp.where(valid, jnp.exp(s - m), 0.0)
                    here = lane == 2 * p + j
                    stm = jnp.where(here, m, stm)
                    stl = jnp.where(here, jnp.sum(w, axis=1, keepdims=True), stl)
                    wts.append(w.astype(BF16))
            out_buf[half, 128:136, :] = stm
            out_buf[half, 136:144, :] = stl
            for p in range(8):
                wp = jnp.concatenate([jnp.concatenate([wts[2 * p], zero], axis=1), jnp.concatenate([zero, wts[2 * p + 1]], axis=1)], axis=0)
                vals = v_buf[pl.ds(first + 16 * h + 2 * p, 2)].reshape(256, 128)
                out_buf[half, 16 * p : 16 * p + 16, :] = jnp.dot(wp, vals, preferred_element_type=F32)
        part_copy(g).start()
        return carry

    lax.fori_loop(0, groups, group, 0)
    for g in range(groups):
        for cp in out_copies(g):
            cp.wait()
        part_copy(g).wait()


def front(lens, x, g, tab, wq, wk, wv, k, v):
    rows, dim = x.shape
    heads = wq.shape[1] // 128
    nblk = wq.shape[1] // (2 * BLK) + 1
    groups = rows // 32
    dma = pltpu.SemaphoreType.DMA
    return pl.pallas_call(
        front_kernel,
        out_shape=(
            jax.ShapeDtypeStruct(k.shape, BF16),
            jax.ShapeDtypeStruct(v.shape, BF16),
            jax.ShapeDtypeStruct((2 * groups, PART, 128), F32),
        ),
        in_specs=[pl.BlockSpec(memory_space=pltpu.SMEM)] + [ANY] * 8,
        out_specs=(ANY, ANY, ANY),
        scratch_shapes=[
            pltpu.VMEM((rows, dim), BF16),
            pltpu.VMEM((dim,), BF16),
            pltpu.VMEM(tab.shape, F32),
            pltpu.VMEM((rows, 256), F32),
            pltpu.VMEM((rows, dim), BF16),
            pltpu.VMEM((nblk, dim, 2 * BLK), BF16),
            pltpu.VMEM(k.shape, BF16),
            pltpu.VMEM(v.shape, BF16),
            pltpu.VMEM((rows * heads, 128), F32),
            pltpu.VMEM((rows * 2, 128), F32),
            pltpu.VMEM((rows * 2, 128), F32),
            pltpu.VMEM((2 * groups, PART, 128), F32),
            dma((3,)),
            dma((nblk + 1,)),
            dma((2, groups)),
            dma((3, groups)),
        ],
        compiler_params=pltpu.CompilerParams(vmem_limit_bytes=63_000_000),
        cost_estimate=pl.CostEstimate(flops=4 * rows * dim * nblk * BLK, bytes_accessed=4 * dim * nblk * BLK + 8 * k.size, transcendentals=0),
        name="front",
    )(lens, x, g, tab, wq, wk, wv, k, v)


def merge(blocks, out_ref, last):
    rows = PART - 16
    maxs = [b[rows : rows + 8, :] for b in blocks]
    top = functools.reduce(jnp.maximum, maxs)
    facs = [jnp.exp(m - top) for m in maxs]
    tot = functools.reduce(jnp.add, [f * b[rows + 8 : rows + 16, :] for f, b in zip(facs, blocks)])
    if last:
        inv = 1.0 / tot
        facs = [f * inv for f in facs]
    else:
        out_ref[rows : rows + 8, :] = top
        out_ref[rows + 8 : rows + 16, :] = tot
    for i in range(rows // 8):
        at = slice(8 * i, 8 * i + 8)
        out_ref[at, :] = functools.reduce(jnp.add, [b[at, :] * f[:, i : i + 1] for f, b in zip(facs, blocks)])


def tail_kernel(
    att_hbm, x_hbm, g_hbm, wo_hbm, wg_hbm, wu_hbm, wd_hbm, y_hbm,
    att_ref, g_ref, d1_buf, m_buf, r1_buf, o_buf, p_buf, z1_buf, a1_buf, h_buf, hb_buf, a_buf, p2_buf, d2_buf, s2_buf, z2_buf, a2_buf, yg_buf, yo_buf, x_buf, hid_buf,
    wo_buf, wg_buf, wu_buf, wd_buf,
    lsem, gsem, usem, dsem, osem, d1s, d1r, r1s, r1r, z1s, z1r, hs, hr, hds, hdr, d2s, d2r, z2s, z2r, ys, yr, ydr,
):
    tp, sp = lax.axis_index("tp"), lax.axis_index("sp")
    core, chip = sp % 2, sp // 2
    cx, cy = chip % 2, chip // 2
    mate = {"tp": tp, "sp": 2 * chip + (1 - core)}
    plane = [(chip + k) % 4 for k in range(4)]
    plane_id = [{"tp": tp, "sp": 2 * q + core} for q in plane]
    side = tp // 2
    inside = tp * (1 - 2 * side) + 3 * side
    is_end, is_in = inside == 0, inside == 1

    def place(m):
        return m + side * (3 - 2 * m)

    near, second, far = place(1 - inside), place(2), place(3)

    def zdev(z):
        return {"tp": z, "sp": sp}

    dim = x_buf.shape[1]
    ring = wg_buf.shape[0]
    half = wd_buf.shape[1]
    nff = half // BLK
    ndn = wd_buf.shape[0]
    dcol = wd_buf.shape[2]

    me8 = pl.multiple_of(32 * sp + 8 * tp, 8)
    x_copy = pltpu.make_async_copy(x_hbm.at[pl.ds(me8, 8), :], x_buf, lsem.at[0])
    wo_copy = pltpu.make_async_copy(wo_hbm, wo_buf, lsem.at[1])

    def ff_copies(j, slot):
        at = pl.ds(pl.multiple_of(core * half + j * BLK, BLK), BLK)
        return (
            pltpu.make_async_copy(wg_hbm.at[:, at], wg_buf.at[slot], gsem.at[slot]),
            pltpu.make_async_copy(wu_hbm.at[:, at], wu_buf.at[slot], usem.at[slot]),
        )

    def dn_copy(j):
        return pltpu.make_async_copy(
            wd_hbm.at[pl.ds(pl.multiple_of(core * half, BLK), half), pl.ds(pl.multiple_of(j * dcol, dcol), dcol)], wd_buf.at[j], dsem.at[j]
        )

    att_copy = pltpu.make_async_copy(att_hbm, att_ref, lsem.at[2])
    g_copy = pltpu.make_async_copy(g_hbm, g_ref, lsem.at[3])
    att_copy.start()
    x_copy.start()
    g_copy.start()
    wo_copy.start()

    def prefetch_ff(lo, hi):
        for j in range(lo, min(hi, ring, nff)):
            for cp in ff_copies(j, j):
                cp.start()

    @pl.when(is_end)
    def _():
        z1_buf[2] = jnp.zeros_like(z1_buf[2])
        z2_buf[2] = jnp.zeros_like(z2_buf[2])

    bar = pltpu.get_barrier_semaphore()
    for dev in [mate] + plane_id[1:] + [zdev((tp + k) % 4) for k in (1, 2, 3)]:
        pl.semaphore_signal(bar, inc=1, device_id=dev, device_id_type=MESH)
    pl.semaphore_wait(bar, 7)

    drains = []

    def send(src, dst, ssem, rsem, dev, cond=None):
        def make():
            return pltpu.make_async_remote_copy(src_ref=src, dst_ref=dst, send_sem=ssem, recv_sem=rsem, device_id=dev, device_id_type=MESH)

        def go():
            make().start()

        def done():
            make().wait_send()

        if cond is None:
            go()
            drains.append(done)
        else:
            pl.when(cond)(go)
            drains.append(lambda: pl.when(cond)(done))

    def landed(ref, rsem):
        pltpu.make_async_copy(ref, ref, rsem).wait()

    order = [1, 2, 3, 0]
    att_copy.wait()
    for k in order:
        send(att_ref.at[pl.ds(4 * plane[k] + 2 * (1 - core), 2)], d1_buf.at[k], d1s.at[k], d1r.at[k], mate)
    for k in order:
        landed(d1_buf.at[k], d1r.at[k])
        for h in range(2):
            merge([att_ref.at[4 * plane[k] + 2 * core + h], d1_buf.at[k, h]], m_buf.at[k, h], False)
        if k:
            send(m_buf.at[k], r1_buf.at[k - 1], r1s.at[k - 1], r1r.at[k - 1], plane_id[k])
    prefetch_ff(0, 2)
    for k in (1, 2, 3):
        landed(r1_buf.at[k - 1], r1r.at[k - 1])
    for h in range(2):
        merge([m_buf.at[0, h]] + [r1_buf.at[k, h] for k in range(3)], o_buf.at[pl.ds(128 * h, 128)], True)

    def rows8(z):
        return pl.ds(pl.multiple_of(8 * z, 8), 8)

    def scatter(j, cols, src, buf, agg, ss, rs):
        send(src.at[rows8(second), cols], buf.at[2 - inside, :, cols], ss.at[j, 0], rs.at[j, 2 - inside], zdev(second))
        send(src.at[rows8(far), cols], agg.at[:, cols], ss.at[j, 1], rs.at[j, 3], zdev(near), is_end)
        send(src.at[rows8(near), cols], buf.at[0, :, cols], ss.at[j, 2], rs.at[j, 0], zdev(near))

    def relay(j, cols, src, buf, agg, ss, rs):
        @pl.when(is_in)
        def _():
            landed(agg.at[:, cols], rs.at[j, 3])
            src[rows8(far), cols] = src[rows8(far), cols] + agg[:, cols]

        send(src.at[rows8(far), cols], buf.at[1, :, cols], ss.at[j, 1], rs.at[j, 1], zdev(far), is_in)

    def gathered(j, cols, src, buf, rs):
        landed(buf.at[0, :, cols], rs.at[j, 0])
        landed(buf.at[1, :, cols], rs.at[j, 1])

        @pl.when(is_in)
        def _():
            landed(buf.at[2, :, cols], rs.at[j, 2])

        return src[rows8(tp), cols] + buf[0, :, cols] + buf[1, :, cols] + buf[2, :, cols]

    o = jnp.concatenate([o_buf[pl.ds(h, 32, stride=8), :].astype(BF16) for h in range(8)], axis=1)
    wo_copy.wait()

    def proj(j, carry):
        at = pl.ds(pl.multiple_of(j * 512, 512), 512)
        p_buf[:, at] = jnp.dot(o, wo_buf[:, at], preferred_element_type=F32)
        return carry

    parts1 = [pl.ds(i * (dim // 2), dim // 2) for i in range(2)]
    for i in range(2):
        lax.fori_loop(i * (dim // 1024), (i + 1) * (dim // 1024), proj, 0)
        scatter(i, parts1[i], p_buf, z1_buf, a1_buf, z1s, z1r)
    prefetch_ff(2, ring)
    for i in range(2):
        relay(i, parts1[i], p_buf, z1_buf, a1_buf, z1s, z1r)
    for j in range(ndn // 2):
        dn_copy(j).start()
    x_copy.wait()
    g_copy.wait()
    for i in range(2):
        hid_buf[:, parts1[i]] = (x_buf[:, parts1[i]].astype(F32) + gathered(i, parts1[i], p_buf, z1_buf, z1r)).astype(BF16).astype(F32)
    hid = hid_buf[...]
    inv = lax.rsqrt(jnp.sum(hid * hid, axis=-1, keepdims=True) * (1.0 / dim) + NORM_EPS)
    mine = core * 4
    h_buf[mine + tp] = (hid * inv * g_ref[...].astype(F32).reshape(1, dim)).astype(BF16).astype(F32)

    def spread(block, ss, rs, first):
        send(block(tp), block(tp), ss(first), rs(tp), zdev(second))
        send(block(tp), block(tp), ss(first + 1), rs(tp), zdev(far), is_in)
        send(block(tp), block(tp), ss(first + 2), rs(tp), zdev(near))

    def h_block(z):
        return h_buf.at[mine + z]

    spread(h_block, lambda i: hs.at[i], lambda z: hr.at[z], 0)
    send(h_block(tp), h_block(tp), hds.at[0], hdr.at[tp], mate)
    for j in range(ndn // 2, ndn):
        dn_copy(j).start()
    for i, z in enumerate((near, second, far)):
        landed(h_block(z), hr.at[z])
        if i == 2:
            send(h_block(z), h_block(z), hs.at[3], hr.at[z], zdev(near), is_in)
        send(h_block(z), h_block(z), hds.at[1 + i], hdr.at[z], mate)
    for z in range(4):
        landed(h_buf.at[4 * (1 - core) + z], hdr.at[z])
    for i in range(4):
        hb_buf[16 * i : 16 * i + 16, :] = jnp.concatenate([h_buf[2 * i], h_buf[2 * i + 1]], axis=0).astype(BF16)

    def ff(j, carry):
        slot = lax.rem(j, ring)
        for cp in ff_copies(j, slot):
            cp.wait()
        gate = jnp.dot(hb_buf[...], wg_buf[slot], preferred_element_type=F32).astype(BF16).astype(F32)
        up = jnp.dot(hb_buf[...], wu_buf[slot], preferred_element_type=F32).astype(BF16).astype(F32)
        a_buf[:, pl.ds(pl.multiple_of(j * BLK, BLK), BLK)] = (gate * jax.nn.sigmoid(gate) * up).astype(BF16)

        @pl.when(j + ring < nff)
        def _():
            for cp in ff_copies(j + ring, slot):
                cp.start()

        return carry

    lax.fori_loop(0, nff, ff, 0)

    nc = CHUNKS
    width = dim // nc
    cols = [pl.ds(j * width, width) for j in range(nc)]
    xn = 2 * cy + (1 - cx)
    yn = 2 * (1 - cy) + cx
    dg = 2 * (1 - cy) + (1 - cx)
    xn_id, yn_id = {"tp": tp, "sp": 2 * xn + core}, {"tp": tp, "sp": 2 * yn + core}
    zorder = (tp, near, second, far)
    count = [0] * nc

    def block(j, c, z):
        return yg_buf.at[4 * (2 * c + core) + z, :, cols[j]]

    def pass_on(j, c, z, dev, rs, cond=None):
        send(block(j, c, z), block(j, c, z), ys.at[j, count[j]], rs, dev, cond)
        count[j] += 1

    def down(j):
        def one(i, carry):
            dn_copy(i).wait()
            p2_buf[:, pl.ds(pl.multiple_of(i * dcol, dcol), dcol)] = jnp.dot(a_buf[...], wd_buf[i], preferred_element_type=F32)
            return carry

        lax.fori_loop(j * ndn // nc, (j + 1) * ndn // nc, one, 0)
        send(p2_buf.at[pl.ds(pl.multiple_of(32 * (1 - core), 32), 32), cols[j]], d2_buf.at[:, cols[j]], d2s.at[j], d2r.at[j], mate)

    def pair(j):
        landed(d2_buf.at[:, cols[j]], d2r.at[j])
        s2_buf[:, cols[j]] = p2_buf[pl.ds(pl.multiple_of(32 * core, 32), 32), cols[j]] + d2_buf[:, cols[j]]
        scatter(j, cols[j], s2_buf, z2_buf, a2_buf, z2s, z2r)

    def mid(j):
        relay(j, cols[j], s2_buf, z2_buf, a2_buf, z2s, z2r)

    def own(j):
        yg_buf[4 * sp + tp, :, cols[j]] = (hid_buf[:, cols[j]] + gathered(j, cols[j], s2_buf, z2_buf, z2r)).astype(BF16).astype(F32)
        pass_on(j, chip, tp, xn_id, yr.at[j, 4 + tp])
        pass_on(j, chip, tp, yn_id, yr.at[j, 8 + tp])
        at = count[j]
        spread(lambda z: block(j, chip, z), lambda i: ys.at[j, i], lambda z: yr.at[j, z], at)
        count[j] = at + 3
        pass_on(j, chip, tp, mate, ydr.at[j, tp])

    def column(j):
        for i, z in enumerate(zorder[1:]):
            landed(block(j, chip, z), yr.at[j, z])
            if i == 2:
                pass_on(j, chip, z, zdev(near), yr.at[j, z], is_in)
            pass_on(j, chip, z, xn_id, yr.at[j, 4 + z])
            pass_on(j, chip, z, yn_id, yr.at[j, 8 + z])
            pass_on(j, chip, z, mate, ydr.at[j, z])

    def around(j):
        for i, z in enumerate(zorder):
            landed(block(j, xn, z), yr.at[j, 4 + z])
            if i % 2 == 0:
                pass_on(j, xn, z, yn_id, yr.at[j, 12 + z])
            pass_on(j, xn, z, mate, ydr.at[j, 4 + z])
            landed(block(j, yn, z), yr.at[j, 8 + z])
            if i % 2 == 1:
                pass_on(j, yn, z, xn_id, yr.at[j, 12 + z])
            pass_on(j, yn, z, mate, ydr.at[j, 8 + z])

    def across(j):
        for z in zorder:
            landed(block(j, dg, z), yr.at[j, 12 + z])
            pass_on(j, dg, z, mate, ydr.at[j, 12 + z])

    def out_copy(j):
        return pltpu.make_async_copy(yo_buf.at[:, cols[j]], y_hbm.at[:, cols[j]], osem.at[j])

    def finish(j):
        for i, c in enumerate((chip, xn, yn, dg)):
            for z in zorder:
                landed(yg_buf.at[4 * (2 * c + (1 - core)) + z, :, cols[j]], ydr.at[j, 4 * i + z])

        def out(i, carry):
            yo_buf[pl.ds(pl.multiple_of(i * 16, 16), 16), cols[j]] = jnp.concatenate([yg_buf[2 * i, :, cols[j]], yg_buf[2 * i + 1, :, cols[j]]], axis=0).astype(BF16)
            return carry

        lax.fori_loop(0, yg_buf.shape[0] // 2, out, 0)
        out_copy(j).start()

    def run(stages, steps):
        for t in range(steps):
            for lag, stage in stages:
                if 0 <= t - lag < nc:
                    stage(t - lag)

    run([(0, down), (1, pair), (2, mid)], nc + 2)
    run([(0, own), (1, column), (2, around), (3, across), (4, finish)], nc + 4)
    for done in drains:
        done()
    for j in range(nc):
        out_copy(j).wait()


def tail(att, x, g, wo, wg, wu, wd):
    batch, dim = x.shape
    half = wg.shape[1] // 2
    ring = min(5, half // BLK)
    ndn = 8
    dma = pltpu.SemaphoreType.DMA
    return pl.pallas_call(
        tail_kernel,
        out_shape=jax.ShapeDtypeStruct((batch, dim), BF16),
        in_specs=[ANY] * 7,
        out_specs=ANY,
        scratch_shapes=[
            pltpu.VMEM(att.shape, F32),
            pltpu.VMEM((dim,), BF16),
            pltpu.VMEM((4, 2, PART, 128), F32),
            pltpu.VMEM((4, 2, PART, 128), F32),
            pltpu.VMEM((3, 2, PART, 128), F32),
            pltpu.VMEM((256, 128), F32),
            pltpu.VMEM((32, dim), F32),
            pltpu.VMEM((3, 8, dim), F32),
            pltpu.VMEM((8, dim), F32),
            pltpu.VMEM((8, 8, dim), F32),
            pltpu.VMEM((64, dim), BF16),
            pltpu.VMEM((64, half), BF16),
            pltpu.VMEM((64, dim), F32),
            pltpu.VMEM((32, dim), F32),
            pltpu.VMEM((32, dim), F32),
            pltpu.VMEM((3, 8, dim), F32),
            pltpu.VMEM((8, dim), F32),
            pltpu.VMEM((batch // 8, 8, dim), F32),
            pltpu.VMEM((batch, dim), BF16),
            pltpu.VMEM((8, dim), BF16),
            pltpu.VMEM((8, dim), F32),
            pltpu.VMEM(wo.shape, BF16),
            pltpu.VMEM((ring, dim, BLK), BF16),
            pltpu.VMEM((ring, dim, BLK), BF16),
            pltpu.VMEM((ndn, half, dim // ndn), BF16),
            dma((4,)), dma((ring,)), dma((ring,)), dma((ndn,)), dma((CHUNKS,)),
            dma((4,)), dma((4,)), dma((3,)), dma((3,)), dma((2, 3)), dma((2, 4)),
            dma((4,)), dma((4,)), dma((4,)), dma((4,)), dma((CHUNKS,)), dma((CHUNKS,)), dma((CHUNKS, 3)), dma((CHUNKS, 4)),
            dma((CHUNKS, 34)), dma((CHUNKS, 16)), dma((CHUNKS, 16)),
        ],
        compiler_params=pltpu.CompilerParams(collective_id=0, has_side_effects=True, vmem_limit_bytes=63_000_000),
        cost_estimate=pl.CostEstimate(flops=2 * 64 * dim * half * 3, bytes_accessed=6 * dim * half, transcendentals=0),
        name="tail",
    )(att, x, g, wo, wg, wu, wd)


def land_kernel(y_hbm, out_hbm, buf, isem, osem):
    n = isem.shape[0]
    rows = buf.shape[0] // n
    ats = [pl.ds(i * rows, rows) for i in range(n)]
    ins = [pltpu.make_async_copy(y_hbm.at[at, :], buf.at[at, :], isem.at[i]) for i, at in enumerate(ats)]
    outs = [pltpu.make_async_copy(buf.at[at, :], out_hbm.at[at, :], osem.at[i]) for i, at in enumerate(ats)]
    for cp in ins:
        cp.start()
    for a, b in zip(ins, outs):
        a.wait()
        b.start()
    for cp in outs:
        cp.wait()


def land(y):
    return pl.pallas_call(
        land_kernel,
        out_shape=jax.ShapeDtypeStruct(y.shape, y.dtype),
        in_specs=[ANY],
        out_specs=ANY,
        scratch_shapes=[pltpu.VMEM(y.shape, y.dtype), pltpu.SemaphoreType.DMA((4,)), pltpu.SemaphoreType.DMA((4,))],
        compiler_params=pltpu.CompilerParams(vmem_limit_bytes=63_000_000),
        name="land",
    )(y)


def rope_table(length):
    freq = np.power(ROPE_BASE, np.arange(64) * (-2.0 / 128)).astype(np.float32)
    angles = (np.arange(length, dtype=np.float32)[:, None] * freq).astype(np.float64)
    cos, sin = np.cos(angles), np.sin(angles)
    return jnp.asarray(np.concatenate([cos, cos, -sin, sin], axis=1), F32)


def solution(mesh):
    cache_spec = P(None, "sp", "tp", None)
    col_spec = P(None, "tp")
    row_spec = P("tp", None)
    full_spec = P()

    def local_step(x_tok, seq_lens, k_blk, v_blk, g_attn, wq, wk, wv, wo, g_mlp, wg, wu, wd):
        batch = x_tok.shape[0]
        shape = (batch, 8, 16, 128)
        k_out, v_out, att = front(seq_lens, x_tok, g_attn, rope_table(k_blk.shape[1] * mesh.shape["sp"]), wq, wk, wv, k_blk.reshape(shape), v_blk.reshape(shape))
        y = tail(att, x_tok, g_mlp, wo, wg, wu, wd)
        return land(y), k_out.reshape(k_blk.shape), v_out.reshape(v_blk.shape)

    return jax.shard_map(local_step, mesh=mesh, in_specs=(full_spec, full_spec, cache_spec, cache_spec, full_spec, col_spec, col_spec, col_spec, row_spec, full_spec, col_spec, col_spec, row_spec), out_specs=(full_spec, cache_spec, cache_spec), check_vma=False)
```

```python
import functools

import jax
import jax.numpy as jnp
import numpy as np
from jax import lax
from jax.experimental import pallas as pl
from jax.experimental.pallas import tpu as pltpu
from jax.sharding import PartitionSpec as P

ROPE_BASE = 500000.0
NORM_EPS = 1e-5
MESH = pl.DeviceIdType.MESH
F32 = jnp.float32
BF16 = jnp.bfloat16
ANY = pl.BlockSpec(memory_space=pl.ANY)
VMEM = pl.BlockSpec(memory_space=pltpu.VMEM)
NEG = -1e30
BLK = 256
CHUNKS = 4
PART = 144


def front_kernel(
    lens_ref, x_hbm, g_hbm, tab_hbm, wq_hbm, wk_hbm, wv_hbm, k_hbm, v_hbm, ko_hbm, vo_hbm, out_hbm,
    x_buf, g_buf, tab_buf, rot_buf, u_buf, w_buf, k_buf, v_buf, q_buf, kn_buf, vn_buf, out_buf, xsem, wsem, kvsem, osem,
):
    rows, dim = x_buf.shape
    wide = 2 * BLK
    nq = wq_hbm.shape[1] // wide
    heads = wq_hbm.shape[1] // 128
    nreq = 32
    groups = rows // nreq
    base = lax.axis_index("sp") * 64

    x_copy = pltpu.make_async_copy(x_hbm, x_buf, xsem.at[0])
    g_copy = pltpu.make_async_copy(g_hbm, g_buf, xsem.at[1])
    tab_copy = pltpu.make_async_copy(tab_hbm, tab_buf, xsem.at[2])
    g_copy.start()
    x_copy.start()
    tab_copy.start()
    w_copies = [[pltpu.make_async_copy(wq_hbm.at[:, pl.ds(i * wide, wide)], w_buf.at[i], wsem.at[i])] for i in range(nq)]
    w_copies.append([
        pltpu.make_async_copy(wk_hbm, w_buf.at[nq, :, pl.ds(0, BLK)], wsem.at[nq]),
        pltpu.make_async_copy(wv_hbm, w_buf.at[nq, :, pl.ds(BLK, BLK)], wsem.at[nq + 1]),
    ])
    w_copies[0][0].start()

    def cache_copies(g):
        at = pl.ds(g * nreq, nreq)
        return (
            pltpu.make_async_copy(k_hbm.at[at], k_buf.at[at], kvsem.at[0, g]),
            pltpu.make_async_copy(v_hbm.at[at], v_buf.at[at], kvsem.at[1, g]),
        )

    def out_copies(g):
        at = pl.ds(g * nreq, nreq)
        return (
            pltpu.make_async_copy(k_buf.at[at], ko_hbm.at[at], osem.at[0, g]),
            pltpu.make_async_copy(v_buf.at[at], vo_hbm.at[at], osem.at[1, g]),
        )

    def part_copy(g):
        return pltpu.make_async_copy(out_buf.at[pl.ds(2 * g, 2)], out_hbm.at[pl.ds(2 * g, 2)], osem.at[2, g])

    def fetch(lo, hi):
        for g in range(lo, hi):
            for cp in cache_copies(g):
                cp.start()

    g_copy.wait()
    gain = g_buf[...].astype(F32).reshape(1, dim)
    x_copy.wait()
    for cps in w_copies[1:]:
        for cp in cps:
            cp.start()

    def norm(i, carry):
        at = pl.ds(pl.multiple_of(i * 16, 16), 16)
        xf = x_buf[at, :].astype(F32)
        inv = lax.rsqrt(jnp.sum(xf * xf, axis=-1, keepdims=True) * (1.0 / dim) + NORM_EPS)
        u_buf[at, :] = (xf * inv * gain).astype(BF16)
        return carry

    lax.fori_loop(0, rows // 16, norm, 0, unroll=2)
    tab_copy.wait()

    def angle(i, carry):
        rot_buf[pl.ds(i, 1), :] = tab_buf[pl.ds(lens_ref[i], 1), :]
        return carry

    lax.fori_loop(0, rows, angle, 0, unroll=16)
    cosv = rot_buf[:, :128]
    sinv = rot_buf[:, 128:]

    def rope(h):
        h = h.astype(BF16).astype(F32)
        return (h * cosv + pltpu.roll(h, 64, 1) * sinv).astype(BF16).astype(F32)

    for i in range(nq + 1):
        for cp in w_copies[i]:
            cp.wait()
        fetch(groups * i // (nq + 1), groups * (i + 1) // (nq + 1))
        prod = jnp.dot(u_buf[...], w_buf[i], preferred_element_type=F32)
        for s in range(4):
            part = prod[:, s * 128 : (s + 1) * 128]
            if i < nq:
                q_buf[pl.ds(4 * i + s, rows, stride=heads), :] = rope(part)
            elif s < 2:
                kn_buf[pl.ds(s, rows, stride=2), :] = rope(part)
            else:
                vn_buf[pl.ds(s - 2, rows, stride=2), :] = part.astype(BF16).astype(F32)

    lane = lax.broadcasted_iota(jnp.int32, (8, 128), 1)
    head = lax.broadcasted_iota(jnp.int32, (8, 128), 0)
    match = (lane % 2) == (head // 4)
    lane_pos = jnp.where(match, lane // 2, 1 << 20)
    row16 = lax.broadcasted_iota(jnp.int32, (16, 128), 0)
    scale = 128.0**-0.5
    zero = jnp.zeros((8, 128), BF16)

    def insert(b, c_buf, n_buf, blk, off):
        row0 = jnp.broadcast_to(n_buf[pl.ds(2 * b, 1), :], (16, 128))
        row1 = jnp.broadcast_to(n_buf[pl.ds(2 * b + 1, 1), :], (16, 128))
        new = jnp.where(row16 == off, row0, row1)
        old = c_buf[b, blk].astype(F32)
        c_buf[b, blk] = jnp.where((row16 == off) | (row16 == off + 1), new, old).astype(BF16)

    def group(g, carry):
        for cp in cache_copies(g):
            cp.wait()

        def put(i, c):
            b = g * nreq + i
            pos = lens_ref[b] - base
            inside = (pos >= 0) & (pos < 64)
            at = jnp.where(inside, pos, 0)
            off = jnp.where(inside, 2 * (at % 8), -8)
            insert(b, k_buf, kn_buf, at // 8, off)
            insert(b, v_buf, vn_buf, at // 8, off)
            return c

        lax.fori_loop(0, nreq, put, 0, unroll=8)
        for cp in out_copies(g):
            cp.start()

        first = g * nreq
        scores = []
        for p in range(16):
            b = first + 2 * p
            keys = k_buf[pl.ds(b, 2)].reshape(256, 128)
            qp = q_buf[pl.ds(pl.multiple_of(b * 8, 16), 16), :].astype(BF16)
            scores.append(lax.dot_general(qp, keys, (((1,), (1,)), ((), ())), preferred_element_type=F32))
        for h in range(2):
            half = g * 2 + h
            wts = []
            stm, stl = jnp.zeros((8, 128), F32), jnp.ones((8, 128), F32)
            for p in range(8):
                for j in range(2):
                    s = scores[8 * h + p][8 * j : 8 * j + 8, 128 * j : 128 * j + 128] * scale
                    valid = lane_pos <= lens_ref[first + 16 * h + 2 * p + j] - base
                    m = jnp.max(jnp.where(valid, s, NEG), axis=1, keepdims=True)
                    w = jnp.where(valid, jnp.exp(s - m), 0.0)
                    here = lane == 2 * p + j
                    stm = jnp.where(here, m, stm)
                    stl = jnp.where(here, jnp.sum(w, axis=1, keepdims=True), stl)
                    wts.append(w.astype(BF16))
            out_buf[half, 128:136, :] = stm
            out_buf[half, 136:144, :] = stl
            for p in range(8):
                wp = jnp.concatenate([jnp.concatenate([wts[2 * p], zero], axis=1), jnp.concatenate([zero, wts[2 * p + 1]], axis=1)], axis=0)
                vals = v_buf[pl.ds(first + 16 * h + 2 * p, 2)].reshape(256, 128)
                out_buf[half, 16 * p : 16 * p + 16, :] = jnp.dot(wp, vals, preferred_element_type=F32)
        part_copy(g).start()
        return carry

    lax.fori_loop(0, groups, group, 0)
    for g in range(groups):
        for cp in out_copies(g):
            cp.wait()
        part_copy(g).wait()


def front(lens, x, g, tab, wq, wk, wv, k, v):
    rows, dim = x.shape
    heads = wq.shape[1] // 128
    nblk = wq.shape[1] // (2 * BLK) + 1
    groups = rows // 32
    dma = pltpu.SemaphoreType.DMA
    return pl.pallas_call(
        front_kernel,
        out_shape=(
            jax.ShapeDtypeStruct(k.shape, BF16),
            jax.ShapeDtypeStruct(v.shape, BF16),
            jax.ShapeDtypeStruct((2 * groups, PART, 128), F32),
        ),
        in_specs=[pl.BlockSpec(memory_space=pltpu.SMEM)] + [ANY] * 8,
        out_specs=(ANY, ANY, ANY),
        scratch_shapes=[
            pltpu.VMEM((rows, dim), BF16),
            pltpu.VMEM((dim,), BF16),
            pltpu.VMEM(tab.shape, F32),
            pltpu.VMEM((rows, 256), F32),
            pltpu.VMEM((rows, dim), BF16),
            pltpu.VMEM((nblk, dim, 2 * BLK), BF16),
            pltpu.VMEM(k.shape, BF16),
            pltpu.VMEM(v.shape, BF16),
            pltpu.VMEM((rows * heads, 128), F32),
            pltpu.VMEM((rows * 2, 128), F32),
            pltpu.VMEM((rows * 2, 128), F32),
            pltpu.VMEM((2 * groups, PART, 128), F32),
            dma((3,)),
            dma((nblk + 1,)),
            dma((2, groups)),
            dma((3, groups)),
        ],
        compiler_params=pltpu.CompilerParams(vmem_limit_bytes=63_000_000),
        cost_estimate=pl.CostEstimate(flops=4 * rows * dim * nblk * BLK, bytes_accessed=4 * dim * nblk * BLK + 8 * k.size, transcendentals=0),
        name="front",
    )(lens, x, g, tab, wq, wk, wv, k, v)


def merge(blocks, out_ref, last):
    rows = PART - 16
    maxs = [b[rows : rows + 8, :] for b in blocks]
    top = functools.reduce(jnp.maximum, maxs)
    facs = [jnp.exp(m - top) for m in maxs]
    tot = functools.reduce(jnp.add, [f * b[rows + 8 : rows + 16, :] for f, b in zip(facs, blocks)])
    if last:
        inv = 1.0 / tot
        facs = [f * inv for f in facs]
    else:
        out_ref[rows : rows + 8, :] = top
        out_ref[rows + 8 : rows + 16, :] = tot
    for i in range(rows // 8):
        at = slice(8 * i, 8 * i + 8)
        out_ref[at, :] = functools.reduce(jnp.add, [b[at, :] * f[:, i : i + 1] for f, b in zip(facs, blocks)])


def tail_kernel(
    att_hbm, x_hbm, g_hbm, wo_hbm, wg_hbm, wu_hbm, wd_hbm, y_hbm,
    att_ref, g_ref, d1_buf, m_buf, r1_buf, o_buf, p_buf, z1_buf, a1_buf, h_buf, hb_buf, a_buf, p2_buf, d2_buf, s2_buf, z2_buf, a2_buf, yg_buf, yo_buf, x_buf, hid_buf,
    wo_buf, wg_buf, wu_buf, wd_buf,
    lsem, gsem, usem, dsem, osem, d1s, d1r, r1s, r1r, z1s, z1r, hs, hr, hds, hdr, d2s, d2r, z2s, z2r, ys, yr, ydr, turn,
):
    tp, sp = lax.axis_index("tp"), lax.axis_index("sp")
    core, chip = sp % 2, sp // 2
    cx, cy = chip % 2, chip // 2
    mate = {"tp": tp, "sp": 2 * chip + (1 - core)}
    plane = [(chip + k) % 4 for k in range(4)]
    plane_id = [{"tp": tp, "sp": 2 * q + core} for q in plane]
    side = tp // 2
    inside = tp * (1 - 2 * side) + 3 * side
    is_end, is_in = inside == 0, inside == 1

    def place(m):
        return m + side * (3 - 2 * m)

    near, second, far = place(1 - inside), place(2), place(3)

    def zdev(z):
        return {"tp": z, "sp": sp}

    dim = x_buf.shape[1]
    ring = wg_buf.shape[0]
    half = wd_buf.shape[1]
    nff = half // BLK
    ndn = wd_buf.shape[0]
    dcol = wd_buf.shape[2]

    me8 = pl.multiple_of(32 * sp + 8 * tp, 8)
    x_copy = pltpu.make_async_copy(x_hbm.at[pl.ds(me8, 8), :], x_buf, lsem.at[0])
    wo_copy = pltpu.make_async_copy(wo_hbm, wo_buf, lsem.at[1])

    def ff_copies(j, slot):
        at = pl.ds(pl.multiple_of(core * half + j * BLK, BLK), BLK)
        return (
            pltpu.make_async_copy(wg_hbm.at[:, at], wg_buf.at[slot], gsem.at[slot]),
            pltpu.make_async_copy(wu_hbm.at[:, at], wu_buf.at[slot], usem.at[slot]),
        )

    def dn_copy(j):
        return pltpu.make_async_copy(
            wd_hbm.at[pl.ds(pl.multiple_of(core * half, BLK), half), pl.ds(pl.multiple_of(j * dcol, dcol), dcol)], wd_buf.at[j], dsem.at[j]
        )

    att_copy = pltpu.make_async_copy(att_hbm, att_ref, lsem.at[2])
    g_copy = pltpu.make_async_copy(g_hbm, g_ref, lsem.at[3])
    att_copy.start()
    x_copy.start()
    g_copy.start()
    wo_copy.start()

    def prefetch_ff(lo, hi):
        for j in range(lo, min(hi, ring, nff)):
            for cp in ff_copies(j, j):
                cp.start()

    @pl.when(is_end)
    def _():
        z1_buf[2] = jnp.zeros_like(z1_buf[2])
        z2_buf[2] = jnp.zeros_like(z2_buf[2])

    bar = pltpu.get_barrier_semaphore()
    for dev in [mate] + plane_id[1:] + [zdev((tp + k) % 4) for k in (1, 2, 3)]:
        pl.semaphore_signal(bar, inc=1, device_id=dev, device_id_type=MESH)
    pl.semaphore_wait(bar, 7)

    drains = []

    def send(src, dst, ssem, rsem, dev, cond=None):
        def make():
            return pltpu.make_async_remote_copy(src_ref=src, dst_ref=dst, send_sem=ssem, recv_sem=rsem, device_id=dev, device_id_type=MESH)

        def go():
            make().start()

        def done():
            make().wait_send()

        if cond is None:
            go()
            drains.append(done)
        else:
            pl.when(cond)(go)
            drains.append(lambda: pl.when(cond)(done))

    def landed(ref, rsem):
        pltpu.make_async_copy(ref, ref, rsem).wait()

    order = [1, 2, 3, 0]
    att_copy.wait()
    for k in order:
        send(att_ref.at[pl.ds(4 * plane[k] + 2 * (1 - core), 2)], d1_buf.at[k], d1s.at[k], d1r.at[k], mate)
    for k in order:
        landed(d1_buf.at[k], d1r.at[k])
        for h in range(2):
            merge([att_ref.at[4 * plane[k] + 2 * core + h], d1_buf.at[k, h]], m_buf.at[k, h], False)

    @pl.when(core == 1)
    def _():
        pl.semaphore_wait(turn, 1)

    before = len(drains)
    for k in (1, 2, 3):
        send(m_buf.at[k], r1_buf.at[k - 1], r1s.at[k - 1], r1r.at[k - 1], plane_id[k])
    plane_sent = drains[before:]
    del drains[before:]

    @pl.when(core == 0)
    def _():
        for done in plane_sent:
            done()
        pl.semaphore_signal(turn, inc=1, device_id=mate, device_id_type=MESH)

    prefetch_ff(0, 2)
    for k in (1, 2, 3):
        landed(r1_buf.at[k - 1], r1r.at[k - 1])
    for h in range(2):
        merge([m_buf.at[0, h]] + [r1_buf.at[k, h] for k in range(3)], o_buf.at[pl.ds(128 * h, 128)], True)

    def rows8(z):
        return pl.ds(pl.multiple_of(8 * z, 8), 8)

    def scatter(j, cols, src, buf, agg, ss, rs):
        send(src.at[rows8(second), cols], buf.at[2 - inside, :, cols], ss.at[j, 0], rs.at[j, 2 - inside], zdev(second))
        send(src.at[rows8(far), cols], agg.at[:, cols], ss.at[j, 1], rs.at[j, 3], zdev(near), is_end)
        send(src.at[rows8(near), cols], buf.at[0, :, cols], ss.at[j, 2], rs.at[j, 0], zdev(near))

    def relay(j, cols, src, buf, agg, ss, rs):
        @pl.when(is_in)
        def _():
            landed(agg.at[:, cols], rs.at[j, 3])
            src[rows8(far), cols] = src[rows8(far), cols] + agg[:, cols]

        send(src.at[rows8(far), cols], buf.at[1, :, cols], ss.at[j, 1], rs.at[j, 1], zdev(far), is_in)

    def gathered(j, cols, src, buf, rs):
        landed(buf.at[0, :, cols], rs.at[j, 0])
        landed(buf.at[1, :, cols], rs.at[j, 1])

        @pl.when(is_in)
        def _():
            landed(buf.at[2, :, cols], rs.at[j, 2])

        return src[rows8(tp), cols] + buf[0, :, cols] + buf[1, :, cols] + buf[2, :, cols]

    o = jnp.concatenate([o_buf[pl.ds(h, 32, stride=8), :].astype(BF16) for h in range(8)], axis=1)
    wo_copy.wait()

    def proj(j, carry):
        at = pl.ds(pl.multiple_of(j * 512, 512), 512)
        p_buf[:, at] = jnp.dot(o, wo_buf[:, at], preferred_element_type=F32)
        return carry

    parts1 = [pl.ds(i * (dim // 2), dim // 2) for i in range(2)]
    for i in range(2):
        lax.fori_loop(i * (dim // 1024), (i + 1) * (dim // 1024), proj, 0)
        scatter(i, parts1[i], p_buf, z1_buf, a1_buf, z1s, z1r)
    prefetch_ff(2, ring)
    for i in range(2):
        relay(i, parts1[i], p_buf, z1_buf, a1_buf, z1s, z1r)
    for j in range(ndn // 2):
        dn_copy(j).start()
    x_copy.wait()
    g_copy.wait()
    for i in range(2):
        hid_buf[:, parts1[i]] = (x_buf[:, parts1[i]].astype(F32) + gathered(i, parts1[i], p_buf, z1_buf, z1r)).astype(BF16).astype(F32)
    hid = hid_buf[...]
    inv = lax.rsqrt(jnp.sum(hid * hid, axis=-1, keepdims=True) * (1.0 / dim) + NORM_EPS)
    mine = core * 4
    h_buf[mine + tp] = (hid * inv * g_ref[...].astype(F32).reshape(1, dim)).astype(BF16).astype(F32)

    def spread(block, ss, rs, first):
        send(block(tp), block(tp), ss(first), rs(tp), zdev(second))
        send(block(tp), block(tp), ss(first + 1), rs(tp), zdev(far), is_in)
        send(block(tp), block(tp), ss(first + 2), rs(tp), zdev(near))

    def h_block(z):
        return h_buf.at[mine + z]

    spread(h_block, lambda i: hs.at[i], lambda z: hr.at[z], 0)
    send(h_block(tp), h_block(tp), hds.at[0], hdr.at[tp], mate)
    for j in range(ndn // 2, ndn):
        dn_copy(j).start()
    for i, z in enumerate((near, second, far)):
        landed(h_block(z), hr.at[z])
        if i == 2:
            send(h_block(z), h_block(z), hs.at[3], hr.at[z], zdev(near), is_in)
        send(h_block(z), h_block(z), hds.at[1 + i], hdr.at[z], mate)
    for z in range(4):
        landed(h_buf.at[4 * (1 - core) + z], hdr.at[z])
    for i in range(4):
        hb_buf[16 * i : 16 * i + 16, :] = jnp.concatenate([h_buf[2 * i], h_buf[2 * i + 1]], axis=0).astype(BF16)

    def ff(j, carry):
        slot = lax.rem(j, ring)
        for cp in ff_copies(j, slot):
            cp.wait()
        gate = jnp.dot(hb_buf[...], wg_buf[slot], preferred_element_type=F32).astype(BF16).astype(F32)
        up = jnp.dot(hb_buf[...], wu_buf[slot], preferred_element_type=F32).astype(BF16).astype(F32)
        a_buf[:, pl.ds(pl.multiple_of(j * BLK, BLK), BLK)] = (gate * jax.nn.sigmoid(gate) * up).astype(BF16)

        @pl.when(j + ring < nff)
        def _():
            for cp in ff_copies(j + ring, slot):
                cp.start()

        return carry

    lax.fori_loop(0, nff, ff, 0)

    nc = CHUNKS
    width = dim // nc
    cols = [pl.ds(j * width, width) for j in range(nc)]
    xn = 2 * cy + (1 - cx)
    yn = 2 * (1 - cy) + cx
    dg = 2 * (1 - cy) + (1 - cx)
    xn_id, yn_id = {"tp": tp, "sp": 2 * xn + core}, {"tp": tp, "sp": 2 * yn + core}
    zorder = (tp, near, second, far)
    count = [0] * nc

    def block(j, c, z):
        return yg_buf.at[4 * (2 * c + core) + z, :, cols[j]]

    def pass_on(j, c, z, dev, rs, cond=None):
        send(block(j, c, z), block(j, c, z), ys.at[j, count[j]], rs, dev, cond)
        count[j] += 1

    def down(j):
        def one(i, carry):
            dn_copy(i).wait()
            p2_buf[:, pl.ds(pl.multiple_of(i * dcol, dcol), dcol)] = jnp.dot(a_buf[...], wd_buf[i], preferred_element_type=F32)
            return carry

        lax.fori_loop(j * ndn // nc, (j + 1) * ndn // nc, one, 0)
        send(p2_buf.at[pl.ds(pl.multiple_of(32 * (1 - core), 32), 32), cols[j]], d2_buf.at[:, cols[j]], d2s.at[j], d2r.at[j], mate)

    def pair(j):
        landed(d2_buf.at[:, cols[j]], d2r.at[j])
        s2_buf[:, cols[j]] = p2_buf[pl.ds(pl.multiple_of(32 * core, 32), 32), cols[j]] + d2_buf[:, cols[j]]
        scatter(j, cols[j], s2_buf, z2_buf, a2_buf, z2s, z2r)

    def mid(j):
        relay(j, cols[j], s2_buf, z2_buf, a2_buf, z2s, z2r)

    def own(j):
        yg_buf[4 * sp + tp, :, cols[j]] = (hid_buf[:, cols[j]] + gathered(j, cols[j], s2_buf, z2_buf, z2r)).astype(BF16).astype(F32)
        pass_on(j, chip, tp, xn_id, yr.at[j, 4 + tp])
        pass_on(j, chip, tp, yn_id, yr.at[j, 8 + tp])
        at = count[j]
        spread(lambda z: block(j, chip, z), lambda i: ys.at[j, i], lambda z: yr.at[j, z], at)
        count[j] = at + 3
        pass_on(j, chip, tp, mate, ydr.at[j, tp])

    def column(j):
        for i, z in enumerate(zorder[1:]):
            landed(block(j, chip, z), yr.at[j, z])
            if i == 2:
                pass_on(j, chip, z, zdev(near), yr.at[j, z], is_in)
            pass_on(j, chip, z, xn_id, yr.at[j, 4 + z])
            pass_on(j, chip, z, yn_id, yr.at[j, 8 + z])
            pass_on(j, chip, z, mate, ydr.at[j, z])

    def around(j):
        for i, z in enumerate(zorder):
            landed(block(j, xn, z), yr.at[j, 4 + z])
            if i % 2 == 0:
                pass_on(j, xn, z, yn_id, yr.at[j, 12 + z])
            pass_on(j, xn, z, mate, ydr.at[j, 4 + z])
            landed(block(j, yn, z), yr.at[j, 8 + z])
            if i % 2 == 1:
                pass_on(j, yn, z, xn_id, yr.at[j, 12 + z])
            pass_on(j, yn, z, mate, ydr.at[j, 8 + z])

    def across(j):
        for z in zorder:
            landed(block(j, dg, z), yr.at[j, 12 + z])
            pass_on(j, dg, z, mate, ydr.at[j, 12 + z])

    def out_copy(j):
        return pltpu.make_async_copy(yo_buf.at[:, cols[j]], y_hbm.at[:, cols[j]], osem.at[j])

    def finish(j):
        for i, c in enumerate((chip, xn, yn, dg)):
            for z in zorder:
                landed(yg_buf.at[4 * (2 * c + (1 - core)) + z, :, cols[j]], ydr.at[j, 4 * i + z])

        def out(i, carry):
            yo_buf[pl.ds(pl.multiple_of(i * 16, 16), 16), cols[j]] = jnp.concatenate([yg_buf[2 * i, :, cols[j]], yg_buf[2 * i + 1, :, cols[j]]], axis=0).astype(BF16)
            return carry

        lax.fori_loop(0, yg_buf.shape[0] // 2, out, 0)
        out_copy(j).start()

    def run(stages, steps):
        for t in range(steps):
            for lag, stage in stages:
                if 0 <= t - lag < nc:
                    stage(t - lag)

    run([(0, down), (1, pair), (2, mid)], nc + 2)
    run([(0, own), (1, column), (2, around), (3, across), (4, finish)], nc + 4)
    for done in drains:
        done()

    @pl.when(core == 1)
    def _():
        for done in plane_sent:
            done()

    for j in range(nc):
        out_copy(j).wait()


def tail(att, x, g, wo, wg, wu, wd):
    batch, dim = x.shape
    half = wg.shape[1] // 2
    ring = min(5, half // BLK)
    ndn = 8
    dma = pltpu.SemaphoreType.DMA
    return pl.pallas_call(
        tail_kernel,
        out_shape=jax.ShapeDtypeStruct((batch, dim), BF16),
        in_specs=[ANY] * 7,
        out_specs=ANY,
        scratch_shapes=[
            pltpu.VMEM(att.shape, F32),
            pltpu.VMEM((dim,), BF16),
            pltpu.VMEM((4, 2, PART, 128), F32),
            pltpu.VMEM((4, 2, PART, 128), F32),
            pltpu.VMEM((3, 2, PART, 128), F32),
            pltpu.VMEM((256, 128), F32),
            pltpu.VMEM((32, dim), F32),
            pltpu.VMEM((3, 8, dim), F32),
            pltpu.VMEM((8, dim), F32),
            pltpu.VMEM((8, 8, dim), F32),
            pltpu.VMEM((64, dim), BF16),
            pltpu.VMEM((64, half), BF16),
            pltpu.VMEM((64, dim), F32),
            pltpu.VMEM((32, dim), F32),
            pltpu.VMEM((32, dim), F32),
            pltpu.VMEM((3, 8, dim), F32),
            pltpu.VMEM((8, dim), F32),
            pltpu.VMEM((batch // 8, 8, dim), F32),
            pltpu.VMEM((batch, dim), BF16),
            pltpu.VMEM((8, dim), BF16),
            pltpu.VMEM((8, dim), F32),
            pltpu.VMEM(wo.shape, BF16),
            pltpu.VMEM((ring, dim, BLK), BF16),
            pltpu.VMEM((ring, dim, BLK), BF16),
            pltpu.VMEM((ndn, half, dim // ndn), BF16),
            dma((4,)), dma((ring,)), dma((ring,)), dma((ndn,)), dma((CHUNKS,)),
            dma((4,)), dma((4,)), dma((3,)), dma((3,)), dma((2, 3)), dma((2, 4)),
            dma((4,)), dma((4,)), dma((4,)), dma((4,)), dma((CHUNKS,)), dma((CHUNKS,)), dma((CHUNKS, 3)), dma((CHUNKS, 4)),
            dma((CHUNKS, 34)), dma((CHUNKS, 16)), dma((CHUNKS, 16)), pltpu.SemaphoreType.REGULAR,
        ],
        compiler_params=pltpu.CompilerParams(collective_id=0, has_side_effects=True, vmem_limit_bytes=63_000_000),
        cost_estimate=pl.CostEstimate(flops=2 * 64 * dim * half * 3, bytes_accessed=6 * dim * half, transcendentals=0),
        name="tail",
    )(att, x, g, wo, wg, wu, wd)


def land_kernel(y_hbm, out_hbm, buf, isem, osem):
    n = isem.shape[0]
    rows = buf.shape[0] // n
    ats = [pl.ds(i * rows, rows) for i in range(n)]
    ins = [pltpu.make_async_copy(y_hbm.at[at, :], buf.at[at, :], isem.at[i]) for i, at in enumerate(ats)]
    outs = [pltpu.make_async_copy(buf.at[at, :], out_hbm.at[at, :], osem.at[i]) for i, at in enumerate(ats)]
    for cp in ins:
        cp.start()
    for a, b in zip(ins, outs):
        a.wait()
        b.start()
    for cp in outs:
        cp.wait()


def land(y):
    return pl.pallas_call(
        land_kernel,
        out_shape=jax.ShapeDtypeStruct(y.shape, y.dtype),
        in_specs=[ANY],
        out_specs=ANY,
        scratch_shapes=[pltpu.VMEM(y.shape, y.dtype), pltpu.SemaphoreType.DMA((4,)), pltpu.SemaphoreType.DMA((4,))],
        compiler_params=pltpu.CompilerParams(vmem_limit_bytes=63_000_000),
        name="land",
    )(y)


def rope_table(length):
    freq = np.power(ROPE_BASE, np.arange(64) * (-2.0 / 128)).astype(np.float32)
    angles = (np.arange(length, dtype=np.float32)[:, None] * freq).astype(np.float64)
    cos, sin = np.cos(angles), np.sin(angles)
    return jnp.asarray(np.concatenate([cos, cos, -sin, sin], axis=1), F32)


def solution(mesh):
    cache_spec = P(None, "sp", "tp", None)
    col_spec = P(None, "tp")
    row_spec = P("tp", None)
    full_spec = P()

    def local_step(x_tok, seq_lens, k_blk, v_blk, g_attn, wq, wk, wv, wo, g_mlp, wg, wu, wd):
        batch = x_tok.shape[0]
        shape = (batch, 8, 16, 128)
        k_out, v_out, att = front(seq_lens, x_tok, g_attn, rope_table(k_blk.shape[1] * mesh.shape["sp"]), wq, wk, wv, k_blk.reshape(shape), v_blk.reshape(shape))
        y = tail(att, x_tok, g_mlp, wo, wg, wu, wd)
        return land(y), k_out.reshape(k_blk.shape), v_out.reshape(v_blk.shape)

    return jax.shard_map(local_step, mesh=mesh, in_specs=(full_spec, full_spec, cache_spec, cache_spec, full_spec, col_spec, col_spec, col_spec, row_spec, full_spec, col_spec, col_spec, row_spec), out_specs=(full_spec, cache_spec, cache_spec), check_vma=False)
```

```python
import functools

import jax
import jax.numpy as jnp
import numpy as np
from jax import lax
from jax.experimental import pallas as pl
from jax.experimental.pallas import tpu as pltpu
from jax.sharding import PartitionSpec as P

ROPE_BASE = 500000.0
NORM_EPS = 1e-5
MESH = pl.DeviceIdType.MESH
F32 = jnp.float32
BF16 = jnp.bfloat16
ANY = pl.BlockSpec(memory_space=pl.ANY)
VMEM = pl.BlockSpec(memory_space=pltpu.VMEM)
NEG = -1e30
BLK = 256
CHUNKS = 4
LEAD = 3
PART = 144


def front_kernel(
    lens_ref, x_hbm, g_hbm, tab_hbm, wq_hbm, wk_hbm, wv_hbm, k_hbm, v_hbm, ko_hbm, vo_hbm, out_hbm,
    x_buf, g_buf, tab_buf, rot_buf, u_buf, w_buf, k_buf, v_buf, q_buf, kn_buf, vn_buf, out_buf, xsem, wsem, kvsem, osem,
):
    rows, dim = x_buf.shape
    wide = 2 * BLK
    nq = wq_hbm.shape[1] // wide
    heads = wq_hbm.shape[1] // 128
    nreq = 32
    groups = rows // nreq
    base = lax.axis_index("sp") * 64

    x_copy = pltpu.make_async_copy(x_hbm, x_buf, xsem.at[0])
    g_copy = pltpu.make_async_copy(g_hbm, g_buf, xsem.at[1])
    tab_copy = pltpu.make_async_copy(tab_hbm, tab_buf, xsem.at[2])
    g_copy.start()
    x_copy.start()
    tab_copy.start()
    w_copies = [[pltpu.make_async_copy(wq_hbm.at[:, pl.ds(i * wide, wide)], w_buf.at[i], wsem.at[i])] for i in range(nq)]
    w_copies.append([
        pltpu.make_async_copy(wk_hbm, w_buf.at[nq, :, pl.ds(0, BLK)], wsem.at[nq]),
        pltpu.make_async_copy(wv_hbm, w_buf.at[nq, :, pl.ds(BLK, BLK)], wsem.at[nq + 1]),
    ])
    w_copies[0][0].start()

    def cache_copies(g):
        at = pl.ds(g * nreq, nreq)
        return (
            pltpu.make_async_copy(k_hbm.at[at], k_buf.at[at], kvsem.at[0, g]),
            pltpu.make_async_copy(v_hbm.at[at], v_buf.at[at], kvsem.at[1, g]),
        )

    def out_copies(g):
        at = pl.ds(g * nreq, nreq)
        return (
            pltpu.make_async_copy(k_buf.at[at], ko_hbm.at[at], osem.at[0, g]),
            pltpu.make_async_copy(v_buf.at[at], vo_hbm.at[at], osem.at[1, g]),
        )

    def part_copy(g):
        return pltpu.make_async_copy(out_buf.at[pl.ds(2 * g, 2)], out_hbm.at[pl.ds(2 * g, 2)], osem.at[2, g])

    def fetch(lo, hi):
        for g in range(lo, hi):
            for cp in cache_copies(g):
                cp.start()

    g_copy.wait()
    gain = g_buf[...].astype(F32).reshape(1, dim)
    x_copy.wait()
    for cps in w_copies[1:]:
        for cp in cps:
            cp.start()

    def norm(i, carry):
        at = pl.ds(pl.multiple_of(i * 16, 16), 16)
        xf = x_buf[at, :].astype(F32)
        inv = lax.rsqrt(jnp.sum(xf * xf, axis=-1, keepdims=True) * (1.0 / dim) + NORM_EPS)
        u_buf[at, :] = (xf * inv * gain).astype(BF16)
        return carry

    lax.fori_loop(0, rows // 16, norm, 0, unroll=2)
    tab_copy.wait()

    def angle(i, carry):
        rot_buf[pl.ds(i, 1), :] = tab_buf[pl.ds(lens_ref[i], 1), :]
        return carry

    lax.fori_loop(0, rows, angle, 0, unroll=16)
    cosv = rot_buf[:, :128]
    sinv = rot_buf[:, 128:]

    def rope(h):
        h = h.astype(BF16).astype(F32)
        return (h * cosv + pltpu.roll(h, 64, 1) * sinv).astype(BF16).astype(F32)

    for i in range(nq + 1):
        for cp in w_copies[i]:
            cp.wait()
        fetch(groups * i // (nq + 1), groups * (i + 1) // (nq + 1))
        prod = jnp.dot(u_buf[...], w_buf[i], preferred_element_type=F32)
        for s in range(4):
            part = prod[:, s * 128 : (s + 1) * 128]
            if i < nq:
                q_buf[pl.ds(4 * i + s, rows, stride=heads), :] = rope(part)
            elif s < 2:
                kn_buf[pl.ds(s, rows, stride=2), :] = rope(part)
            else:
                vn_buf[pl.ds(s - 2, rows, stride=2), :] = part.astype(BF16).astype(F32)

    lane = lax.broadcasted_iota(jnp.int32, (8, 128), 1)
    head = lax.broadcasted_iota(jnp.int32, (8, 128), 0)
    match = (lane % 2) == (head // 4)
    lane_pos = jnp.where(match, lane // 2, 1 << 20)
    row16 = lax.broadcasted_iota(jnp.int32, (16, 128), 0)
    scale = 128.0**-0.5
    zero = jnp.zeros((8, 128), BF16)

    def insert(b, c_buf, n_buf, blk, off):
        row0 = jnp.broadcast_to(n_buf[pl.ds(2 * b, 1), :], (16, 128))
        row1 = jnp.broadcast_to(n_buf[pl.ds(2 * b + 1, 1), :], (16, 128))
        new = jnp.where(row16 == off, row0, row1)
        old = c_buf[b, blk].astype(F32)
        c_buf[b, blk] = jnp.where((row16 == off) | (row16 == off + 1), new, old).astype(BF16)

    def group(g, carry):
        for cp in cache_copies(g):
            cp.wait()

        def put(i, c):
            b = g * nreq + i
            pos = lens_ref[b] - base
            inside = (pos >= 0) & (pos < 64)
            at = jnp.where(inside, pos, 0)
            off = jnp.where(inside, 2 * (at % 8), -8)
            insert(b, k_buf, kn_buf, at // 8, off)
            insert(b, v_buf, vn_buf, at // 8, off)
            return c

        lax.fori_loop(0, nreq, put, 0, unroll=8)
        for cp in out_copies(g):
            cp.start()

        first = g * nreq
        scores = []
        for p in range(16):
            b = first + 2 * p
            keys = k_buf[pl.ds(b, 2)].reshape(256, 128)
            qp = q_buf[pl.ds(pl.multiple_of(b * 8, 16), 16), :].astype(BF16)
            scores.append(lax.dot_general(qp, keys, (((1,), (1,)), ((), ())), preferred_element_type=F32))
        for h in range(2):
            half = g * 2 + h
            wts = []
            stm, stl = jnp.zeros((8, 128), F32), jnp.ones((8, 128), F32)
            for p in range(8):
                for j in range(2):
                    s = scores[8 * h + p][8 * j : 8 * j + 8, 128 * j : 128 * j + 128] * scale
                    valid = lane_pos <= lens_ref[first + 16 * h + 2 * p + j] - base
                    m = jnp.max(jnp.where(valid, s, NEG), axis=1, keepdims=True)
                    w = jnp.where(valid, jnp.exp(s - m), 0.0)
                    here = lane == 2 * p + j
                    stm = jnp.where(here, m, stm)
                    stl = jnp.where(here, jnp.sum(w, axis=1, keepdims=True), stl)
                    wts.append(w.astype(BF16))
            out_buf[half, 128:136, :] = stm
            out_buf[half, 136:144, :] = stl
            for p in range(8):
                wp = jnp.concatenate([jnp.concatenate([wts[2 * p], zero], axis=1), jnp.concatenate([zero, wts[2 * p + 1]], axis=1)], axis=0)
                vals = v_buf[pl.ds(first + 16 * h + 2 * p, 2)].reshape(256, 128)
                out_buf[half, 16 * p : 16 * p + 16, :] = jnp.dot(wp, vals, preferred_element_type=F32)
        part_copy(g).start()
        return carry

    lax.fori_loop(0, groups, group, 0)
    for g in range(groups):
        for cp in out_copies(g):
            cp.wait()
        part_copy(g).wait()


def front(lens, x, g, tab, wq, wk, wv, k, v):
    rows, dim = x.shape
    heads = wq.shape[1] // 128
    nblk = wq.shape[1] // (2 * BLK) + 1
    groups = rows // 32
    dma = pltpu.SemaphoreType.DMA
    return pl.pallas_call(
        front_kernel,
        out_shape=(
            jax.ShapeDtypeStruct(k.shape, BF16),
            jax.ShapeDtypeStruct(v.shape, BF16),
            jax.ShapeDtypeStruct((2 * groups, PART, 128), F32),
        ),
        in_specs=[pl.BlockSpec(memory_space=pltpu.SMEM)] + [ANY] * 8,
        out_specs=(ANY, ANY, ANY),
        scratch_shapes=[
            pltpu.VMEM((rows, dim), BF16),
            pltpu.VMEM((dim,), BF16),
            pltpu.VMEM(tab.shape, F32),
            pltpu.VMEM((rows, 256), F32),
            pltpu.VMEM((rows, dim), BF16),
            pltpu.VMEM((nblk, dim, 2 * BLK), BF16),
            pltpu.VMEM(k.shape, BF16),
            pltpu.VMEM(v.shape, BF16),
            pltpu.VMEM((rows * heads, 128), F32),
            pltpu.VMEM((rows * 2, 128), F32),
            pltpu.VMEM((rows * 2, 128), F32),
            pltpu.VMEM((2 * groups, PART, 128), F32),
            dma((3,)),
            dma((nblk + 1,)),
            dma((2, groups)),
            dma((3, groups)),
        ],
        compiler_params=pltpu.CompilerParams(vmem_limit_bytes=63_000_000),
        cost_estimate=pl.CostEstimate(flops=4 * rows * dim * nblk * BLK, bytes_accessed=4 * dim * nblk * BLK + 8 * k.size, transcendentals=0),
        name="front",
    )(lens, x, g, tab, wq, wk, wv, k, v)


def merge(blocks, out_ref, last):
    rows = PART - 16
    maxs = [b[rows : rows + 8, :] for b in blocks]
    top = functools.reduce(jnp.maximum, maxs)
    facs = [jnp.exp(m - top) for m in maxs]
    tot = functools.reduce(jnp.add, [f * b[rows + 8 : rows + 16, :] for f, b in zip(facs, blocks)])
    if last:
        inv = 1.0 / tot
        facs = [f * inv for f in facs]
    else:
        out_ref[rows : rows + 8, :] = top
        out_ref[rows + 8 : rows + 16, :] = tot
    for i in range(rows // 8):
        at = slice(8 * i, 8 * i + 8)
        out_ref[at, :] = functools.reduce(jnp.add, [b[at, :] * f[:, i : i + 1] for f, b in zip(facs, blocks)])


def tail_kernel(
    att_hbm, x_hbm, g_hbm, wo_hbm, wg_hbm, wu_hbm, wd_hbm, y_hbm,
    att_ref, g_ref, d1_buf, m_buf, r1_buf, o_buf, p_buf, z1_buf, a1_buf, h_buf, hb_buf, a_buf, p2_buf, d2_buf, s2_buf, z2_buf, a2_buf, yg_buf, yo_buf, x_buf, hid_buf,
    wo_buf, wg_buf, wu_buf, wd_buf,
    lsem, gsem, usem, dsem, osem, d1s, d1r, r1s, r1r, z1s, z1r, hs, hr, hds, hdr, d2s, d2r, z2s, z2r, ys, yr, ydr, turn,
):
    tp, sp = lax.axis_index("tp"), lax.axis_index("sp")
    core, chip = sp % 2, sp // 2
    cx, cy = chip % 2, chip // 2
    mate = {"tp": tp, "sp": 2 * chip + (1 - core)}
    plane = [(chip + k) % 4 for k in range(4)]
    plane_id = [{"tp": tp, "sp": 2 * q + core} for q in plane]
    side = tp // 2
    inside = tp * (1 - 2 * side) + 3 * side
    is_end, is_in = inside == 0, inside == 1

    def place(m):
        return m + side * (3 - 2 * m)

    near, second, far = place(1 - inside), place(2), place(3)

    def zdev(z):
        return {"tp": z, "sp": sp}

    dim = x_buf.shape[1]
    ring = wg_buf.shape[0]
    half = wd_buf.shape[1]
    nff = half // BLK
    ndn = wd_buf.shape[0]
    dcol = wd_buf.shape[2]

    me8 = pl.multiple_of(32 * sp + 8 * tp, 8)
    x_copy = pltpu.make_async_copy(x_hbm.at[pl.ds(me8, 8), :], x_buf, lsem.at[0])
    wo_copy = pltpu.make_async_copy(wo_hbm, wo_buf, lsem.at[1])

    def ff_copies(j, slot):
        at = pl.ds(pl.multiple_of(core * half + j * BLK, BLK), BLK)
        return (
            pltpu.make_async_copy(wg_hbm.at[:, at], wg_buf.at[slot], gsem.at[slot]),
            pltpu.make_async_copy(wu_hbm.at[:, at], wu_buf.at[slot], usem.at[slot]),
        )

    def dn_copy(j):
        return pltpu.make_async_copy(
            wd_hbm.at[pl.ds(pl.multiple_of(core * half, BLK), half), pl.ds(pl.multiple_of(j * dcol, dcol), dcol)], wd_buf.at[j], dsem.at[j]
        )

    att_copy = pltpu.make_async_copy(att_hbm, att_ref, lsem.at[2])
    g_copy = pltpu.make_async_copy(g_hbm, g_ref, lsem.at[3])
    att_copy.start()
    x_copy.start()
    g_copy.start()

    def prefetch_ff(lo, hi):
        for j in range(lo, min(hi, ring, nff)):
            for cp in ff_copies(j, j):
                cp.start()

    @pl.when(is_end)
    def _():
        z1_buf[2] = jnp.zeros_like(z1_buf[2])
        z2_buf[2] = jnp.zeros_like(z2_buf[2])

    bar = pltpu.get_barrier_semaphore()
    for dev in [mate] + plane_id[1:] + [zdev((tp + k) % 4) for k in (1, 2, 3)]:
        pl.semaphore_signal(bar, inc=1, device_id=dev, device_id_type=MESH)
    pl.semaphore_wait(bar, 7)

    drains = []

    def send(src, dst, ssem, rsem, dev, cond=None):
        def make():
            return pltpu.make_async_remote_copy(src_ref=src, dst_ref=dst, send_sem=ssem, recv_sem=rsem, device_id=dev, device_id_type=MESH)

        def go():
            make().start()

        def done():
            make().wait_send()

        if cond is None:
            go()
            drains.append(done)
        else:
            pl.when(cond)(go)
            drains.append(lambda: pl.when(cond)(done))

    def landed(ref, rsem):
        pltpu.make_async_copy(ref, ref, rsem).wait()

    order = [1, 2, 3, 0]
    att_copy.wait()
    wo_copy.start()
    for k in order:
        send(att_ref.at[pl.ds(4 * plane[k] + 2 * (1 - core), 2)], d1_buf.at[k], d1s.at[k], d1r.at[k], mate)
    for k in order:
        landed(d1_buf.at[k], d1r.at[k])
        for h in range(2):
            merge([att_ref.at[4 * plane[k] + 2 * core + h], d1_buf.at[k, h]], m_buf.at[k, h], False)

    @pl.when(core == 1)
    def _():
        pl.semaphore_wait(turn, 1)

    before = len(drains)
    for k in (1, 2, 3):
        send(m_buf.at[k], r1_buf.at[k - 1], r1s.at[k - 1], r1r.at[k - 1], plane_id[k])
    plane_sent = drains[before:]
    del drains[before:]

    @pl.when(core == 0)
    def _():
        for done in plane_sent:
            done()
        pl.semaphore_signal(turn, inc=1, device_id=mate, device_id_type=MESH)

    prefetch_ff(0, 2)
    for k in (1, 2, 3):
        landed(r1_buf.at[k - 1], r1r.at[k - 1])
    for h in range(2):
        merge([m_buf.at[0, h]] + [r1_buf.at[k, h] for k in range(3)], o_buf.at[pl.ds(128 * h, 128)], True)

    def rows8(z):
        return pl.ds(pl.multiple_of(8 * z, 8), 8)

    def scatter(j, cols, src, buf, agg, ss, rs):
        send(src.at[rows8(second), cols], buf.at[2 - inside, :, cols], ss.at[j, 0], rs.at[j, 2 - inside], zdev(second))
        send(src.at[rows8(far), cols], agg.at[:, cols], ss.at[j, 1], rs.at[j, 3], zdev(near), is_end)
        send(src.at[rows8(near), cols], buf.at[0, :, cols], ss.at[j, 2], rs.at[j, 0], zdev(near))

    def relay(j, cols, src, buf, agg, ss, rs):
        @pl.when(is_in)
        def _():
            landed(agg.at[:, cols], rs.at[j, 3])
            src[rows8(far), cols] = src[rows8(far), cols] + agg[:, cols]

        send(src.at[rows8(far), cols], buf.at[1, :, cols], ss.at[j, 1], rs.at[j, 1], zdev(far), is_in)

    def gathered(j, cols, src, buf, rs):
        landed(buf.at[0, :, cols], rs.at[j, 0])
        landed(buf.at[1, :, cols], rs.at[j, 1])

        @pl.when(is_in)
        def _():
            landed(buf.at[2, :, cols], rs.at[j, 2])

        return src[rows8(tp), cols] + buf[0, :, cols] + buf[1, :, cols] + buf[2, :, cols]

    o = jnp.concatenate([o_buf[pl.ds(h, 32, stride=8), :].astype(BF16) for h in range(8)], axis=1)
    wo_copy.wait()

    def proj(j, carry):
        at = pl.ds(pl.multiple_of(j * 512, 512), 512)
        p_buf[:, at] = jnp.dot(o, wo_buf[:, at], preferred_element_type=F32)
        return carry

    parts1 = [pl.ds(i * (dim // 2), dim // 2) for i in range(2)]
    for i in range(2):
        lax.fori_loop(i * (dim // 1024), (i + 1) * (dim // 1024), proj, 0)
        scatter(i, parts1[i], p_buf, z1_buf, a1_buf, z1s, z1r)
    prefetch_ff(2, ring)
    for i in range(2):
        relay(i, parts1[i], p_buf, z1_buf, a1_buf, z1s, z1r)
    for j in range(ndn // 2):
        dn_copy(j).start()
    x_copy.wait()
    g_copy.wait()
    for i in range(2):
        hid_buf[:, parts1[i]] = (x_buf[:, parts1[i]].astype(F32) + gathered(i, parts1[i], p_buf, z1_buf, z1r)).astype(BF16).astype(F32)
    hid = hid_buf[...]
    inv = lax.rsqrt(jnp.sum(hid * hid, axis=-1, keepdims=True) * (1.0 / dim) + NORM_EPS)
    mine = core * 4
    h_buf[mine + tp] = (hid * inv * g_ref[...].astype(F32).reshape(1, dim)).astype(BF16).astype(F32)

    def spread(block, ss, rs, first):
        send(block(tp), block(tp), ss(first), rs(tp), zdev(second))
        send(block(tp), block(tp), ss(first + 1), rs(tp), zdev(far), is_in)
        send(block(tp), block(tp), ss(first + 2), rs(tp), zdev(near))

    def h_block(z):
        return h_buf.at[mine + z]

    spread(h_block, lambda i: hs.at[i], lambda z: hr.at[z], 0)
    send(h_block(tp), h_block(tp), hds.at[0], hdr.at[tp], mate)
    for j in range(ndn // 2, ndn):
        dn_copy(j).start()
    for i, z in enumerate((near, second, far)):
        landed(h_block(z), hr.at[z])
        if i == 2:
            send(h_block(z), h_block(z), hs.at[3], hr.at[z], zdev(near), is_in)
        send(h_block(z), h_block(z), hds.at[1 + i], hdr.at[z], mate)
    for z in range(4):
        landed(h_buf.at[4 * (1 - core) + z], hdr.at[z])
    for i in range(4):
        hb_buf[16 * i : 16 * i + 16, :] = jnp.concatenate([h_buf[2 * i], h_buf[2 * i + 1]], axis=0).astype(BF16)

    def ff(j, carry):
        slot = lax.rem(j, ring)
        for cp in ff_copies(j, slot):
            cp.wait()
        gate = jnp.dot(hb_buf[...], wg_buf[slot], preferred_element_type=F32).astype(BF16).astype(F32)
        up = jnp.dot(hb_buf[...], wu_buf[slot], preferred_element_type=F32).astype(BF16).astype(F32)
        a_buf[:, pl.ds(pl.multiple_of(j * BLK, BLK), BLK)] = (gate * jax.nn.sigmoid(gate) * up).astype(BF16)

        @pl.when(j + ring < nff)
        def _():
            for cp in ff_copies(j + ring, slot):
                cp.start()

        return carry

    lax.fori_loop(0, nff, ff, 0)

    nc = CHUNKS
    width = dim // nc
    cols = [pl.ds(j * width, width) for j in range(nc)]
    xn = 2 * cy + (1 - cx)
    yn = 2 * (1 - cy) + cx
    dg = 2 * (1 - cy) + (1 - cx)
    xn_id, yn_id = {"tp": tp, "sp": 2 * xn + core}, {"tp": tp, "sp": 2 * yn + core}
    zorder = (tp, near, second, far)
    count = [0] * nc

    def block(j, c, z):
        return yg_buf.at[4 * (2 * c + core) + z, :, cols[j]]

    def pass_on(j, c, z, dev, rs, cond=None):
        send(block(j, c, z), block(j, c, z), ys.at[j, count[j]], rs, dev, cond)
        count[j] += 1

    def down(j):
        def one(i, carry):
            dn_copy(i).wait()
            p2_buf[:, pl.ds(pl.multiple_of(i * dcol, dcol), dcol)] = jnp.dot(a_buf[...], wd_buf[i], preferred_element_type=F32)
            return carry

        lax.fori_loop(j * ndn // nc, (j + 1) * ndn // nc, one, 0)
        send(p2_buf.at[pl.ds(pl.multiple_of(32 * (1 - core), 32), 32), cols[j]], d2_buf.at[:, cols[j]], d2s.at[j], d2r.at[j], mate)

    def pair(j):
        landed(d2_buf.at[:, cols[j]], d2r.at[j])
        s2_buf[:, cols[j]] = p2_buf[pl.ds(pl.multiple_of(32 * core, 32), 32), cols[j]] + d2_buf[:, cols[j]]
        scatter(j, cols[j], s2_buf, z2_buf, a2_buf, z2s, z2r)

    def mid(j):
        relay(j, cols[j], s2_buf, z2_buf, a2_buf, z2s, z2r)

    def own(j):
        yg_buf[4 * sp + tp, :, cols[j]] = (hid_buf[:, cols[j]] + gathered(j, cols[j], s2_buf, z2_buf, z2r)).astype(BF16).astype(F32)
        pass_on(j, chip, tp, xn_id, yr.at[j, 4 + tp])
        pass_on(j, chip, tp, yn_id, yr.at[j, 8 + tp])
        at = count[j]
        spread(lambda z: block(j, chip, z), lambda i: ys.at[j, i], lambda z: yr.at[j, z], at)
        count[j] = at + 3
        pass_on(j, chip, tp, mate, ydr.at[j, tp])

    def column(j):
        for i, z in enumerate(zorder[1:]):
            landed(block(j, chip, z), yr.at[j, z])
            if i == 2:
                pass_on(j, chip, z, zdev(near), yr.at[j, z], is_in)
            pass_on(j, chip, z, xn_id, yr.at[j, 4 + z])
            pass_on(j, chip, z, yn_id, yr.at[j, 8 + z])
            pass_on(j, chip, z, mate, ydr.at[j, z])

    def around(j):
        for i, z in enumerate(zorder):
            landed(block(j, xn, z), yr.at[j, 4 + z])
            if i % 2 == 0:
                pass_on(j, xn, z, yn_id, yr.at[j, 12 + z])
            pass_on(j, xn, z, mate, ydr.at[j, 4 + z])
            landed(block(j, yn, z), yr.at[j, 8 + z])
            if i % 2 == 1:
                pass_on(j, yn, z, xn_id, yr.at[j, 12 + z])
            pass_on(j, yn, z, mate, ydr.at[j, 8 + z])

    def across(j):
        for z in zorder:
            landed(block(j, dg, z), yr.at[j, 12 + z])
            pass_on(j, dg, z, mate, ydr.at[j, 12 + z])

    def out_copy(j):
        return pltpu.make_async_copy(yo_buf.at[:, cols[j]], y_hbm.at[:, cols[j]], osem.at[j])

    def finish(j):
        for i, c in enumerate((chip, xn, yn, dg)):
            for z in zorder:
                landed(yg_buf.at[4 * (2 * c + (1 - core)) + z, :, cols[j]], ydr.at[j, 4 * i + z])

        def out(i, carry):
            yo_buf[pl.ds(pl.multiple_of(i * 16, 16), 16), cols[j]] = jnp.concatenate([yg_buf[2 * i, :, cols[j]], yg_buf[2 * i + 1, :, cols[j]]], axis=0).astype(BF16)
            return carry

        lax.fori_loop(0, yg_buf.shape[0] // 2, out, 0)
        out_copy(j).start()

    down(0)
    for j in range(nc + 4):
        if j == 0:
            for i in range(1, nc + 1):
                if i < nc:
                    down(i)
                if i <= LEAD:
                    pair(i - 1)
                if 2 <= i <= LEAD + 1:
                    mid(i - 2)
        if j < nc:
            own(j)
        if j + LEAD < nc:
            pair(j + LEAD)
        if 1 <= j and j + LEAD - 1 < nc:
            if j <= nc:
                column(j - 1)
            mid(j + LEAD - 1)
        elif 1 <= j <= nc:
            column(j - 1)
        if 2 <= j <= nc + 1:
            around(j - 2)
        if 3 <= j <= nc + 2:
            across(j - 3)
        if 4 <= j:
            finish(j - 4)
    for done in drains:
        done()

    @pl.when(core == 1)
    def _():
        for done in plane_sent:
            done()

    for j in range(nc):
        out_copy(j).wait()


def tail(att, x, g, wo, wg, wu, wd):
    batch, dim = x.shape
    half = wg.shape[1] // 2
    ring = min(5, half // BLK)
    ndn = 8
    dma = pltpu.SemaphoreType.DMA
    return pl.pallas_call(
        tail_kernel,
        out_shape=jax.ShapeDtypeStruct((batch, dim), BF16),
        in_specs=[ANY] * 7,
        out_specs=ANY,
        scratch_shapes=[
            pltpu.VMEM(att.shape, F32),
            pltpu.VMEM((dim,), BF16),
            pltpu.VMEM((4, 2, PART, 128), F32),
            pltpu.VMEM((4, 2, PART, 128), F32),
            pltpu.VMEM((3, 2, PART, 128), F32),
            pltpu.VMEM((256, 128), F32),
            pltpu.VMEM((32, dim), F32),
            pltpu.VMEM((3, 8, dim), F32),
            pltpu.VMEM((8, dim), F32),
            pltpu.VMEM((8, 8, dim), F32),
            pltpu.VMEM((64, dim), BF16),
            pltpu.VMEM((64, half), BF16),
            pltpu.VMEM((64, dim), F32),
            pltpu.VMEM((32, dim), F32),
            pltpu.VMEM((32, dim), F32),
            pltpu.VMEM((3, 8, dim), F32),
            pltpu.VMEM((8, dim), F32),
            pltpu.VMEM((batch // 8, 8, dim), F32),
            pltpu.VMEM((batch, dim), BF16),
            pltpu.VMEM((8, dim), BF16),
            pltpu.VMEM((8, dim), F32),
            pltpu.VMEM(wo.shape, BF16),
            pltpu.VMEM((ring, dim, BLK), BF16),
            pltpu.VMEM((ring, dim, BLK), BF16),
            pltpu.VMEM((ndn, half, dim // ndn), BF16),
            dma((4,)), dma((ring,)), dma((ring,)), dma((ndn,)), dma((CHUNKS,)),
            dma((4,)), dma((4,)), dma((3,)), dma((3,)), dma((2, 3)), dma((2, 4)),
            dma((4,)), dma((4,)), dma((4,)), dma((4,)), dma((CHUNKS,)), dma((CHUNKS,)), dma((CHUNKS, 3)), dma((CHUNKS, 4)),
            dma((CHUNKS, 34)), dma((CHUNKS, 16)), dma((CHUNKS, 16)), pltpu.SemaphoreType.REGULAR,
        ],
        compiler_params=pltpu.CompilerParams(collective_id=0, has_side_effects=True, vmem_limit_bytes=63_000_000),
        cost_estimate=pl.CostEstimate(flops=2 * 64 * dim * half * 3, bytes_accessed=6 * dim * half, transcendentals=0),
        name="tail",
    )(att, x, g, wo, wg, wu, wd)


def land_kernel(y_hbm, out_hbm, buf, isem, osem):
    n = isem.shape[0]
    rows = buf.shape[0] // n
    ats = [pl.ds(i * rows, rows) for i in range(n)]
    ins = [pltpu.make_async_copy(y_hbm.at[at, :], buf.at[at, :], isem.at[i]) for i, at in enumerate(ats)]
    outs = [pltpu.make_async_copy(buf.at[at, :], out_hbm.at[at, :], osem.at[i]) for i, at in enumerate(ats)]
    for cp in ins:
        cp.start()
    for a, b in zip(ins, outs):
        a.wait()
        b.start()
    for cp in outs:
        cp.wait()


def land(y):
    return pl.pallas_call(
        land_kernel,
        out_shape=jax.ShapeDtypeStruct(y.shape, y.dtype),
        in_specs=[ANY],
        out_specs=ANY,
        scratch_shapes=[pltpu.VMEM(y.shape, y.dtype), pltpu.SemaphoreType.DMA((4,)), pltpu.SemaphoreType.DMA((4,))],
        compiler_params=pltpu.CompilerParams(vmem_limit_bytes=63_000_000),
        name="land",
    )(y)


def rope_table(length):
    freq = np.power(ROPE_BASE, np.arange(64) * (-2.0 / 128)).astype(np.float32)
    angles = (np.arange(length, dtype=np.float32)[:, None] * freq).astype(np.float64)
    cos, sin = np.cos(angles), np.sin(angles)
    return jnp.asarray(np.concatenate([cos, cos, -sin, sin], axis=1), F32)


def solution(mesh):
    cache_spec = P(None, "sp", "tp", None)
    col_spec = P(None, "tp")
    row_spec = P("tp", None)
    full_spec = P()

    def local_step(x_tok, seq_lens, k_blk, v_blk, g_attn, wq, wk, wv, wo, g_mlp, wg, wu, wd):
        batch = x_tok.shape[0]
        shape = (batch, 8, 16, 128)
        k_out, v_out, att = front(seq_lens, x_tok, g_attn, rope_table(k_blk.shape[1] * mesh.shape["sp"]), wq, wk, wv, k_blk.reshape(shape), v_blk.reshape(shape))
        y = tail(att, x_tok, g_mlp, wo, wg, wu, wd)
        return land(y), k_out.reshape(k_blk.shape), v_out.reshape(v_blk.shape)

    return jax.shard_map(local_step, mesh=mesh, in_specs=(full_spec, full_spec, cache_spec, cache_spec, full_spec, col_spec, col_spec, col_spec, row_spec, full_spec, col_spec, col_spec, row_spec), out_specs=(full_spec, cache_spec, cache_spec), check_vma=False)
```

```python
import functools

import jax
import jax.numpy as jnp
import numpy as np
from jax import lax
from jax.experimental import pallas as pl
from jax.experimental.pallas import tpu as pltpu
from jax.sharding import PartitionSpec as P

ROPE_BASE = 500000.0
NORM_EPS = 1e-5
MESH = pl.DeviceIdType.MESH
F32 = jnp.float32
BF16 = jnp.bfloat16
ANY = pl.BlockSpec(memory_space=pl.ANY)
VMEM = pl.BlockSpec(memory_space=pltpu.VMEM)
NEG = -1e30
BLK = 256
CHUNKS = 8
LEAD = 5
LAGS = (2, 4, 5, 6)
PART = 144


def front_kernel(
    lens_ref, x_hbm, g_hbm, tab_hbm, wq_hbm, wk_hbm, wv_hbm, k_hbm, v_hbm, ko_hbm, vo_hbm, out_hbm,
    x_buf, g_buf, tab_buf, rot_buf, u_buf, w_buf, k_buf, v_buf, q_buf, kn_buf, vn_buf, out_buf, xsem, wsem, kvsem, osem,
):
    rows, dim = x_buf.shape
    wide = 2 * BLK
    nq = wq_hbm.shape[1] // wide
    heads = wq_hbm.shape[1] // 128
    nreq = 32
    groups = rows // nreq
    base = lax.axis_index("sp") * 64

    x_copy = pltpu.make_async_copy(x_hbm, x_buf, xsem.at[0])
    g_copy = pltpu.make_async_copy(g_hbm, g_buf, xsem.at[1])
    tab_copy = pltpu.make_async_copy(tab_hbm, tab_buf, xsem.at[2])
    g_copy.start()
    x_copy.start()
    tab_copy.start()
    w_copies = [[pltpu.make_async_copy(wq_hbm.at[:, pl.ds(i * wide, wide)], w_buf.at[i], wsem.at[i])] for i in range(nq)]
    w_copies.append([
        pltpu.make_async_copy(wk_hbm, w_buf.at[nq, :, pl.ds(0, BLK)], wsem.at[nq]),
        pltpu.make_async_copy(wv_hbm, w_buf.at[nq, :, pl.ds(BLK, BLK)], wsem.at[nq + 1]),
    ])
    w_copies[0][0].start()

    def cache_copies(g):
        at = pl.ds(g * nreq, nreq)
        return (
            pltpu.make_async_copy(k_hbm.at[at], k_buf.at[at], kvsem.at[0, g]),
            pltpu.make_async_copy(v_hbm.at[at], v_buf.at[at], kvsem.at[1, g]),
        )

    def out_copies(g):
        at = pl.ds(g * nreq, nreq)
        return (
            pltpu.make_async_copy(k_buf.at[at], ko_hbm.at[at], osem.at[0, g]),
            pltpu.make_async_copy(v_buf.at[at], vo_hbm.at[at], osem.at[1, g]),
        )

    def part_copy(g):
        return pltpu.make_async_copy(out_buf.at[pl.ds(2 * g, 2)], out_hbm.at[pl.ds(2 * g, 2)], osem.at[2, g])

    def fetch(lo, hi):
        for g in range(lo, hi):
            for cp in cache_copies(g):
                cp.start()

    g_copy.wait()
    gain = g_buf[...].astype(F32).reshape(1, dim)
    x_copy.wait()
    for cps in w_copies[1:]:
        for cp in cps:
            cp.start()

    def norm(i, carry):
        at = pl.ds(pl.multiple_of(i * 16, 16), 16)
        xf = x_buf[at, :].astype(F32)
        inv = lax.rsqrt(jnp.sum(xf * xf, axis=-1, keepdims=True) * (1.0 / dim) + NORM_EPS)
        u_buf[at, :] = (xf * inv * gain).astype(BF16)
        return carry

    lax.fori_loop(0, rows // 16, norm, 0, unroll=2)
    tab_copy.wait()

    def angle(i, carry):
        rot_buf[pl.ds(i, 1), :] = tab_buf[pl.ds(lens_ref[i], 1), :]
        return carry

    lax.fori_loop(0, rows, angle, 0, unroll=16)
    cosv = rot_buf[:, :128]
    sinv = rot_buf[:, 128:]

    def rope(h):
        h = h.astype(BF16).astype(F32)
        return (h * cosv + pltpu.roll(h, 64, 1) * sinv).astype(BF16).astype(F32)

    for i in range(nq + 1):
        for cp in w_copies[i]:
            cp.wait()
        fetch(groups * i // (nq + 1), groups * (i + 1) // (nq + 1))
        prod = jnp.dot(u_buf[...], w_buf[i], preferred_element_type=F32)
        for s in range(4):
            part = prod[:, s * 128 : (s + 1) * 128]
            if i < nq:
                q_buf[pl.ds(4 * i + s, rows, stride=heads), :] = rope(part)
            elif s < 2:
                kn_buf[pl.ds(s, rows, stride=2), :] = rope(part)
            else:
                vn_buf[pl.ds(s - 2, rows, stride=2), :] = part.astype(BF16).astype(F32)

    lane = lax.broadcasted_iota(jnp.int32, (8, 128), 1)
    head = lax.broadcasted_iota(jnp.int32, (8, 128), 0)
    match = (lane % 2) == (head // 4)
    lane_pos = jnp.where(match, lane // 2, 1 << 20)
    row16 = lax.broadcasted_iota(jnp.int32, (16, 128), 0)
    scale = 128.0**-0.5
    zero = jnp.zeros((8, 128), BF16)

    def insert(b, c_buf, n_buf, blk, off):
        row0 = jnp.broadcast_to(n_buf[pl.ds(2 * b, 1), :], (16, 128))
        row1 = jnp.broadcast_to(n_buf[pl.ds(2 * b + 1, 1), :], (16, 128))
        new = jnp.where(row16 == off, row0, row1)
        old = c_buf[b, blk].astype(F32)
        c_buf[b, blk] = jnp.where((row16 == off) | (row16 == off + 1), new, old).astype(BF16)

    def group(g, carry):
        for cp in cache_copies(g):
            cp.wait()

        def put(i, c):
            b = g * nreq + i
            pos = lens_ref[b] - base
            inside = (pos >= 0) & (pos < 64)
            at = jnp.where(inside, pos, 0)
            off = jnp.where(inside, 2 * (at % 8), -8)
            insert(b, k_buf, kn_buf, at // 8, off)
            insert(b, v_buf, vn_buf, at // 8, off)
            return c

        lax.fori_loop(0, nreq, put, 0, unroll=8)
        for cp in out_copies(g):
            cp.start()

        first = g * nreq
        scores = []
        for p in range(16):
            b = first + 2 * p
            keys = k_buf[pl.ds(b, 2)].reshape(256, 128)
            qp = q_buf[pl.ds(pl.multiple_of(b * 8, 16), 16), :].astype(BF16)
            scores.append(lax.dot_general(qp, keys, (((1,), (1,)), ((), ())), preferred_element_type=F32))
        for h in range(2):
            half = g * 2 + h
            wts = []
            stm, stl = jnp.zeros((8, 128), F32), jnp.ones((8, 128), F32)
            for p in range(8):
                for j in range(2):
                    s = scores[8 * h + p][8 * j : 8 * j + 8, 128 * j : 128 * j + 128] * scale
                    valid = lane_pos <= lens_ref[first + 16 * h + 2 * p + j] - base
                    m = jnp.max(jnp.where(valid, s, NEG), axis=1, keepdims=True)
                    w = jnp.where(valid, jnp.exp(s - m), 0.0)
                    here = lane == 2 * p + j
                    stm = jnp.where(here, m, stm)
                    stl = jnp.where(here, jnp.sum(w, axis=1, keepdims=True), stl)
                    wts.append(w.astype(BF16))
            out_buf[half, 128:136, :] = stm
            out_buf[half, 136:144, :] = stl
            for p in range(8):
                wp = jnp.concatenate([jnp.concatenate([wts[2 * p], zero], axis=1), jnp.concatenate([zero, wts[2 * p + 1]], axis=1)], axis=0)
                vals = v_buf[pl.ds(first + 16 * h + 2 * p, 2)].reshape(256, 128)
                out_buf[half, 16 * p : 16 * p + 16, :] = jnp.dot(wp, vals, preferred_element_type=F32)
        part_copy(g).start()
        return carry

    lax.fori_loop(0, groups, group, 0)
    for g in range(groups):
        for cp in out_copies(g):
            cp.wait()
        part_copy(g).wait()


def front(lens, x, g, tab, wq, wk, wv, k, v):
    rows, dim = x.shape
    heads = wq.shape[1] // 128
    nblk = wq.shape[1] // (2 * BLK) + 1
    groups = rows // 32
    dma = pltpu.SemaphoreType.DMA
    return pl.pallas_call(
        front_kernel,
        out_shape=(
            jax.ShapeDtypeStruct(k.shape, BF16),
            jax.ShapeDtypeStruct(v.shape, BF16),
            jax.ShapeDtypeStruct((2 * groups, PART, 128), F32),
        ),
        in_specs=[pl.BlockSpec(memory_space=pltpu.SMEM)] + [ANY] * 8,
        out_specs=(ANY, ANY, ANY),
        scratch_shapes=[
            pltpu.VMEM((rows, dim), BF16),
            pltpu.VMEM((dim,), BF16),
            pltpu.VMEM(tab.shape, F32),
            pltpu.VMEM((rows, 256), F32),
            pltpu.VMEM((rows, dim), BF16),
            pltpu.VMEM((nblk, dim, 2 * BLK), BF16),
            pltpu.VMEM(k.shape, BF16),
            pltpu.VMEM(v.shape, BF16),
            pltpu.VMEM((rows * heads, 128), F32),
            pltpu.VMEM((rows * 2, 128), F32),
            pltpu.VMEM((rows * 2, 128), F32),
            pltpu.VMEM((2 * groups, PART, 128), F32),
            dma((3,)),
            dma((nblk + 1,)),
            dma((2, groups)),
            dma((3, groups)),
        ],
        compiler_params=pltpu.CompilerParams(vmem_limit_bytes=63_000_000),
        cost_estimate=pl.CostEstimate(flops=4 * rows * dim * nblk * BLK, bytes_accessed=4 * dim * nblk * BLK + 8 * k.size, transcendentals=0),
        name="front",
    )(lens, x, g, tab, wq, wk, wv, k, v)


def merge(blocks, out_ref, last):
    rows = PART - 16
    maxs = [b[rows : rows + 8, :] for b in blocks]
    top = functools.reduce(jnp.maximum, maxs)
    facs = [jnp.exp(m - top) for m in maxs]
    tot = functools.reduce(jnp.add, [f * b[rows + 8 : rows + 16, :] for f, b in zip(facs, blocks)])
    if last:
        inv = 1.0 / tot
        facs = [f * inv for f in facs]
    else:
        out_ref[rows : rows + 8, :] = top
        out_ref[rows + 8 : rows + 16, :] = tot
    for i in range(rows // 8):
        at = slice(8 * i, 8 * i + 8)
        out_ref[at, :] = functools.reduce(jnp.add, [b[at, :] * f[:, i : i + 1] for f, b in zip(facs, blocks)])


def tail_kernel(
    att_hbm, x_hbm, g_hbm, wo_hbm, wg_hbm, wu_hbm, wd_hbm, y_hbm,
    att_ref, g_ref, d1_buf, m_buf, r1_buf, o_buf, p_buf, z1_buf, a1_buf, h_buf, hb_buf, a_buf, p2_buf, d2_buf, s2_buf, z2_buf, a2_buf, yg_buf, yo_buf, x_buf, hid_buf,
    wo_buf, wg_buf, wu_buf, wd_buf,
    lsem, gsem, usem, dsem, osem, d1s, d1r, r1s, r1r, z1s, z1r, hs, hr, hds, hdr, d2s, d2r, z2s, z2r, ys, yr, ydr, turn,
):
    tp, sp = lax.axis_index("tp"), lax.axis_index("sp")
    core, chip = sp % 2, sp // 2
    cx, cy = chip % 2, chip // 2
    mate = {"tp": tp, "sp": 2 * chip + (1 - core)}
    plane = [(chip + k) % 4 for k in range(4)]
    plane_id = [{"tp": tp, "sp": 2 * q + core} for q in plane]
    side = tp // 2
    inside = tp * (1 - 2 * side) + 3 * side
    is_end, is_in = inside == 0, inside == 1

    def place(m):
        return m + side * (3 - 2 * m)

    near, second, far = place(1 - inside), place(2), place(3)

    def zdev(z):
        return {"tp": z, "sp": sp}

    dim = x_buf.shape[1]
    ring = wg_buf.shape[0]
    half = wd_buf.shape[1]
    nff = half // BLK
    ndn = wd_buf.shape[0]
    dcol = wd_buf.shape[2]

    me8 = pl.multiple_of(32 * sp + 8 * tp, 8)
    x_copy = pltpu.make_async_copy(x_hbm.at[pl.ds(me8, 8), :], x_buf, lsem.at[0])
    wo_copy = pltpu.make_async_copy(wo_hbm, wo_buf, lsem.at[1])

    def ff_copies(j, slot):
        at = pl.ds(pl.multiple_of(core * half + j * BLK, BLK), BLK)
        return (
            pltpu.make_async_copy(wg_hbm.at[:, at], wg_buf.at[slot], gsem.at[slot]),
            pltpu.make_async_copy(wu_hbm.at[:, at], wu_buf.at[slot], usem.at[slot]),
        )

    def dn_copy(j):
        return pltpu.make_async_copy(
            wd_hbm.at[pl.ds(pl.multiple_of(core * half, BLK), half), pl.ds(pl.multiple_of(j * dcol, dcol), dcol)], wd_buf.at[j], dsem.at[j]
        )

    att_copy = pltpu.make_async_copy(att_hbm, att_ref, lsem.at[2])
    g_copy = pltpu.make_async_copy(g_hbm, g_ref, lsem.at[3])
    att_copy.start()
    x_copy.start()
    g_copy.start()

    def prefetch_ff(lo, hi):
        for j in range(lo, min(hi, ring, nff)):
            for cp in ff_copies(j, j):
                cp.start()

    @pl.when(is_end)
    def _():
        z1_buf[2] = jnp.zeros_like(z1_buf[2])
        z2_buf[2] = jnp.zeros_like(z2_buf[2])

    bar = pltpu.get_barrier_semaphore()
    for dev in [mate] + plane_id[1:] + [zdev((tp + k) % 4) for k in (1, 2, 3)]:
        pl.semaphore_signal(bar, inc=1, device_id=dev, device_id_type=MESH)
    pl.semaphore_wait(bar, 7)

    drains = []

    def send(src, dst, ssem, rsem, dev, cond=None):
        def make():
            return pltpu.make_async_remote_copy(src_ref=src, dst_ref=dst, send_sem=ssem, recv_sem=rsem, device_id=dev, device_id_type=MESH)

        def go():
            make().start()

        def done():
            make().wait_send()

        if cond is None:
            go()
            drains.append(done)
        else:
            pl.when(cond)(go)
            drains.append(lambda: pl.when(cond)(done))

    def landed(ref, rsem):
        pltpu.make_async_copy(ref, ref, rsem).wait()

    order = [1, 2, 3, 0]
    att_copy.wait()
    wo_copy.start()
    for k in order:
        send(att_ref.at[pl.ds(4 * plane[k] + 2 * (1 - core), 2)], d1_buf.at[k], d1s.at[k], d1r.at[k], mate)
    for k in order:
        landed(d1_buf.at[k], d1r.at[k])
        for h in range(2):
            merge([att_ref.at[4 * plane[k] + 2 * core + h], d1_buf.at[k, h]], m_buf.at[k, h], False)

    @pl.when(core == 1)
    def _():
        pl.semaphore_wait(turn, 1)

    before = len(drains)
    for k in (1, 2, 3):
        send(m_buf.at[k], r1_buf.at[k - 1], r1s.at[k - 1], r1r.at[k - 1], plane_id[k])
    plane_sent = drains[before:]
    del drains[before:]

    @pl.when(core == 0)
    def _():
        for done in plane_sent:
            done()
        pl.semaphore_signal(turn, inc=1, device_id=mate, device_id_type=MESH)

    prefetch_ff(0, 2)
    for k in (1, 2, 3):
        landed(r1_buf.at[k - 1], r1r.at[k - 1])
    for h in range(2):
        merge([m_buf.at[0, h]] + [r1_buf.at[k, h] for k in range(3)], o_buf.at[pl.ds(128 * h, 128)], True)

    def rows8(z):
        return pl.ds(pl.multiple_of(8 * z, 8), 8)

    def scatter(j, cols, src, buf, agg, ss, rs):
        send(src.at[rows8(second), cols], buf.at[2 - inside, :, cols], ss.at[j, 0], rs.at[j, 2 - inside], zdev(second))
        send(src.at[rows8(far), cols], agg.at[:, cols], ss.at[j, 1], rs.at[j, 3], zdev(near), is_end)
        send(src.at[rows8(near), cols], buf.at[0, :, cols], ss.at[j, 2], rs.at[j, 0], zdev(near))

    def relay(j, cols, src, buf, agg, ss, rs):
        @pl.when(is_in)
        def _():
            landed(agg.at[:, cols], rs.at[j, 3])
            src[rows8(far), cols] = src[rows8(far), cols] + agg[:, cols]

        send(src.at[rows8(far), cols], buf.at[1, :, cols], ss.at[j, 1], rs.at[j, 1], zdev(far), is_in)

    def gathered(j, cols, src, buf, rs):
        landed(buf.at[0, :, cols], rs.at[j, 0])
        landed(buf.at[1, :, cols], rs.at[j, 1])

        @pl.when(is_in)
        def _():
            landed(buf.at[2, :, cols], rs.at[j, 2])

        return src[rows8(tp), cols] + buf[0, :, cols] + buf[1, :, cols] + buf[2, :, cols]

    o = jnp.concatenate([o_buf[pl.ds(h, 32, stride=8), :].astype(BF16) for h in range(8)], axis=1)
    wo_copy.wait()

    def proj(j, carry):
        at = pl.ds(pl.multiple_of(j * 512, 512), 512)
        p_buf[:, at] = jnp.dot(o, wo_buf[:, at], preferred_element_type=F32)
        return carry

    parts1 = [pl.ds(i * (dim // 2), dim // 2) for i in range(2)]
    for i in range(2):
        lax.fori_loop(i * (dim // 1024), (i + 1) * (dim // 1024), proj, 0)
        scatter(i, parts1[i], p_buf, z1_buf, a1_buf, z1s, z1r)
    prefetch_ff(2, ring)
    for i in range(2):
        relay(i, parts1[i], p_buf, z1_buf, a1_buf, z1s, z1r)
    for j in range(ndn // 2):
        dn_copy(j).start()
    x_copy.wait()
    g_copy.wait()
    for i in range(2):
        hid_buf[:, parts1[i]] = (x_buf[:, parts1[i]].astype(F32) + gathered(i, parts1[i], p_buf, z1_buf, z1r)).astype(BF16).astype(F32)
    hid = hid_buf[...]
    inv = lax.rsqrt(jnp.sum(hid * hid, axis=-1, keepdims=True) * (1.0 / dim) + NORM_EPS)
    mine = core * 4
    h_buf[mine + tp] = (hid * inv * g_ref[...].astype(F32).reshape(1, dim)).astype(BF16).astype(F32)

    def spread(block, ss, rs, first):
        send(block(tp), block(tp), ss(first), rs(tp), zdev(second))
        send(block(tp), block(tp), ss(first + 1), rs(tp), zdev(far), is_in)
        send(block(tp), block(tp), ss(first + 2), rs(tp), zdev(near))

    def h_block(z):
        return h_buf.at[mine + z]

    spread(h_block, lambda i: hs.at[i], lambda z: hr.at[z], 0)
    send(h_block(tp), h_block(tp), hds.at[0], hdr.at[tp], mate)
    for j in range(ndn // 2, ndn):
        dn_copy(j).start()
    for i, z in enumerate((near, second, far)):
        landed(h_block(z), hr.at[z])
        if i == 2:
            send(h_block(z), h_block(z), hs.at[3], hr.at[z], zdev(near), is_in)
        send(h_block(z), h_block(z), hds.at[1 + i], hdr.at[z], mate)
    for z in range(4):
        landed(h_buf.at[4 * (1 - core) + z], hdr.at[z])
    for i in range(4):
        hb_buf[16 * i : 16 * i + 16, :] = jnp.concatenate([h_buf[2 * i], h_buf[2 * i + 1]], axis=0).astype(BF16)

    def ff(j, carry):
        slot = lax.rem(j, ring)
        for cp in ff_copies(j, slot):
            cp.wait()
        gate = jnp.dot(hb_buf[...], wg_buf[slot], preferred_element_type=F32).astype(BF16).astype(F32)
        up = jnp.dot(hb_buf[...], wu_buf[slot], preferred_element_type=F32).astype(BF16).astype(F32)
        a_buf[:, pl.ds(pl.multiple_of(j * BLK, BLK), BLK)] = (gate * jax.nn.sigmoid(gate) * up).astype(BF16)

        @pl.when(j + ring < nff)
        def _():
            for cp in ff_copies(j + ring, slot):
                cp.start()

        return carry

    lax.fori_loop(0, nff, ff, 0)

    nc = CHUNKS
    width = dim // nc
    cols = [pl.ds(j * width, width) for j in range(nc)]
    xn = 2 * cy + (1 - cx)
    yn = 2 * (1 - cy) + cx
    dg = 2 * (1 - cy) + (1 - cx)
    xn_id, yn_id = {"tp": tp, "sp": 2 * xn + core}, {"tp": tp, "sp": 2 * yn + core}
    zorder = (tp, near, second, far)
    count = [0] * nc

    def block(j, c, z):
        return yg_buf.at[4 * (2 * c + core) + z, :, cols[j]]

    def pass_on(j, c, z, dev, rs, cond=None):
        send(block(j, c, z), block(j, c, z), ys.at[j, count[j]], rs, dev, cond)
        count[j] += 1

    def down(j):
        def one(i, carry):
            dn_copy(i).wait()
            p2_buf[:, pl.ds(pl.multiple_of(i * dcol, dcol), dcol)] = jnp.dot(a_buf[...], wd_buf[i], preferred_element_type=F32)
            return carry

        lax.fori_loop(j * ndn // nc, (j + 1) * ndn // nc, one, 0)
        send(p2_buf.at[pl.ds(pl.multiple_of(32 * (1 - core), 32), 32), cols[j]], d2_buf.at[:, cols[j]], d2s.at[j], d2r.at[j], mate)

    def pair(j):
        landed(d2_buf.at[:, cols[j]], d2r.at[j])
        s2_buf[:, cols[j]] = p2_buf[pl.ds(pl.multiple_of(32 * core, 32), 32), cols[j]] + d2_buf[:, cols[j]]
        scatter(j, cols[j], s2_buf, z2_buf, a2_buf, z2s, z2r)

    def mid(j):
        relay(j, cols[j], s2_buf, z2_buf, a2_buf, z2s, z2r)

    def own(j):
        yg_buf[4 * sp + tp, :, cols[j]] = (hid_buf[:, cols[j]] + gathered(j, cols[j], s2_buf, z2_buf, z2r)).astype(BF16).astype(F32)
        pass_on(j, chip, tp, xn_id, yr.at[j, 4 + tp])
        pass_on(j, chip, tp, yn_id, yr.at[j, 8 + tp])
        at = count[j]
        spread(lambda z: block(j, chip, z), lambda i: ys.at[j, i], lambda z: yr.at[j, z], at)
        count[j] = at + 3

    def four(j, c, which):
        return yg_buf.at[pl.ds(4 * (2 * c + which), 4), :, cols[j]]

    def hand_over(j, c, i):
        send(four(j, c, core), four(j, c, core), ys.at[j, count[j]], ydr.at[j, i], mate)
        count[j] += 1

    def column(j):
        for i, z in enumerate(zorder[1:]):
            landed(block(j, chip, z), yr.at[j, z])
            if i == 2:
                pass_on(j, chip, z, zdev(near), yr.at[j, z], is_in)
            pass_on(j, chip, z, xn_id, yr.at[j, 4 + z])
            pass_on(j, chip, z, yn_id, yr.at[j, 8 + z])
        hand_over(j, chip, 0)

    def around(j):
        for i, z in enumerate(zorder):
            landed(block(j, xn, z), yr.at[j, 4 + z])
            if i % 2 == 0:
                pass_on(j, xn, z, yn_id, yr.at[j, 12 + z])
            landed(block(j, yn, z), yr.at[j, 8 + z])
            if i % 2 == 1:
                pass_on(j, yn, z, xn_id, yr.at[j, 12 + z])
        hand_over(j, xn, 1)
        hand_over(j, yn, 2)

    def across(j):
        for z in zorder:
            landed(block(j, dg, z), yr.at[j, 12 + z])
        hand_over(j, dg, 3)

    def out_copy(j):
        return pltpu.make_async_copy(yo_buf.at[:, cols[j]], y_hbm.at[:, cols[j]], osem.at[j])

    def finish(j):
        for i, c in enumerate((chip, xn, yn, dg)):
            landed(four(j, c, 1 - core), ydr.at[j, i])

        def out(i, carry):
            yo_buf[pl.ds(pl.multiple_of(i * 16, 16), 16), cols[j]] = jnp.concatenate([yg_buf[2 * i, :, cols[j]], yg_buf[2 * i + 1, :, cols[j]]], axis=0).astype(BF16)
            return carry

        lax.fori_loop(0, yg_buf.shape[0] // 2, out, 0)
        out_copy(j).start()

    down(0)
    for i in range(1, max(nc, LEAD + 2)):
        if i < nc:
            down(i)
        if i <= LEAD:
            pair(i - 1)
        if 2 <= i <= LEAD + 1:
            mid(i - 2)
    stages = [(0, own), (-LEAD, pair), (LAGS[0], column), (1 - LEAD, mid), (LAGS[1], around), (LAGS[2], across), (LAGS[3], finish)]
    for t in range(nc + LAGS[3]):
        for lag, stage in stages:
            j = t - lag
            if j < nc and (j >= 0 if lag >= 0 else j >= LEAD):
                stage(j)
    for done in drains:
        done()

    @pl.when(core == 1)
    def _():
        for done in plane_sent:
            done()

    for j in range(nc):
        out_copy(j).wait()


def tail(att, x, g, wo, wg, wu, wd):
    batch, dim = x.shape
    half = wg.shape[1] // 2
    ring = min(5, half // BLK)
    ndn = 8
    dma = pltpu.SemaphoreType.DMA
    return pl.pallas_call(
        tail_kernel,
        out_shape=jax.ShapeDtypeStruct((batch, dim), BF16),
        in_specs=[ANY] * 7,
        out_specs=ANY,
        scratch_shapes=[
            pltpu.VMEM(att.shape, F32),
            pltpu.VMEM((dim,), BF16),
            pltpu.VMEM((4, 2, PART, 128), F32),
            pltpu.VMEM((4, 2, PART, 128), F32),
            pltpu.VMEM((3, 2, PART, 128), F32),
            pltpu.VMEM((256, 128), F32),
            pltpu.VMEM((32, dim), F32),
            pltpu.VMEM((3, 8, dim), F32),
            pltpu.VMEM((8, dim), F32),
            pltpu.VMEM((8, 8, dim), F32),
            pltpu.VMEM((64, dim), BF16),
            pltpu.VMEM((64, half), BF16),
            pltpu.VMEM((64, dim), F32),
            pltpu.VMEM((32, dim), F32),
            pltpu.VMEM((32, dim), F32),
            pltpu.VMEM((3, 8, dim), F32),
            pltpu.VMEM((8, dim), F32),
            pltpu.VMEM((batch // 8, 8, dim), F32),
            pltpu.VMEM((batch, dim), BF16),
            pltpu.VMEM((8, dim), BF16),
            pltpu.VMEM((8, dim), F32),
            pltpu.VMEM(wo.shape, BF16),
            pltpu.VMEM((ring, dim, BLK), BF16),
            pltpu.VMEM((ring, dim, BLK), BF16),
            pltpu.VMEM((ndn, half, dim // ndn), BF16),
            dma((4,)), dma((ring,)), dma((ring,)), dma((ndn,)), dma((CHUNKS,)),
            dma((4,)), dma((4,)), dma((3,)), dma((3,)), dma((2, 3)), dma((2, 4)),
            dma((4,)), dma((4,)), dma((4,)), dma((4,)), dma((CHUNKS,)), dma((CHUNKS,)), dma((CHUNKS, 3)), dma((CHUNKS, 4)),
            dma((CHUNKS, 22)), dma((CHUNKS, 16)), dma((CHUNKS, 4)), pltpu.SemaphoreType.REGULAR,
        ],
        compiler_params=pltpu.CompilerParams(collective_id=0, has_side_effects=True, vmem_limit_bytes=63_000_000),
        cost_estimate=pl.CostEstimate(flops=2 * 64 * dim * half * 3, bytes_accessed=6 * dim * half, transcendentals=0),
        name="tail",
    )(att, x, g, wo, wg, wu, wd)


def land_kernel(y_hbm, out_hbm, buf, isem, osem):
    n = isem.shape[0]
    rows = buf.shape[0] // n
    ats = [pl.ds(i * rows, rows) for i in range(n)]
    ins = [pltpu.make_async_copy(y_hbm.at[at, :], buf.at[at, :], isem.at[i]) for i, at in enumerate(ats)]
    outs = [pltpu.make_async_copy(buf.at[at, :], out_hbm.at[at, :], osem.at[i]) for i, at in enumerate(ats)]
    for cp in ins:
        cp.start()
    for a, b in zip(ins, outs):
        a.wait()
        b.start()
    for cp in outs:
        cp.wait()


def land(y):
    return pl.pallas_call(
        land_kernel,
        out_shape=jax.ShapeDtypeStruct(y.shape, y.dtype),
        in_specs=[ANY],
        out_specs=ANY,
        scratch_shapes=[pltpu.VMEM(y.shape, y.dtype), pltpu.SemaphoreType.DMA((4,)), pltpu.SemaphoreType.DMA((4,))],
        compiler_params=pltpu.CompilerParams(vmem_limit_bytes=63_000_000),
        name="land",
    )(y)


def rope_table(length):
    freq = np.power(ROPE_BASE, np.arange(64) * (-2.0 / 128)).astype(np.float32)
    angles = (np.arange(length, dtype=np.float32)[:, None] * freq).astype(np.float64)
    cos, sin = np.cos(angles), np.sin(angles)
    return jnp.asarray(np.concatenate([cos, cos, -sin, sin], axis=1), F32)


def solution(mesh):
    cache_spec = P(None, "sp", "tp", None)
    col_spec = P(None, "tp")
    row_spec = P("tp", None)
    full_spec = P()

    def local_step(x_tok, seq_lens, k_blk, v_blk, g_attn, wq, wk, wv, wo, g_mlp, wg, wu, wd):
        batch = x_tok.shape[0]
        shape = (batch, 8, 16, 128)
        k_out, v_out, att = front(seq_lens, x_tok, g_attn, rope_table(k_blk.shape[1] * mesh.shape["sp"]), wq, wk, wv, k_blk.reshape(shape), v_blk.reshape(shape))
        y = tail(att, x_tok, g_mlp, wo, wg, wu, wd)
        return land(y), k_out.reshape(k_blk.shape), v_out.reshape(v_blk.shape)

    return jax.shard_map(local_step, mesh=mesh, in_specs=(full_spec, full_spec, cache_spec, cache_spec, full_spec, col_spec, col_spec, col_spec, row_spec, full_spec, col_spec, col_spec, row_spec), out_specs=(full_spec, cache_spec, cache_spec), check_vma=False)
```

```python
import functools

import jax
import jax.numpy as jnp
import numpy as np
from jax import lax
from jax.experimental import pallas as pl
from jax.experimental.pallas import tpu as pltpu
from jax.sharding import PartitionSpec as P

ROPE_BASE = 500000.0
NORM_EPS = 1e-5
MESH = pl.DeviceIdType.MESH
F32 = jnp.float32
BF16 = jnp.bfloat16
ANY = pl.BlockSpec(memory_space=pl.ANY)
VMEM = pl.BlockSpec(memory_space=pltpu.VMEM)
NEG = -1e30
BLK = 256
CHUNKS = 4
LEAD = 3
LAGS = (1, 2, 3, 4)
PART = 144


def front_kernel(
    lens_ref, x_hbm, g_hbm, tab_hbm, wq_hbm, wk_hbm, wv_hbm, k_hbm, v_hbm, ko_hbm, vo_hbm, out_hbm,
    x_buf, g_buf, tab_buf, rot_buf, u_buf, w_buf, k_buf, v_buf, q_buf, kn_buf, vn_buf, out_buf, xsem, wsem, kvsem, osem,
):
    rows, dim = x_buf.shape
    wide = 2 * BLK
    nq = wq_hbm.shape[1] // wide
    heads = wq_hbm.shape[1] // 128
    nreq = 32
    groups = rows // nreq
    base = lax.axis_index("sp") * 64

    x_copy = pltpu.make_async_copy(x_hbm, x_buf, xsem.at[0])
    g_copy = pltpu.make_async_copy(g_hbm, g_buf, xsem.at[1])
    tab_copy = pltpu.make_async_copy(tab_hbm, tab_buf, xsem.at[2])
    g_copy.start()
    x_copy.start()
    tab_copy.start()
    w_copies = [[pltpu.make_async_copy(wq_hbm.at[:, pl.ds(i * wide, wide)], w_buf.at[i], wsem.at[i])] for i in range(nq)]
    w_copies.append([
        pltpu.make_async_copy(wk_hbm, w_buf.at[nq, :, pl.ds(0, BLK)], wsem.at[nq]),
        pltpu.make_async_copy(wv_hbm, w_buf.at[nq, :, pl.ds(BLK, BLK)], wsem.at[nq + 1]),
    ])
    w_copies[0][0].start()

    def cache_copies(g):
        at = pl.ds(g * nreq, nreq)
        return (
            pltpu.make_async_copy(k_hbm.at[at], k_buf.at[at], kvsem.at[0, g]),
            pltpu.make_async_copy(v_hbm.at[at], v_buf.at[at], kvsem.at[1, g]),
        )

    def out_copies(g):
        at = pl.ds(g * nreq, nreq)
        return (
            pltpu.make_async_copy(k_buf.at[at], ko_hbm.at[at], osem.at[0, g]),
            pltpu.make_async_copy(v_buf.at[at], vo_hbm.at[at], osem.at[1, g]),
        )

    def part_copy(g):
        return pltpu.make_async_copy(out_buf.at[pl.ds(2 * g, 2)], out_hbm.at[pl.ds(2 * g, 2)], osem.at[2, g])

    def fetch(lo, hi):
        for g in range(lo, hi):
            for cp in cache_copies(g):
                cp.start()

    g_copy.wait()
    gain = g_buf[...].astype(F32).reshape(1, dim)
    x_copy.wait()
    for cps in w_copies[1:]:
        for cp in cps:
            cp.start()

    def norm(i, carry):
        at = pl.ds(pl.multiple_of(i * 16, 16), 16)
        xf = x_buf[at, :].astype(F32)
        inv = lax.rsqrt(jnp.sum(xf * xf, axis=-1, keepdims=True) * (1.0 / dim) + NORM_EPS)
        u_buf[at, :] = (xf * inv * gain).astype(BF16)
        return carry

    lax.fori_loop(0, rows // 16, norm, 0, unroll=2)
    tab_copy.wait()

    def angle(i, carry):
        rot_buf[pl.ds(i, 1), :] = tab_buf[pl.ds(lens_ref[i], 1), :]
        return carry

    lax.fori_loop(0, rows, angle, 0, unroll=16)
    cosv = rot_buf[:, :128]
    sinv = rot_buf[:, 128:]

    def rope(h):
        h = h.astype(BF16).astype(F32)
        return (h * cosv + pltpu.roll(h, 64, 1) * sinv).astype(BF16).astype(F32)

    for i in range(nq + 1):
        for cp in w_copies[i]:
            cp.wait()
        fetch(groups * i // (nq + 1), groups * (i + 1) // (nq + 1))
        prod = jnp.dot(u_buf[...], w_buf[i], preferred_element_type=F32)
        for s in range(4):
            part = prod[:, s * 128 : (s + 1) * 128]
            if i < nq:
                q_buf[pl.ds(4 * i + s, rows, stride=heads), :] = rope(part)
            elif s < 2:
                kn_buf[pl.ds(s, rows, stride=2), :] = rope(part)
            else:
                vn_buf[pl.ds(s - 2, rows, stride=2), :] = part.astype(BF16).astype(F32)

    lane = lax.broadcasted_iota(jnp.int32, (8, 128), 1)
    head = lax.broadcasted_iota(jnp.int32, (8, 128), 0)
    match = (lane % 2) == (head // 4)
    lane_pos = jnp.where(match, lane // 2, 1 << 20)
    row16 = lax.broadcasted_iota(jnp.int32, (16, 128), 0)
    scale = 128.0**-0.5
    zero = jnp.zeros((8, 128), BF16)

    def insert(b, c_buf, n_buf, blk, off):
        row0 = jnp.broadcast_to(n_buf[pl.ds(2 * b, 1), :], (16, 128))
        row1 = jnp.broadcast_to(n_buf[pl.ds(2 * b + 1, 1), :], (16, 128))
        new = jnp.where(row16 == off, row0, row1)
        old = c_buf[b, blk].astype(F32)
        c_buf[b, blk] = jnp.where((row16 == off) | (row16 == off + 1), new, old).astype(BF16)

    def group(g, carry):
        for cp in cache_copies(g):
            cp.wait()

        def put(i, c):
            b = g * nreq + i
            pos = lens_ref[b] - base
            inside = (pos >= 0) & (pos < 64)
            at = jnp.where(inside, pos, 0)
            off = jnp.where(inside, 2 * (at % 8), -8)
            insert(b, k_buf, kn_buf, at // 8, off)
            insert(b, v_buf, vn_buf, at // 8, off)
            return c

        lax.fori_loop(0, nreq, put, 0, unroll=8)
        for cp in out_copies(g):
            cp.start()

        first = g * nreq
        scores = []
        for p in range(16):
            b = first + 2 * p
            keys = k_buf[pl.ds(b, 2)].reshape(256, 128)
            qp = q_buf[pl.ds(pl.multiple_of(b * 8, 16), 16), :].astype(BF16)
            scores.append(lax.dot_general(qp, keys, (((1,), (1,)), ((), ())), preferred_element_type=F32))
        for h in range(2):
            half = g * 2 + h
            wts = []
            stm, stl = jnp.zeros((8, 128), F32), jnp.ones((8, 128), F32)
            for p in range(8):
                for j in range(2):
                    s = scores[8 * h + p][8 * j : 8 * j + 8, 128 * j : 128 * j + 128] * scale
                    valid = lane_pos <= lens_ref[first + 16 * h + 2 * p + j] - base
                    m = jnp.max(jnp.where(valid, s, NEG), axis=1, keepdims=True)
                    w = jnp.where(valid, jnp.exp(s - m), 0.0)
                    here = lane == 2 * p + j
                    stm = jnp.where(here, m, stm)
                    stl = jnp.where(here, jnp.sum(w, axis=1, keepdims=True), stl)
                    wts.append(w.astype(BF16))
            out_buf[half, 128:136, :] = stm
            out_buf[half, 136:144, :] = stl
            for p in range(8):
                wp = jnp.concatenate([jnp.concatenate([wts[2 * p], zero], axis=1), jnp.concatenate([zero, wts[2 * p + 1]], axis=1)], axis=0)
                vals = v_buf[pl.ds(first + 16 * h + 2 * p, 2)].reshape(256, 128)
                out_buf[half, 16 * p : 16 * p + 16, :] = jnp.dot(wp, vals, preferred_element_type=F32)
        part_copy(g).start()
        return carry

    lax.fori_loop(0, groups, group, 0)
    for g in range(groups):
        for cp in out_copies(g):
            cp.wait()
        part_copy(g).wait()


def front(lens, x, g, tab, wq, wk, wv, k, v):
    rows, dim = x.shape
    heads = wq.shape[1] // 128
    nblk = wq.shape[1] // (2 * BLK) + 1
    groups = rows // 32
    dma = pltpu.SemaphoreType.DMA
    return pl.pallas_call(
        front_kernel,
        out_shape=(
            jax.ShapeDtypeStruct(k.shape, BF16),
            jax.ShapeDtypeStruct(v.shape, BF16),
            jax.ShapeDtypeStruct((2 * groups, PART, 128), F32),
        ),
        in_specs=[pl.BlockSpec(memory_space=pltpu.SMEM)] + [ANY] * 8,
        out_specs=(ANY, ANY, ANY),
        scratch_shapes=[
            pltpu.VMEM((rows, dim), BF16),
            pltpu.VMEM((dim,), BF16),
            pltpu.VMEM(tab.shape, F32),
            pltpu.VMEM((rows, 256), F32),
            pltpu.VMEM((rows, dim), BF16),
            pltpu.VMEM((nblk, dim, 2 * BLK), BF16),
            pltpu.VMEM(k.shape, BF16),
            pltpu.VMEM(v.shape, BF16),
            pltpu.VMEM((rows * heads, 128), F32),
            pltpu.VMEM((rows * 2, 128), F32),
            pltpu.VMEM((rows * 2, 128), F32),
            pltpu.VMEM((2 * groups, PART, 128), F32),
            dma((3,)),
            dma((nblk + 1,)),
            dma((2, groups)),
            dma((3, groups)),
        ],
        compiler_params=pltpu.CompilerParams(vmem_limit_bytes=63_000_000),
        cost_estimate=pl.CostEstimate(flops=4 * rows * dim * nblk * BLK, bytes_accessed=4 * dim * nblk * BLK + 8 * k.size, transcendentals=0),
        name="front",
    )(lens, x, g, tab, wq, wk, wv, k, v)


def merge(blocks, out_ref, last):
    rows = PART - 16
    maxs = [b[rows : rows + 8, :] for b in blocks]
    top = functools.reduce(jnp.maximum, maxs)
    facs = [jnp.exp(m - top) for m in maxs]
    tot = functools.reduce(jnp.add, [f * b[rows + 8 : rows + 16, :] for f, b in zip(facs, blocks)])
    if last:
        inv = 1.0 / tot
        facs = [f * inv for f in facs]
    else:
        out_ref[rows : rows + 8, :] = top
        out_ref[rows + 8 : rows + 16, :] = tot
    for i in range(rows // 8):
        at = slice(8 * i, 8 * i + 8)
        out_ref[at, :] = functools.reduce(jnp.add, [b[at, :] * f[:, i : i + 1] for f, b in zip(facs, blocks)])


def tail_kernel(
    att_hbm, x_hbm, g_hbm, wo_hbm, wg_hbm, wu_hbm, wd_hbm, y_hbm,
    att_ref, g_ref, d1_buf, m_buf, r1_buf, o_buf, p_buf, z1_buf, a1_buf, h_buf, hb_buf, a_buf, p2_buf, d2_buf, s2_buf, z2_buf, a2_buf, yg_buf, yo_buf, x_buf, hid_buf,
    wo_buf, wg_buf, wu_buf, wd_buf,
    lsem, gsem, usem, dsem, osem, d1s, d1r, r1s, r1r, z1s, z1r, hs, hr, hds, hdr, d2s, d2r, z2s, z2r, ys, yr, ydr, turn,
):
    tp, sp = lax.axis_index("tp"), lax.axis_index("sp")
    core, chip = sp % 2, sp // 2
    cx, cy = chip % 2, chip // 2
    mate = {"tp": tp, "sp": 2 * chip + (1 - core)}
    plane = [(chip + k) % 4 for k in range(4)]
    plane_id = [{"tp": tp, "sp": 2 * q + core} for q in plane]
    side = tp // 2
    inside = tp * (1 - 2 * side) + 3 * side
    is_end, is_in = inside == 0, inside == 1

    def place(m):
        return m + side * (3 - 2 * m)

    near, second, far = place(1 - inside), place(2), place(3)

    def zdev(z):
        return {"tp": z, "sp": sp}

    dim = x_buf.shape[1]
    ring = wg_buf.shape[0]
    half = wd_buf.shape[1]
    nff = half // BLK
    ndn = wd_buf.shape[0]
    dcol = wd_buf.shape[2]

    me8 = pl.multiple_of(32 * sp + 8 * tp, 8)
    x_copy = pltpu.make_async_copy(x_hbm.at[pl.ds(me8, 8), :], x_buf, lsem.at[0])
    wo_copy = pltpu.make_async_copy(wo_hbm, wo_buf, lsem.at[1])

    def ff_copies(j, slot):
        at = pl.ds(pl.multiple_of(core * half + j * BLK, BLK), BLK)
        return (
            pltpu.make_async_copy(wg_hbm.at[:, at], wg_buf.at[slot], gsem.at[slot]),
            pltpu.make_async_copy(wu_hbm.at[:, at], wu_buf.at[slot], usem.at[slot]),
        )

    def dn_copy(j):
        return pltpu.make_async_copy(
            wd_hbm.at[pl.ds(pl.multiple_of(core * half, BLK), half), pl.ds(pl.multiple_of(j * dcol, dcol), dcol)], wd_buf.at[j], dsem.at[j]
        )

    att_copy = pltpu.make_async_copy(att_hbm, att_ref, lsem.at[2])
    g_copy = pltpu.make_async_copy(g_hbm, g_ref, lsem.at[3])
    att_copy.start()
    x_copy.start()
    g_copy.start()

    def prefetch_ff(lo, hi):
        for j in range(lo, min(hi, ring, nff)):
            for cp in ff_copies(j, j):
                cp.start()

    @pl.when(is_end)
    def _():
        z1_buf[2] = jnp.zeros_like(z1_buf[2])
        z2_buf[2] = jnp.zeros_like(z2_buf[2])

    bar = pltpu.get_barrier_semaphore()
    for dev in [mate] + plane_id[1:] + [zdev((tp + k) % 4) for k in (1, 2, 3)]:
        pl.semaphore_signal(bar, inc=1, device_id=dev, device_id_type=MESH)
    pl.semaphore_wait(bar, 7)

    drains = []

    def send(src, dst, ssem, rsem, dev, cond=None):
        def make():
            return pltpu.make_async_remote_copy(src_ref=src, dst_ref=dst, send_sem=ssem, recv_sem=rsem, device_id=dev, device_id_type=MESH)

        def go():
            make().start()

        def done():
            make().wait_send()

        if cond is None:
            go()
            drains.append(done)
        else:
            pl.when(cond)(go)
            drains.append(lambda: pl.when(cond)(done))

    def landed(ref, rsem):
        pltpu.make_async_copy(ref, ref, rsem).wait()

    order = [1, 2, 3, 0]
    att_copy.wait()
    wo_copy.start()
    for k in order:
        send(att_ref.at[pl.ds(4 * plane[k] + 2 * (1 - core), 2)], d1_buf.at[k], d1s.at[k], d1r.at[k], mate)
    for k in order:
        landed(d1_buf.at[k], d1r.at[k])
        for h in range(2):
            merge([att_ref.at[4 * plane[k] + 2 * core + h], d1_buf.at[k, h]], m_buf.at[k, h], False)

    @pl.when(core == 1)
    def _():
        pl.semaphore_wait(turn, 1)

    before = len(drains)
    for k in (1, 2, 3):
        send(m_buf.at[k], r1_buf.at[k - 1], r1s.at[k - 1], r1r.at[k - 1], plane_id[k])
    plane_sent = drains[before:]
    del drains[before:]

    @pl.when(core == 0)
    def _():
        for done in plane_sent:
            done()
        pl.semaphore_signal(turn, inc=1, device_id=mate, device_id_type=MESH)

    prefetch_ff(0, 2)
    for k in (1, 2, 3):
        landed(r1_buf.at[k - 1], r1r.at[k - 1])
    for h in range(2):
        merge([m_buf.at[0, h]] + [r1_buf.at[k, h] for k in range(3)], o_buf.at[pl.ds(128 * h, 128)], True)

    def rows8(z):
        return pl.ds(pl.multiple_of(8 * z, 8), 8)

    def scatter(j, cols, src, buf, agg, ss, rs):
        send(src.at[rows8(second), cols], buf.at[2 - inside, :, cols], ss.at[j, 0], rs.at[j, 2 - inside], zdev(second))
        send(src.at[rows8(far), cols], agg.at[:, cols], ss.at[j, 1], rs.at[j, 3], zdev(near), is_end)
        send(src.at[rows8(near), cols], buf.at[0, :, cols], ss.at[j, 2], rs.at[j, 0], zdev(near))

    def relay(j, cols, src, buf, agg, ss, rs):
        @pl.when(is_in)
        def _():
            landed(agg.at[:, cols], rs.at[j, 3])
            src[rows8(far), cols] = src[rows8(far), cols] + agg[:, cols]

        send(src.at[rows8(far), cols], buf.at[1, :, cols], ss.at[j, 1], rs.at[j, 1], zdev(far), is_in)

    def gathered(j, cols, src, buf, rs):
        landed(buf.at[0, :, cols], rs.at[j, 0])
        landed(buf.at[1, :, cols], rs.at[j, 1])

        @pl.when(is_in)
        def _():
            landed(buf.at[2, :, cols], rs.at[j, 2])

        return src[rows8(tp), cols] + buf[0, :, cols] + buf[1, :, cols] + buf[2, :, cols]

    o = jnp.concatenate([o_buf[pl.ds(h, 32, stride=8), :].astype(BF16) for h in range(8)], axis=1)
    wo_copy.wait()

    def proj(j, carry):
        at = pl.ds(pl.multiple_of(j * 512, 512), 512)
        p_buf[:, at] = jnp.dot(o, wo_buf[:, at], preferred_element_type=F32)
        return carry

    parts1 = [pl.ds(i * (dim // 2), dim // 2) for i in range(2)]
    for i in range(2):
        lax.fori_loop(i * (dim // 1024), (i + 1) * (dim // 1024), proj, 0)
        scatter(i, parts1[i], p_buf, z1_buf, a1_buf, z1s, z1r)
    prefetch_ff(2, ring)
    for i in range(2):
        relay(i, parts1[i], p_buf, z1_buf, a1_buf, z1s, z1r)
    for j in range(ndn // 2):
        dn_copy(j).start()
    x_copy.wait()
    g_copy.wait()
    for i in range(2):
        hid_buf[:, parts1[i]] = (x_buf[:, parts1[i]].astype(F32) + gathered(i, parts1[i], p_buf, z1_buf, z1r)).astype(BF16).astype(F32)
    hid = hid_buf[...]
    inv = lax.rsqrt(jnp.sum(hid * hid, axis=-1, keepdims=True) * (1.0 / dim) + NORM_EPS)
    mine = core * 4
    h_buf[mine + tp] = (hid * inv * g_ref[...].astype(F32).reshape(1, dim)).astype(BF16).astype(F32)

    def spread(block, ss, rs, first):
        send(block(tp), block(tp), ss(first), rs(tp), zdev(second))
        send(block(tp), block(tp), ss(first + 1), rs(tp), zdev(far), is_in)
        send(block(tp), block(tp), ss(first + 2), rs(tp), zdev(near))

    def h_block(z):
        return h_buf.at[mine + z]

    spread(h_block, lambda i: hs.at[i], lambda z: hr.at[z], 0)
    send(h_block(tp), h_block(tp), hds.at[0], hdr.at[tp], mate)
    for j in range(ndn // 2, ndn):
        dn_copy(j).start()
    for i, z in enumerate((near, second, far)):
        landed(h_block(z), hr.at[z])
        if i == 2:
            send(h_block(z), h_block(z), hs.at[3], hr.at[z], zdev(near), is_in)
        send(h_block(z), h_block(z), hds.at[1 + i], hdr.at[z], mate)
    for z in range(4):
        landed(h_buf.at[4 * (1 - core) + z], hdr.at[z])
    for i in range(4):
        hb_buf[16 * i : 16 * i + 16, :] = jnp.concatenate([h_buf[2 * i], h_buf[2 * i + 1]], axis=0).astype(BF16)

    def ff(j, carry):
        slot = lax.rem(j, ring)
        for cp in ff_copies(j, slot):
            cp.wait()
        gate = jnp.dot(hb_buf[...], wg_buf[slot], preferred_element_type=F32).astype(BF16).astype(F32)
        up = jnp.dot(hb_buf[...], wu_buf[slot], preferred_element_type=F32).astype(BF16).astype(F32)
        a_buf[:, pl.ds(pl.multiple_of(j * BLK, BLK), BLK)] = (gate * jax.nn.sigmoid(gate) * up).astype(BF16)

        @pl.when(j + ring < nff)
        def _():
            for cp in ff_copies(j + ring, slot):
                cp.start()

        return carry

    lax.fori_loop(0, nff, ff, 0)

    nc = CHUNKS
    width = dim // nc
    cols = [pl.ds(j * width, width) for j in range(nc)]
    xn = 2 * cy + (1 - cx)
    yn = 2 * (1 - cy) + cx
    dg = 2 * (1 - cy) + (1 - cx)
    xn_id, yn_id = {"tp": tp, "sp": 2 * xn + core}, {"tp": tp, "sp": 2 * yn + core}
    zorder = (tp, near, second, far)
    count = [0] * nc

    def block(j, c, z):
        return yg_buf.at[4 * (2 * c + core) + z, :, cols[j]]

    def pass_on(j, c, z, dev, rs, cond=None):
        send(block(j, c, z), block(j, c, z), ys.at[j, count[j]], rs, dev, cond)
        count[j] += 1

    def down(j):
        def one(i, carry):
            dn_copy(i).wait()
            p2_buf[:, pl.ds(pl.multiple_of(i * dcol, dcol), dcol)] = jnp.dot(a_buf[...], wd_buf[i], preferred_element_type=F32)
            return carry

        lax.fori_loop(j * ndn // nc, (j + 1) * ndn // nc, one, 0)
        send(p2_buf.at[pl.ds(pl.multiple_of(32 * (1 - core), 32), 32), cols[j]], d2_buf.at[:, cols[j]], d2s.at[j], d2r.at[j], mate)

    def pair(j):
        landed(d2_buf.at[:, cols[j]], d2r.at[j])
        s2_buf[:, cols[j]] = p2_buf[pl.ds(pl.multiple_of(32 * core, 32), 32), cols[j]] + d2_buf[:, cols[j]]
        scatter(j, cols[j], s2_buf, z2_buf, a2_buf, z2s, z2r)

    def mid(j):
        relay(j, cols[j], s2_buf, z2_buf, a2_buf, z2s, z2r)

    def own(j):
        yg_buf[4 * sp + tp, :, cols[j]] = (hid_buf[:, cols[j]] + gathered(j, cols[j], s2_buf, z2_buf, z2r)).astype(BF16).astype(F32)
        pass_on(j, chip, tp, xn_id, yr.at[j, 4 + tp])
        pass_on(j, chip, tp, yn_id, yr.at[j, 8 + tp])
        at = count[j]
        spread(lambda z: block(j, chip, z), lambda i: ys.at[j, i], lambda z: yr.at[j, z], at)
        count[j] = at + 3

    def four(j, c, which):
        return yg_buf.at[pl.ds(4 * (2 * c + which), 4), :, cols[j]]

    def hand_over(j, c, i):
        send(four(j, c, core), four(j, c, core), ys.at[j, count[j]], ydr.at[j, i], mate)
        count[j] += 1

    def column(j):
        for i, z in enumerate(zorder[1:]):
            landed(block(j, chip, z), yr.at[j, z])
            if i == 2:
                pass_on(j, chip, z, zdev(near), yr.at[j, z], is_in)
            pass_on(j, chip, z, xn_id, yr.at[j, 4 + z])
            pass_on(j, chip, z, yn_id, yr.at[j, 8 + z])
        hand_over(j, chip, 0)

    def around(j):
        for i, z in enumerate(zorder):
            landed(block(j, xn, z), yr.at[j, 4 + z])
            if i % 2 == 0:
                pass_on(j, xn, z, yn_id, yr.at[j, 12 + z])
            landed(block(j, yn, z), yr.at[j, 8 + z])
            if i % 2 == 1:
                pass_on(j, yn, z, xn_id, yr.at[j, 12 + z])
        hand_over(j, xn, 1)
        hand_over(j, yn, 2)

    def across(j):
        for z in zorder:
            landed(block(j, dg, z), yr.at[j, 12 + z])
        hand_over(j, dg, 3)

    def out_copy(j):
        return pltpu.make_async_copy(yo_buf.at[:, cols[j]], y_hbm.at[:, cols[j]], osem.at[j])

    def finish(j):
        for i, c in enumerate((chip, xn, yn, dg)):
            landed(four(j, c, 1 - core), ydr.at[j, i])

        def out(i, carry):
            yo_buf[pl.ds(pl.multiple_of(i * 16, 16), 16), cols[j]] = jnp.concatenate([yg_buf[2 * i, :, cols[j]], yg_buf[2 * i + 1, :, cols[j]]], axis=0).astype(BF16)
            return carry

        lax.fori_loop(0, yg_buf.shape[0] // 2, out, 0)
        out_copy(j).start()

    down(0)
    for i in range(1, max(nc, LEAD + 2)):
        if i < nc:
            down(i)
        if i <= LEAD:
            pair(i - 1)
        if 2 <= i <= LEAD + 1:
            mid(i - 2)
    stages = [(0, own), (-LEAD, pair), (LAGS[0], column), (1 - LEAD, mid), (LAGS[1], around), (LAGS[2], across), (LAGS[3], finish)]
    for t in range(nc + LAGS[3]):
        for lag, stage in stages:
            j = t - lag
            if j < nc and (j >= 0 if lag >= 0 else j >= LEAD):
                stage(j)
    for done in drains:
        done()

    @pl.when(core == 1)
    def _():
        for done in plane_sent:
            done()

    for j in range(nc):
        out_copy(j).wait()


def tail(att, x, g, wo, wg, wu, wd):
    batch, dim = x.shape
    half = wg.shape[1] // 2
    ring = min(5, half // BLK)
    ndn = 8
    dma = pltpu.SemaphoreType.DMA
    return pl.pallas_call(
        tail_kernel,
        out_shape=jax.ShapeDtypeStruct((batch, dim), BF16),
        in_specs=[ANY] * 7,
        out_specs=ANY,
        scratch_shapes=[
            pltpu.VMEM(att.shape, F32),
            pltpu.VMEM((dim,), BF16),
            pltpu.VMEM((4, 2, PART, 128), F32),
            pltpu.VMEM((4, 2, PART, 128), F32),
            pltpu.VMEM((3, 2, PART, 128), F32),
            pltpu.VMEM((256, 128), F32),
            pltpu.VMEM((32, dim), F32),
            pltpu.VMEM((3, 8, dim), F32),
            pltpu.VMEM((8, dim), F32),
            pltpu.VMEM((8, 8, dim), F32),
            pltpu.VMEM((64, dim), BF16),
            pltpu.VMEM((64, half), BF16),
            pltpu.VMEM((64, dim), F32),
            pltpu.VMEM((32, dim), F32),
            pltpu.VMEM((32, dim), F32),
            pltpu.VMEM((3, 8, dim), F32),
            pltpu.VMEM((8, dim), F32),
            pltpu.VMEM((batch // 8, 8, dim), F32),
            pltpu.VMEM((batch, dim), BF16),
            pltpu.VMEM((8, dim), BF16),
            pltpu.VMEM((8, dim), F32),
            pltpu.VMEM(wo.shape, BF16),
            pltpu.VMEM((ring, dim, BLK), BF16),
            pltpu.VMEM((ring, dim, BLK), BF16),
            pltpu.VMEM((ndn, half, dim // ndn), BF16),
            dma((4,)), dma((ring,)), dma((ring,)), dma((ndn,)), dma((CHUNKS,)),
            dma((4,)), dma((4,)), dma((3,)), dma((3,)), dma((2, 3)), dma((2, 4)),
            dma((4,)), dma((4,)), dma((4,)), dma((4,)), dma((CHUNKS,)), dma((CHUNKS,)), dma((CHUNKS, 3)), dma((CHUNKS, 4)),
            dma((CHUNKS, 22)), dma((CHUNKS, 16)), dma((CHUNKS, 4)), pltpu.SemaphoreType.REGULAR,
        ],
        compiler_params=pltpu.CompilerParams(collective_id=0, has_side_effects=True, vmem_limit_bytes=63_000_000),
        cost_estimate=pl.CostEstimate(flops=2 * 64 * dim * half * 3, bytes_accessed=6 * dim * half, transcendentals=0),
        name="tail",
    )(att, x, g, wo, wg, wu, wd)


def land_kernel(y_hbm, out_hbm, buf, isem, osem):
    n = isem.shape[0]
    rows = buf.shape[0] // n
    ats = [pl.ds(i * rows, rows) for i in range(n)]
    ins = [pltpu.make_async_copy(y_hbm.at[at, :], buf.at[at, :], isem.at[i]) for i, at in enumerate(ats)]
    outs = [pltpu.make_async_copy(buf.at[at, :], out_hbm.at[at, :], osem.at[i]) for i, at in enumerate(ats)]
    for cp in ins:
        cp.start()
    for a, b in zip(ins, outs):
        a.wait()
        b.start()
    for cp in outs:
        cp.wait()


def land(y):
    return pl.pallas_call(
        land_kernel,
        out_shape=jax.ShapeDtypeStruct(y.shape, y.dtype),
        in_specs=[ANY],
        out_specs=ANY,
        scratch_shapes=[pltpu.VMEM(y.shape, y.dtype), pltpu.SemaphoreType.DMA((4,)), pltpu.SemaphoreType.DMA((4,))],
        compiler_params=pltpu.CompilerParams(vmem_limit_bytes=63_000_000),
        name="land",
    )(y)


def rope_table(length):
    freq = np.power(ROPE_BASE, np.arange(64) * (-2.0 / 128)).astype(np.float32)
    angles = (np.arange(length, dtype=np.float32)[:, None] * freq).astype(np.float64)
    cos, sin = np.cos(angles), np.sin(angles)
    return jnp.asarray(np.concatenate([cos, cos, -sin, sin], axis=1), F32)


def solution(mesh):
    cache_spec = P(None, "sp", "tp", None)
    col_spec = P(None, "tp")
    row_spec = P("tp", None)
    full_spec = P()

    def local_step(x_tok, seq_lens, k_blk, v_blk, g_attn, wq, wk, wv, wo, g_mlp, wg, wu, wd):
        batch = x_tok.shape[0]
        shape = (batch, 8, 16, 128)
        k_out, v_out, att = front(seq_lens, x_tok, g_attn, rope_table(k_blk.shape[1] * mesh.shape["sp"]), wq, wk, wv, k_blk.reshape(shape), v_blk.reshape(shape))
        y = tail(att, x_tok, g_mlp, wo, wg, wu, wd)
        return land(y), k_out.reshape(k_blk.shape), v_out.reshape(v_blk.shape)

    return jax.shard_map(local_step, mesh=mesh, in_specs=(full_spec, full_spec, cache_spec, cache_spec, full_spec, col_spec, col_spec, col_spec, row_spec, full_spec, col_spec, col_spec, row_spec), out_specs=(full_spec, cache_spec, cache_spec), check_vma=False)
```
